32 devices in a mesh: wide: 8 (over z, x), narrow: 4 (over y, core).
Axes of the slice: x: 2, y: 2, z: 4, core: 2. Of those that a mesh axis runs over, the one named last changes fastest.
Arguments:
- images: bfloat16 [512, 82, 512], P(('wide', 'narrow')), may hold values from -6 to 6
- grid_sizes: int32 [512], P(('wide', 'narrow')), may hold values from 5 to 9, as said below
- qkv_weight: bfloat16 [2, 786432], P(None, ('wide', 'narrow')), may hold values from -0.375 to 0.375
- proj_weight: bfloat16 [2, 262144], P(None, ('wide', 'narrow')), may hold values from -0.25 to 0.25
- fc1_weight: bfloat16 [2, 1048576], P(None, ('wide', 'narrow')), may hold values from -0.25 to 0.25
- fc2_weight: bfloat16 [2, 1048576], P(None, ('wide', 'narrow')), may hold values from -0.125 to 0.125
- small_params: bfloat16 [2, 36864], P(None, ('wide', 'narrow'))
- cotangent: bfloat16 [512, 82, 512], P(('wide', 'narrow')), may hold values from -6 to 6
Outputs:
- output: bfloat16 [512, 82, 512], P(('wide', 'narrow'))
- grad_images: float32 [512, 82, 512], P(('wide', 'narrow'))
- grad_qkv: float32 [2, 786432], P(None, ('wide', 'narrow'))
- grad_proj: float32 [2, 262144], P(None, ('wide', 'narrow'))
- grad_fc1: float32 [2, 1048576], P(None, ('wide', 'narrow'))
- grad_fc2: float32 [2, 1048576], P(None, ('wide', 'narrow'))
- grad_small: float32 [2, 36864], P(None, ('wide', 'narrow'))
The draws below stay inside these ranges and needn't reach their ends.
Inputs may be any that keep to these rules, and one draw needn't show every extreme that they name: `grid_sizes`: each image's grid side is one of 5, 7, 9; some image has side 9.
All inputs are finite; a program needn't handle non-finite values.
Results may differ from the reference program's by a relative error of at most 0.0095.
Values may be sent and summed in bfloat16 or wider, within the bound.
A program may use at most 320 MiB of HBM per device.

```python
import jax
import jax.numpy as jnp
from jax import lax

D = 512
FF = 2048
HEADS = 8
LAYERS = 2
GRID_MAX = 9
SLOT = 82
SMALL_COLS = 58
CPE_COLS = 10
SMALLS = 36864
IMG_DEV = 16
IMAGES = 512


def draw_grid_sizes(key, part):
    picks = jax.random.randint(key, (IMAGES,), 0, 3)
    grid_sides = 5 + 2 * picks
    position = lax.broadcasted_iota(jnp.int32, (IMAGES,), 0)
    grid_sides = jnp.where(position == 0, GRID_MAX, jnp.where(position == 1, 5, grid_sides))
    return grid_sides.astype(jnp.int32)


def draw_small_params(key, part):
    shaped = (LAYERS, SMALLS)
    base = jax.random.normal(key, shaped, jnp.float32)
    flat_index = lax.broadcasted_iota(jnp.int32, shaped, 1)
    table_end = SMALL_COLS * D
    column = flat_index % SMALL_COLS
    in_table = flat_index < table_end
    gain_col = in_table & ((column == 0) | (column == 2))
    kernel_col = in_table & (column >= 9)
    scale_of = jnp.where(gain_col, 0.15, jnp.where(kernel_col, 0.2, 0.3))
    offset = jnp.where(gain_col, 1.0, 0.0)
    return (offset + scale_of * base).astype(jnp.bfloat16)


def levels(key, extent, cuts, low, top_value):
    gain, own = 1.0, jax.random.fold_in(key, 6)
    for dim, blocks in cuts:
        heights = jnp.exp(jax.random.uniform(jax.random.fold_in(own, dim), (blocks,), jnp.float32, low / len(cuts), top_value / len(cuts)))
        gain = gain * jnp.repeat(heights, extent[dim] // blocks).reshape([-1 if axis == dim else 1 for axis in range(len(extent))])
    return gain


def noise(key, shape, deviation, reach, shards=(), held_as=jnp.bfloat16):
    level = levels(key, shape, shards, -0.22, 0.18) if shards else 1.0
    entries = jax.random.normal(key, shape, jnp.float32) * deviation * level
    return jnp.minimum(jnp.maximum(entries, -reach), reach).astype(held_as)


def setup_inputs(seed: int = 0) -> dict:
    arg_keys = jax.random.split(jax.random.key(seed), 9)
    return {
        "images": noise(arg_keys[0], (IMAGES, SLOT, D), 1.0, 6.0, ((0, 32),)),
        "grid_sizes": draw_grid_sizes(jax.random.fold_in(arg_keys[8], 71), 0),
        "qkv_weight": noise(arg_keys[2], (LAYERS, 3 * D * D), (D // 2) ** -0.5, 0.375, ((1, 32),)),
        "proj_weight": noise(arg_keys[3], (LAYERS, D * D), D ** -0.5, 0.25, ((1, 32),)),
        "fc1_weight": noise(arg_keys[4], (LAYERS, D * FF), D ** -0.5, 0.25, ((1, 32),)),
        "fc2_weight": noise(arg_keys[5], (LAYERS, FF * D), FF ** -0.5, 0.125, ((1, 32),)),
        "small_params": draw_small_params(jax.random.fold_in(arg_keys[8], 71), 0),
        "cotangent": noise(arg_keys[7], (IMAGES, SLOT, D), 1.0, 6.0, ((0, 32),)),
    }


PRECISE = lax.Precision.HIGHEST
NORM_EPS = 1e-06
ROOT_HALF = 0.7071067811865476

@jax.custom_vjp
def low(v):
    return lax.optimization_barrier(v.astype(jnp.bfloat16)).astype(jnp.float32)

@jax.custom_vjp
def low_back(v):
    return v

def low_keep(v):
    return (low(v), None)

def low_pass(kept, grad):
    return (grad,)

def back_keep(v):
    return (v, None)

def back_low(kept, grad):
    return (low(grad),)
low.defvjp(low_keep, low_pass)
low_back.defvjp(back_keep, back_low)

def grid_masks(grid_sides):
    slot_index = lax.broadcasted_iota(jnp.int32, (grid_sides.shape[0], SLOT), 1)
    cell_index = jnp.maximum(slot_index - 1, 0)
    side_col = grid_sides[:, None]
    inside = (slot_index >= 1) & (cell_index // GRID_MAX < side_col) & (cell_index % GRID_MAX < side_col)
    present = inside | (slot_index == 0)
    return (present.astype(jnp.float32)[:, :, None], inside.astype(jnp.float32)[:, :, None])

def to_grid(stream):
    return stream[:, 1:, :].reshape(stream.shape[0], GRID_MAX, GRID_MAX, stream.shape[2])

def from_grid(grid_cells):
    images_in = grid_cells.shape[0]
    channels = grid_cells.shape[3]
    flat_cells = grid_cells.reshape(images_in, GRID_MAX * GRID_MAX, channels)
    return jnp.concatenate([jnp.zeros((images_in, 1, channels), grid_cells.dtype), flat_cells], axis=1)

def depthwise(grid_cells, kernel, radius):
    span_taps = 2 * radius + 1
    padded = jnp.pad(grid_cells, ((0, 0), (radius, radius), (radius, radius), (0, 0)))
    summed = jnp.zeros_like(grid_cells)
    for row_tap in range(span_taps):
        for col_tap in range(span_taps):
            window_part = padded[:, row_tap:row_tap + GRID_MAX, col_tap:col_tap + GRID_MAX, :]
            summed = summed + window_part * kernel[:, row_tap * span_taps + col_tap]
    return summed

def window_mask(channels):
    channel = lax.broadcasted_iota(jnp.int32, (channels, 49), 0)
    tap_pos = lax.broadcasted_iota(jnp.int32, (channels, 49), 1)
    head_num = channel // (channels // HEADS)
    radius_of = jnp.where(head_num < 2, 1, jnp.where(head_num < 5, 2, 3))
    inside = (jnp.abs(tap_pos // 7 - 3) <= radius_of) & (jnp.abs(tap_pos % 7 - 3) <= radius_of)
    return inside.astype(jnp.float32)

def layer_norm(stream, gain_col, shift_col):
    average = lax.optimization_barrier(jnp.mean(stream, axis=-1, keepdims=True))
    centred = stream - average
    inv_std = lax.rsqrt(lax.optimization_barrier(jnp.mean(centred * centred, axis=-1, keepdims=True)) + NORM_EPS)
    return centred * inv_std * gain_col + shift_col

def matmul(left_side, right_side):
    return jnp.einsum('bsd,de->bse', left_side, right_side, precision=PRECISE)

def unpack(pieces):
    qkv_flat, proj_flat, fc1_flat, fc2_flat, small_vec = pieces
    table_end = SMALL_COLS * D
    table_cols = small_vec[:table_end].reshape(D, SMALL_COLS)
    fc1_bias = small_vec[table_end:table_end + FF]
    cpe_cols = small_vec[table_end + FF:].reshape(D, CPE_COLS)
    return (qkv_flat.reshape(D, 3 * D), proj_flat.reshape(D, D), fc1_flat.reshape(D, FF), fc2_flat.reshape(FF, D), table_cols, fc1_bias, cpe_cols)

def mix_block(stream, pieces, present, inside):
    qkv_mat, proj_mat, fc1_mat, fc2_mat, table_cols, fc1_bias, cpe_cols = unpack(pieces)
    window = window_mask(D)
    head_dim = D // HEADS
    shaped = (stream.shape[0], stream.shape[1], HEADS, head_dim)
    conv_part = from_grid(depthwise(to_grid(stream * inside), cpe_cols[:, 0:9], 1))
    first = stream + inside * (conv_part + cpe_cols[:, 9])
    normed_one = low(layer_norm(first, table_cols[:, 0], table_cols[:, 1]))
    qkv_bias = jnp.concatenate([table_cols[:, 4], jnp.zeros_like(table_cols[:, 4]), table_cols[:, 5]])
    joined = low_back(matmul(normed_one, qkv_mat) + qkv_bias)
    query, keys, values = jnp.split(joined, 3, axis=2)
    masked = jnp.where(present > 0, keys, -1e+30)
    largest = lax.optimization_barrier(jnp.max(masked, axis=1, keepdims=True))
    raised = jnp.exp(masked - largest)
    key_probs = raised / lax.optimization_barrier(jnp.sum(raised, axis=1, keepdims=True))
    summary = jnp.einsum('bshi,bshj->bhij', key_probs.reshape(shaped), values.reshape(shaped), precision=PRECISE)
    factor = jnp.einsum('bshi,bhij->bshj', query.reshape(shaped), summary, precision=PRECISE).reshape(stream.shape)
    relative = from_grid(depthwise(to_grid(values * inside), table_cols[:, 9:] * window, 3)) + table_cols[:, 8]
    attended = low(factor * head_dim ** (-0.5) + inside * query * relative)
    second = first + low_back(matmul(attended, proj_mat) + table_cols[:, 6])
    normed_two = low(layer_norm(second, table_cols[:, 2], table_cols[:, 3]))
    hidden_pre = low_back(matmul(normed_two, fc1_mat) + fc1_bias)
    activated = low(0.5 * hidden_pre * (1.0 + lax.erf(hidden_pre * ROOT_HALF)))
    return second + low_back(matmul(activated, fc2_mat) + table_cols[:, 7])

def forward(stream, params, grid_sides):
    present, inside = grid_masks(grid_sides)
    for layer_index in range(LAYERS):
        pieces = tuple((member[layer_index] for member in params))
        stream = mix_block(stream, pieces, present, inside)
    return stream * present

def reference(images, grid_sizes, qkv_weight, proj_weight, fc1_weight, fc2_weight, small_params, cotangent):
    params = tuple((member.astype(jnp.float32) for member in (qkv_weight, proj_weight, fc1_weight, fc2_weight, small_params)))
    per_group = 2 * IMG_DEV
    groups = IMAGES // per_group
    stream_all = images.astype(jnp.float32).reshape(groups, per_group, SLOT, D)
    cot_all = cotangent.astype(jnp.float32).reshape(groups, per_group, SLOT, D)
    side_all = grid_sizes.reshape(groups, per_group)

    def one_group(totals, inputs):
        stream_part, side_part, cot_part = inputs

        def local_forward(stream_in, params_in):
            return forward(stream_in, params_in, side_part)
        result, pull = jax.vjp(local_forward, stream_part, params)
        grad_stream, grad_params = pull(cot_part)
        totals = tuple((first_sum + second_sum for first_sum, second_sum in zip(totals, grad_params)))
        return (totals, (result, grad_stream))
    zero_sums = tuple((jnp.zeros_like(member) for member in params))
    totals, (results, grad_streams) = lax.scan(one_group, zero_sums, (stream_all, side_all, cot_all))
    output = results.reshape(IMAGES, SLOT, D).astype(jnp.bfloat16)
    grad_images = grad_streams.reshape(IMAGES, SLOT, D)
    return (output, grad_images, totals[0], totals[1], totals[2], totals[3], totals[4])
```

```python
import functools
import jax
import jax.numpy as jnp
from jax import lax
from jax.experimental import pallas as pl
from jax.experimental.pallas import tpu as pltpu

F32, BF16 = jnp.float32, jnp.bfloat16
D, FF, HEADS, GRID, SLOT = 512, 2048, 8, 9, 82
TABLE = 58
EPS = 1e-6
NI = 16
R = SLOT * NI
PADS = 96
RP = PADS * NI
RADII = (1, 2, 3, 3)
TAPS, CPE, CPEB, TROWS = 9, 58, 67, 72


def ds(start, size, align=8):
    if not isinstance(start, int):
        start = pl.multiple_of(start, align)
    return pl.ds(start, size)


def row8(ref, i, lg):
    return ref[lg, pl.ds(i, 8, stride=0), :]


def row(tab, i, j=None):
    parts = range(4) if j is None else (2 * j, 2 * j + 1)
    return jnp.concatenate([tab[g, i:i + 1, :] for g in parts], axis=1)


def put2(ref, at, j, val):
    ref[2 * j, at, :] = val[:, :128]
    ref[2 * j + 1, at, :] = val[:, 128:]


def cell(y, x, ig):
    return ds((1 + GRID * y + x) * NI + 8 * ig, 8)


def inside_at(sz, y, x):
    return sz > max(y, x)


def conv_pass(load_row, load_tap, radius, emit, flip=False):
    span = 2 * radius + 1
    for y in range(GRID):
        acc = [None] * GRID
        for a in range(span):
            yy = y - (a - radius) if flip else y + a - radius
            if not 0 <= yy < GRID:
                continue
            row = load_row(yy)
            for b in range(span):
                tap = load_tap(a - radius, b - radius)
                for x in range(GRID):
                    xx = x - (b - radius) if flip else x + b - radius
                    if 0 <= xx < GRID:
                        term = row[xx] * tap
                        acc[x] = term if acc[x] is None else acc[x] + term
        emit(y, acc)


def conv_kgrad(load_grad, load_src, radius, emit):
    span = 2 * radius + 1
    for a in range(span):
        acc = [None] * span
        for y in range(GRID):
            yy = y + a - radius
            if not 0 <= yy < GRID:
                continue
            grad = load_grad(y)
            src = load_src(yy)
            for b in range(span):
                for x in range(GRID):
                    xx = x + b - radius
                    if 0 <= xx < GRID:
                        term = grad[x] * src[xx]
                        acc[b] = term if acc[b] is None else acc[b] + term
        for b in range(span):
            emit(a - radius, b - radius, acc[b])


def lane_of(lg):
    return ds(lg * 128, 128, 128)


def for_groups(body):
    def one(radius, base):
        def run(i, c):
            body(radius, base + i // 2, i % 2)
            return c
        return run
    lax.fori_loop(0, 2, one(1, 0), 0)
    lax.fori_loop(0, 2, one(2, 1), 0)
    lax.fori_loop(0, 4, one(3, 2), 0)


def norm_rows(x):
    mean = jnp.mean(x, axis=-1, keepdims=True)
    cen = x - mean
    inv = lax.rsqrt(jnp.mean(cen * cen, axis=-1, keepdims=True) + EPS)
    return cen * inv, inv


def normal_cdf(u):
    a = jnp.abs(u)
    t = 1.0 / (1.0 + a * (0.3275911 * 0.7071067811865476))
    e = jnp.exp(-0.5 * u * u)
    poly = t * (0.5 * 0.254829592 + t * (0.5 * -0.284496736 + t * (0.5 * 1.421413741 + t * (0.5 * -1.453152027 + t * (0.5 * 1.061405429)))))
    tail = poly * e
    return jnp.where(u >= 0, 1.0 - tail, tail), e


LN_T = 112
ROW_T = 336


def tile_start(i, size):
    return pl.multiple_of(jnp.minimum(i * size, R - size), 16)


def head_mask():
    r = lax.broadcasted_iota(jnp.int32, (256, 256), 0) // 64
    c = lax.broadcasted_iota(jnp.int32, (256, 256), 1) // 64
    return r == c


def dot(a, b, ca, cb):
    return lax.dot_general(a, b, (((ca,), (cb,)), ((), ())), preferred_element_type=F32)


def fwd_conv1(x, sz, tab, x1):
    def body(i, c):
        lg, ig = i // 2, i % 2
        lane = lane_of(lg)
        size = sz[ds(8 * ig, 8), :]
        cls = ds(8 * ig, 8)
        x1[cls, lane] = x[cls, lane].astype(F32)
        bias = row8(tab, CPEB, lg)

        def load_row(y):
            return [jnp.where(inside_at(size, y, k), x[cell(y, k, ig), lane].astype(F32), 0.0) for k in range(GRID)]

        def emit(y, acc):
            for k in range(GRID):
                at = cell(y, k, ig)
                x1[at, lane] = x[at, lane].astype(F32) + jnp.where(inside_at(size, y, k), acc[k] + bias, 0.0)

        conv_pass(load_row, lambda a, b: row8(tab, CPE + (a + 1) * 3 + b + 1, lg), 1, emit)
        return c
    lax.fori_loop(0, 8, body, 0)


def norm_phase(src, tab, gain, shift, hat, low, inv_ref):
    def body(i, c):
        at = pl.ds(tile_start(i, LN_T), LN_T)
        n, inv = norm_rows(src[at, :])
        hat[at, :] = n.astype(BF16)
        low[at, :] = (n * row(tab, gain) + row(tab, shift)).astype(BF16)
        inv_ref[at, :] = jnp.broadcast_to(inv, (LN_T, 128))
        return c
    lax.fori_loop(0, 12, body, 0)


def fwd_qkv(low, w, tab, q, k, v):
    def body(i, c):
        at = pl.ds(tile_start(i, ROW_T), ROW_T)
        h = low[at, :]
        for j in range(2):
            cols = slice(256 * j, 256 * j + 256)
            put2(q, at, j, dot(h, w[:, cols], 1, 0) + row(tab, 4, j))
            put2(k, at, j, dot(h, w[:, 512 + 256 * j:768 + 256 * j], 1, 0))
            put2(v, at, j, dot(h, w[:, 1024 + 256 * j:1280 + 256 * j], 1, 0) + row(tab, 5, j))
        return c
    lax.fori_loop(0, 4, body, 0)
    tail = slice(R, RP)
    for ref in (q, k, v):
        ref[:, tail, :] = jnp.zeros((4, RP - R, 128), F32)


def each_pos(size, ig, fn):
    fn(ds(8 * ig, 8), None)
    for y in range(GRID):
        for x in range(GRID):
            fn(cell(y, x, ig), inside_at(size, y, x))


def fwd_softmax(k, sz):
    def body(i, c):
        lg, ig = i // 2, i % 2
        lane = lane_of(lg)
        size = sz[ds(8 * ig, 8), :]
        best = [None] * 4
        cnt = [0]

        def first(at, ok):
            val = k[lg, at, :]
            if ok is not None:
                val = jnp.where(ok, val, -1e30)
            j = cnt[0] % 4
            best[j] = val if best[j] is None else jnp.maximum(best[j], val)
            cnt[0] += 1
        each_pos(size, ig, first)
        top = jnp.maximum(jnp.maximum(best[0], best[1]), jnp.maximum(best[2], best[3]))
        total = [None] * 4
        cnt[0] = 0

        def second(at, ok):
            val = jnp.exp(k[lg, at, :] - top)
            if ok is not None:
                val = jnp.where(ok, val, 0.0)
            k[lg, at, :] = val
            j = cnt[0] % 4
            total[j] = val if total[j] is None else total[j] + val
            cnt[0] += 1
        each_pos(size, ig, second)
        scale = 1.0 / ((total[0] + total[1]) + (total[2] + total[3]))

        def third(at, ok):
            k[lg, at, :] = k[lg, at, :] * scale
        each_pos(size, ig, third)
        return c
    lax.fori_loop(0, 8, body, 0)


def img_load(ref, i, half):
    return jnp.concatenate([ref[2 * half + j, pl.ds(i, PADS, stride=NI), :] for j in range(2)], axis=1)


def img_store(ref, i, half, val):
    for j in range(2):
        ref[2 * half + j, pl.ds(i, PADS, stride=NI), :] = val[:, 128 * j:128 * j + 128]


def fwd_attn(q, p, v, s, f):
    def body(t, c):
        i, half = t // 2, t % 2
        pi = img_load(p, i, half).astype(BF16)
        vi = img_load(v, i, half).astype(BF16)
        summ = jnp.where(head_mask(), dot(pi, vi, 0, 0), 0.0).astype(BF16)
        s[t] = summ
        qi = img_load(q, i, half).astype(BF16)
        img_store(f, i, half, dot(qi, summ, 1, 0) * 0.125)
        return c
    lax.fori_loop(0, 2 * NI, body, 0)


def fwd_conv3(v, q, f, sz, tab, rel, att):
    def body(radius, lg, ig):
        lane = lane_of(lg)
        size = sz[ds(8 * ig, 8), :]
        bias = row8(tab, 8, lg)

        def load_row(y):
            return [jnp.where(inside_at(size, y, k), v[lg, cell(y, k, ig), :], 0.0) for k in range(GRID)]

        def emit(y, acc):
            for k in range(GRID):
                at = cell(y, k, ig)
                r = acc[k] + bias
                rel[lg, at, :] = r
                att[lg, at, :] = f[lg, at, :] + jnp.where(inside_at(size, y, k), q[lg, at, :] * r, 0.0)
        conv_pass(load_row, lambda a, b: row8(tab, TAPS + (a + 3) * 7 + b + 3, lg), radius, emit)
    for_groups(body)


def fwd_proj(att, w, tab, x1, a_low):
    def body(i, c):
        at = pl.ds(pl.multiple_of(i * 656, 16), 656)
        low = jnp.concatenate([att[g, at, :] for g in range(4)], axis=1).astype(BF16)
        a_low[at, :] = low
        for j in range(2):
            cols = slice(256 * j, 256 * j + 256)
            x1[at, cols] = x1[at, cols] + dot(low, w[:, cols], 1, 0) + row(tab, 6, j)
        return c
    lax.fori_loop(0, 2, body, 0)


def fwd_fc1(low, w, b1, g, slope):
    def body(t, c):
        i, j = t // 8, t % 8
        at = pl.ds(tile_start(i, ROW_T), ROW_T)
        cols = pl.ds(pl.multiple_of(j * 256, 256), 256)
        u = dot(low[at, :], w[:, cols], 1, 0) + b1[:, cols]
        cdf, e = normal_cdf(u)
        g[at, cols] = (u * cdf).astype(BF16)
        slope[at, cols] = (cdf + u * e * 0.3989422804014327).astype(BF16)
        return c
    lax.fori_loop(0, 32, body, 0)


def fwd_fc2(g, w, tab, x2, x3):
    def body(i, c):
        at = pl.ds(pl.multiple_of(i * 656, 16), 656)
        for j in range(2):
            cols = slice(256 * j, 256 * j + 256)
            x3[at, cols] = x2[at, cols] + dot(g[at, :], w[:, cols], 1, 0) + row(tab, 7, j)
        return c
    lax.fori_loop(0, 2, body, 0)


def fwd_kernel(x, sz, tab, b1, wqkv, wproj, w1, w2,
               x3, n1, inv1, h1, q, p, v, s, rel, a_low, n2, inv2, h2, g, slope,
               x1, f):
    fwd_conv1(x, sz, tab, x1)
    norm_phase(x1, tab, 0, 1, n1, h1, inv1)
    fwd_qkv(h1, wqkv, tab, q, p, v)
    fwd_softmax(p, sz)
    fwd_attn(q, p, v, s, f)
    fwd_conv3(v, q, f, sz, tab, rel, f)
    fwd_proj(f, wproj, tab, x1, a_low)
    norm_phase(x1, tab, 2, 3, n2, h2, inv2)
    fwd_fc1(h2, w1, b1, g, slope)
    fwd_fc2(g, w2, tab, x1, x3)


RES = (
    ("n1", (R, D), BF16), ("inv1", (R, 128), F32), ("h1", (R, D), BF16),
    ("q", (4, RP, 128), F32), ("p", (4, RP, 128), F32), ("v", (4, RP, 128), F32),
    ("s", (2 * NI, 256, 256), BF16), ("rel", (4, R, 128), F32), ("a", (R, D), BF16),
    ("n2", (R, D), BF16), ("inv2", (R, 128), F32), ("h2", (R, D), BF16),
    ("g", (R, FF), BF16), ("slope", (R, FF), BF16))


def vspec(n):
    return [pl.BlockSpec(memory_space=pltpu.VMEM)] * n


PARAMS = pltpu.CompilerParams(vmem_limit_bytes=67043328)


def fwd_layer(x, sz, tab, b1, wqkv, wproj, w1, w2):
    outs = [jax.ShapeDtypeStruct((R, D), F32)] + [jax.ShapeDtypeStruct(sh, dt) for _, sh, dt in RES]
    return pl.pallas_call(
        fwd_kernel, out_shape=outs, in_specs=vspec(8), out_specs=vspec(len(outs)),
        scratch_shapes=[pltpu.VMEM((R, D), F32), pltpu.VMEM((4, RP, 128), F32)],
        compiler_params=PARAMS, name="block_fwd",
    )(x, sz, tab, b1, wqkv, wproj, w1, w2)


def add_rows(ref, row, val):
    total = val[0:8]
    for i in range(1, val.shape[0] // 8):
        total = total + val[8 * i:8 * i + 8]
    ref[8 * row:8 * row + 8, :] += total


def bwd_du(dx, w2, slope, dm, gb1):
    def cast(i, c):
        at = pl.ds(pl.multiple_of(i * 32, 16), 32)
        dm[at, :] = dx[at, :].astype(BF16)
        return c
    lax.fori_loop(0, 41, cast, 0)

    def body(t, c):
        i, j = t // 8, t % 8
        at = pl.ds(pl.multiple_of(i * 656, 16), 656)
        cols = pl.ds(pl.multiple_of(j * 256, 256), 256)
        d = dot(dm[at, :], w2[cols, :], 1, 1) * slope[at, cols].astype(F32)
        slope[at, cols] = d.astype(BF16)
        total = d[0:8]
        for k in range(1, 82):
            total = total + d[8 * k:8 * k + 8]
        keep = jnp.where(i == 0, 0.0, 1.0)
        gb1[:, cols] = gb1[:, cols] * keep + total
        return c
    gb1[...] = jnp.zeros_like(gb1)
    lax.fori_loop(0, 16, body, 0)


def norm_back_phase(up, hat, inv_ref, tab, gain, res, out_low, sums, rg, rs, rb):
    def body(i, c):
        at = pl.ds(pl.multiple_of(i * 32, 16), 32)
        u = up[at, :]
        n = hat[at, :].astype(F32)
        e = u * row(tab, gain)
        m1 = jnp.mean(e, axis=-1, keepdims=True)
        m2 = jnp.mean(e * n, axis=-1, keepdims=True)
        inv = inv_ref[at, 0:1]
        d = res[at, :] + inv * (e - m1 - n * m2)
        res[at, :] = d
        add_rows(sums, rg, u * n)
        add_rows(sums, rs, u)
        if out_low is not None:
            out_low[at, :] = d.astype(BF16)
        return c
    lax.fori_loop(0, 41, body, 0)


def mm_nt(a, w, out, split=False):
    def body(i, c):
        at = pl.ds(pl.multiple_of(i * 656, 16), 656)
        for j in range(2):
            val = dot(a[at, :], w[256 * j:256 * j + 256, :], 1, 1)
            if split:
                put2(out, at, j, val)
            else:
                out[at, 256 * j:256 * j + 256] = val
        return c
    lax.fori_loop(0, 2, body, 0)


def wgrad(left, right, out):
    wide_left = left.shape[1] > 512
    blocks = max(left.shape[1], right.shape[1]) // 512
    for j in range(blocks):
        cols = slice(512 * j, 512 * j + 512)
        if wide_left:
            out[cols, :] = dot(left[:, cols], right[...], 0, 0).astype(BF16)
        else:
            out[:, cols] = dot(left[...], right[:, cols], 0, 0).astype(BF16)


def bwd_attn1(q, p, v, s, da, dq, dv, dk):
    def body(t, c):
        i, half = t // 2, t % 2
        df = (img_load(da, i, half) * 0.125).astype(BF16)
        qi = img_load(q, i, half).astype(BF16)
        dsum = jnp.where(head_mask(), dot(qi, df, 0, 0), 0.0).astype(BF16)
        img_store(dq, i, half, dot(df, s[t], 1, 1))
        pi = img_load(p, i, half).astype(BF16)
        img_store(dv, i, half, dot(pi, dsum, 1, 0))
        vi = img_load(v, i, half).astype(BF16)
        img_store(dk, i, half, dot(vi, dsum, 1, 1))
        return c
    lax.fori_loop(0, 2 * NI, body, 0)


def bwd_mix(q, p, v, rel, da, dq, dv, dk, dj, sz, tab, gsum, gtap):
    def body(radius, lg, ig):
        lane = lane_of(lg)
        size = sz[ds(8 * ig, 8), :]

        acc = {"r": None, "q": None, "s": [None] * 4, "n": 0}

        def first(at, ok):
            d = da[lg, at, :]
            qv = q[lg, at, :]
            if ok is None:
                dqv = dq[lg, at, :]
                da[lg, at, :] = jnp.zeros_like(d)
            else:
                d = jnp.where(ok, d, 0.0)
                dr = qv * d
                da[lg, at, :] = dr
                acc["r"] = dr if acc["r"] is None else acc["r"] + dr
                dqv = dq[lg, at, :] + rel[lg, at, :] * d
            dq[lg, at, :] = dqv
            acc["q"] = dqv if acc["q"] is None else acc["q"] + dqv
            t = p[lg, at, :] * dk[lg, at, :]
            j = acc["n"] % 4
            acc["s"][j] = t if acc["s"][j] is None else acc["s"][j] + t
            acc["n"] += 1
        each_pos(size, ig, first)
        dot_sum = (acc["s"][0] + acc["s"][1]) + (acc["s"][2] + acc["s"][3])

        def second(at, ok):
            dk[lg, at, :] = p[lg, at, :] * (dk[lg, at, :] - dot_sum)
        each_pos(size, ig, second)
        gsum[ds(8 * (8 + 8 * 0), 8), lane] += acc["r"]
        gsum[ds(8 * 4, 8), lane] += acc["q"]

        def load_grad(y):
            return [da[lg, cell(y, k, ig), :] for k in range(GRID)]

        def load_src(y):
            return [jnp.where(inside_at(size, y, k), v[lg, cell(y, k, ig), :], 0.0) for k in range(GRID)]

        def emit_tap(a, b, val):
            at = ds(8 * (TAPS + (a + 3) * 7 + b + 3), 8)
            gsum[at, lane] += val
        conv_kgrad(load_grad, load_src, radius, emit_tap)
        vs = [dv[lg, ds(8 * ig, 8), :]]

        def emit(y, out):
            for k in range(GRID):
                at = cell(y, k, ig)
                val = dv[lg, at, :] + jnp.where(inside_at(size, y, k), out[k], 0.0)
                dv[lg, at, :] = val
                vs[0] = vs[0] + val
        conv_pass(load_grad, lambda a, b: row8(tab, TAPS + (a + 3) * 7 + b + 3, lg), radius, emit, flip=True)
        gsum[ds(8 * 5, 8), lane] += vs[0]
    for_groups(body)

    def cast(i, c):
        at = pl.ds(pl.multiple_of(i * 32, 16), 32)
        for j, ref in enumerate((dq, dk, dv)):
            for g in range(4):
                dj[at, 512 * j + 128 * g:512 * j + 128 * g + 128] = ref[g, at, :].astype(BF16)
        return c
    lax.fori_loop(0, 41, cast, 0)


def bwd_conv1(x, dx1, dx, sz, tab, gsum):
    def body(i, c):
        lg, ig = i // 2, i % 2
        lane = lane_of(lg)
        size = sz[ds(8 * ig, 8), :]
        cls = ds(8 * ig, 8)
        dx[cls, lane] = dx1[cls, lane]

        def load_grad(y):
            return [jnp.where(inside_at(size, y, k), dx1[cell(y, k, ig), lane], 0.0) for k in range(GRID)]

        def load_src(y):
            return [jnp.where(inside_at(size, y, k), x[cell(y, k, ig), lane].astype(F32), 0.0) for k in range(GRID)]

        def emit_tap(a, b, val):
            at = ds(8 * (CPE + (a + 1) * 3 + b + 1), 8)
            gsum[at, lane] += val
        conv_kgrad(load_grad, load_src, 1, emit_tap)
        bias = [jnp.zeros((8, 128), F32)]

        def emit(y, out):
            for k in range(GRID):
                at = cell(y, k, ig)
                g = dx1[at, lane]
                ok = inside_at(size, y, k)
                bias[0] = bias[0] + jnp.where(ok, g, 0.0)
                dx[at, lane] = g + jnp.where(ok, out[k], 0.0)
        conv_pass(load_grad, lambda a, b: row8(tab, CPE + (a + 1) * 3 + b + 1, lg), 1, emit, flip=True)
        gsum[ds(8 * CPEB, 8), lane] += bias[0]
        return c
    lax.fori_loop(0, 8, body, 0)


def col_sum(src, gsum, row):
    def body(i, c):
        at = pl.ds(pl.multiple_of(i * 32, 16), 32)
        add_rows(gsum, row, src[at, :].astype(F32))
        return c
    lax.fori_loop(0, 41, body, 0)


def bwd_e_kernel(dx3, tab, wproj, w1, w2, a_low, n2, inv2, h2, g, slope,
                 dx2, da, gw1, gw2, gproj, gsum, gb1, dm, up):
    gsum[...] = jnp.zeros_like(gsum)
    dx2[...] = dx3[...]
    bwd_du(dx2, w2, slope, dm, gb1)
    col_sum(dm, gsum, 7)
    wgrad(g, dm, gw2)
    wgrad(h2, slope, gw1)
    mm_nt(slope, w1, up)
    norm_back_phase(up, n2, inv2, tab, 2, dx2, dm, gsum, 2, 3, None)
    col_sum(dm, gsum, 6)
    wgrad(a_low, dm, gproj)
    mm_nt(dm, wproj, da, True)
    da[:, R:RP, :] = jnp.zeros((4, RP - R, 128), F32)


def bwd_f_kernel(x, sz, tab, wqkv, n1, inv1, h1, q, p, v, s, rel, dx2, da, gsum_in,
                 dx, gqkv, gsum, dq, dk, dv, dj, up):
    gsum[...] = gsum_in[...]
    bwd_attn1(q, p, v, s, da, dq, dv, dk)
    bwd_mix(q, p, v, rel, da, dq, dv, dk, dj, sz, tab, gsum, None)
    wgrad(h1, dj, gqkv)
    mm_nt(dj, wqkv, up)
    norm_back_phase(up, n1, inv1, tab, 0, dx2, None, gsum, 0, 1, None)
    bwd_conv1(x, dx2, dx, sz, tab, gsum)


def bwd_layer(dx3, x, sz, tab, b1, wqkv, wproj, w1, w2, res):
    sd = jax.ShapeDtypeStruct
    r = dict(zip([n for n, _, _ in RES], res))
    dx2, da, gw1, gw2, gproj, gsum, gb1 = pl.pallas_call(
        bwd_e_kernel,
        out_shape=[sd((R, D), F32), sd((4, RP, 128), F32), sd((D, FF), BF16), sd((FF, D), BF16), sd((D, D), BF16), sd((8 * TROWS, D), F32), sd((8, FF), F32)],
        in_specs=vspec(11), out_specs=vspec(7),
        scratch_shapes=[pltpu.VMEM((R, D), BF16), pltpu.VMEM((R, D), F32)],
        compiler_params=PARAMS, name="block_bwd_e",
    )(dx3, tab, wproj, w1, w2, r["a"], r["n2"], r["inv2"], r["h2"], r["g"], r["slope"])
    dx, gqkv, gsum = pl.pallas_call(
        bwd_f_kernel,
        out_shape=[sd((R, D), F32), sd((D, 3 * D), BF16), sd((8 * TROWS, D), F32)],
        in_specs=vspec(15), out_specs=vspec(3),
        scratch_shapes=[pltpu.VMEM((4, RP, 128), F32)] * 3 + [pltpu.VMEM((R, 3 * D), BF16), pltpu.VMEM((R, D), F32)],
        compiler_params=PARAMS, name="block_bwd_f",
    )(x, sz, tab, wqkv, r["n1"], r["inv1"], r["h1"], r["q"], r["p"], r["v"], r["s"], r["rel"], dx2, da, gsum)
    return dx, gqkv, gproj, gw1, gw2, gsum, gb1


AXES = ("wide", "narrow")


def window_mask():
    channel = lax.broadcasted_iota(jnp.int32, (49, D), 1)
    tap = lax.broadcasted_iota(jnp.int32, (49, D), 0)
    head = channel // (D // HEADS)
    reach = jnp.where(head < 2, 1, jnp.where(head < 5, 2, 3))
    return ((jnp.abs(tap // 7 - 3) <= reach) & (jnp.abs(tap % 7 - 3) <= reach)).astype(F32)


def blocks_of(flat, rows, cols):
    return flat.reshape(rows, cols // D, D).transpose(1, 0, 2).reshape(rows * cols // D, D)


def pack(qkv, proj, fc1, fc2, small, n):
    per = D // n
    width = small.shape[0]
    pad = -width % D
    parts = [blocks_of(qkv, per, 3 * D), proj.reshape(per, D), blocks_of(fc1, per, FF), fc2.reshape(FF // n, D), jnp.pad(small, (0, pad)).reshape(-1, D)]
    return jnp.concatenate(parts)


def unpack(full, n, small_count):
    per = D // n

    def block(j):
        return full[:, j * per:(j + 1) * per].reshape(D, D)
    wqkv = jnp.concatenate([block(0), block(1), block(2)], axis=1)
    w1 = jnp.concatenate([block(4 + j) for j in range(4)], axis=1)
    w2 = full[:, 8 * per:8 * per + FF // n].reshape(FF, D)
    small = full[:, 8 * per + FF // n:].reshape(n, -1)[:, :small_count].reshape(-1)
    return wqkv, block(3), w1, w2, small


def pack_grads(gqkv, gproj, gw1, gw2, small, n):
    per = D // n
    width = small.shape[0] // n
    pad = -width % D
    cols = [gqkv[:, j * D:(j + 1) * D] for j in range(3)] + [gproj] + [gw1[:, j * D:(j + 1) * D] for j in range(4)]
    parts = [c.reshape(n, per, D) for c in cols] + [gw2.reshape(n, FF // n, D)]
    parts.append(jnp.pad(small.reshape(n, width), ((0, 0), (0, pad))).reshape(n, -1, D).astype(BF16))
    return jnp.concatenate(parts, axis=1)


def split_grads(shard, n, width):
    per = D // n

    def cols(first, count):
        return shard[first * per:(first + count) * per].reshape(count, per, D).transpose(1, 0, 2).reshape(-1)
    fc2 = shard[8 * per:8 * per + FF // n].reshape(-1)
    small = shard[8 * per + FF // n:].reshape(-1)[:width]
    return cols(0, 3), cols(3, 1), cols(4, 4), fc2, small


def tables(small):
    small = small.astype(F32)
    end = TABLE * D
    tb = small[:end].reshape(D, TABLE).T
    cpe = small[end + FF:].reshape(D, 10).T
    tab = jnp.concatenate([tb[:9], tb[9:] * window_mask(), cpe, jnp.zeros((TROWS - 68, D), F32)])
    return tab.reshape(TROWS, 4, 128).transpose(1, 0, 2), small[end:end + FF][None]


def small_grads(gsum, gb1):
    s = gsum.reshape(TROWS, 8, D).sum(1)
    tb = jnp.concatenate([s[:9], s[9:58] * window_mask()]).T
    return jnp.concatenate([tb.reshape(-1), gb1.sum(0), s[58:68].T.reshape(-1)])


def to_rows(a):
    return jnp.transpose(a, (1, 0, 2)).reshape(R, D)


def from_rows(a):
    return jnp.transpose(a.reshape(SLOT, NI, D), (1, 0, 2))


def shards(n, images, grid_sizes, qkv, proj, fc1, fc2, small, cotangent):
    layers = qkv.shape[0]
    width = small.shape[1]
    packed = [pack(qkv[l], proj[l], fc1[l], fc2[l], small[l], n) for l in range(layers)]
    slot = lax.broadcasted_iota(jnp.int32, (SLOT, 1), 0)
    cellno = jnp.maximum(slot - 1, 0)
    far = jnp.maximum(cellno // GRID, cellno % GRID)
    present = ((slot == 0) | (far < grid_sizes[None, :]))[:, :, None]
    sz = jnp.broadcast_to(grid_sizes[:, None], (NI, 128))
    x = to_rows(images)
    saved = []
    for l in range(layers):
        full = lax.all_gather(packed[l][None], AXES, axis=0, tiled=True)
        wqkv, wproj, w1, w2, vec = unpack(full, n, width)
        tab, b1 = tables(vec)
        out = fwd_layer(x, sz, tab, b1, wqkv, wproj, w1, w2)
        saved.append((x, tab, b1, wqkv, wproj, w1, w2, out[1:]))
        x = out[0]
    output = from_rows(jnp.where(present, x.reshape(SLOT, NI, D), 0.0).astype(BF16))
    dx = jnp.where(present, jnp.transpose(cotangent, (1, 0, 2)), 0).astype(F32).reshape(R, D)
    shares = [None] * layers
    for l in reversed(range(layers)):
        xin, tab, b1, wqkv, wproj, w1, w2, res = saved[l]
        dx, gqkv, gproj, gw1, gw2, gsum, gb1 = bwd_layer(dx, xin, sz, tab, b1, wqkv, wproj, w1, w2, res)
        g = pack_grads(gqkv, gproj, gw1, gw2, small_grads(gsum, gb1), n)
        shares[l] = split_grads(lax.psum_scatter(g, AXES, scatter_dimension=0, tiled=True)[0].astype(F32), n, width)
    grads = [jnp.stack([shares[l][i] for l in range(layers)]) for i in range(5)]
    return (output, from_rows(dx), *grads)


def solution(mesh):
    n = mesh.shape["wide"] * mesh.shape["narrow"]
    from jax.sharding import PartitionSpec as P
    rows, flat = P(AXES, None, None), P(None, AXES)
    return jax.shard_map(
        functools.partial(shards, n), mesh=mesh,
        in_specs=(rows, P(AXES), flat, flat, flat, flat, flat, rows),
        out_specs=(rows, rows, flat, flat, flat, flat, flat),
        check_vma=False)
```

```python
import functools
import jax
import jax.numpy as jnp
from jax import lax
from jax.experimental import pallas as pl
from jax.experimental.pallas import tpu as pltpu

F32, BF16 = jnp.float32, jnp.bfloat16
D, FF, HEADS, GRID, SLOT = 512, 2048, 8, 9, 82
TABLE = 58
EPS = 1e-6
NI = 16
R = SLOT * NI
PADS = 96
RP = PADS * NI
RADII = (1, 2, 3, 3)
AXES = ("wide", "narrow")
WROWS = 192
TAPS, CPE, CPEB, TROWS = 9, 64, 73, 80


def ds(start, size, align=8):
    if not isinstance(start, int):
        start = pl.multiple_of(start, align)
    return pl.ds(start, size)


def row8(ref, i, lg):
    return ref[lg, pl.ds(i, 8, stride=0), :]


def row(tab, i, j=None):
    parts = range(4) if j is None else (2 * j, 2 * j + 1)
    return jnp.concatenate([tab[g, i:i + 1, :] for g in parts], axis=1)


def put2(ref, at, j, val):
    ref[2 * j, at, :] = val[:, :128]
    ref[2 * j + 1, at, :] = val[:, 128:]


def cell(y, x, ig):
    return ds((1 + GRID * y + x) * NI + 8 * ig, 8)


def inside_at(sz, y, x):
    return sz > max(y, x)


def conv_pass(load_row, load_tap, radius, emit, flip=False):
    span = 2 * radius + 1
    for y in range(GRID):
        acc = [None] * GRID
        for a in range(span):
            yy = y - (a - radius) if flip else y + a - radius
            if not 0 <= yy < GRID:
                continue
            row = load_row(yy)
            for b in range(span):
                tap = load_tap(a - radius, b - radius)
                for x in range(GRID):
                    xx = x - (b - radius) if flip else x + b - radius
                    if 0 <= xx < GRID:
                        term = row[xx] * tap
                        acc[x] = term if acc[x] is None else acc[x] + term
        emit(y, acc)


def conv_kgrad(load_grad, load_src, radius, emit):
    span = 2 * radius + 1
    for a in range(span):
        acc = [None] * span
        for y in range(GRID):
            yy = y + a - radius
            if not 0 <= yy < GRID:
                continue
            grad = load_grad(y)
            src = load_src(yy)
            for b in range(span):
                for x in range(GRID):
                    xx = x + b - radius
                    if 0 <= xx < GRID:
                        term = grad[x] * src[xx]
                        acc[b] = term if acc[b] is None else acc[b] + term
        for b in range(span):
            emit(a - radius, b - radius, acc[b])


def lane_of(lg):
    return ds(lg * 128, 128, 128)


def for_groups(body):
    def one(radius, base):
        def run(i, c):
            body(radius, base + i // 2, i % 2)
            return c
        return run
    lax.fori_loop(0, 2, one(1, 0), 0)
    lax.fori_loop(0, 2, one(2, 1), 0)
    lax.fori_loop(0, 4, one(3, 2), 0)


def norm_rows(x):
    mean = jnp.mean(x, axis=-1, keepdims=True)
    cen = x - mean
    inv = lax.rsqrt(jnp.mean(cen * cen, axis=-1, keepdims=True) + EPS)
    return cen * inv, inv


def normal_cdf(u):
    a = jnp.abs(u)
    t = 1.0 / (1.0 + a * (0.3275911 * 0.7071067811865476))
    e = jnp.exp(-0.5 * u * u)
    poly = t * (0.5 * 0.254829592 + t * (0.5 * -0.284496736 + t * (0.5 * 1.421413741 + t * (0.5 * -1.453152027 + t * (0.5 * 1.061405429)))))
    tail = poly * e
    return jnp.where(u >= 0, 1.0 - tail, tail), e


LN_T = 112
ROW_T = 336


def tile_start(i, size):
    return pl.multiple_of(jnp.minimum(i * size, R - size), 16)


def head_mask():
    r = lax.broadcasted_iota(jnp.int32, (256, 256), 0) // 64
    c = lax.broadcasted_iota(jnp.int32, (256, 256), 1) // 64
    return r == c


def dot(a, b, ca, cb):
    return lax.dot_general(a, b, (((ca,), (cb,)), ((), ())), preferred_element_type=F32)


def fwd_conv1(x, sz, tab, x1):
    def body(i, c):
        lg, ig = i // 2, i % 2
        lane = lane_of(lg)
        size = sz[ds(8 * ig, 8), :]
        cls = ds(8 * ig, 8)
        x1[cls, lane] = x[cls, lane].astype(F32)
        bias = row8(tab, CPEB, lg)

        def load_row(y):
            return [jnp.where(inside_at(size, y, k), x[cell(y, k, ig), lane].astype(F32), 0.0) for k in range(GRID)]

        def emit(y, acc):
            for k in range(GRID):
                at = cell(y, k, ig)
                x1[at, lane] = x[at, lane].astype(F32) + jnp.where(inside_at(size, y, k), acc[k] + bias, 0.0)

        conv_pass(load_row, lambda a, b: row8(tab, CPE + (a + 1) * 3 + b + 1, lg), 1, emit)
        return c
    lax.fori_loop(0, 8, body, 0)


def norm_phase(src, tab, gain, shift, hat, low, inv_ref):
    def body(i, c):
        at = pl.ds(tile_start(i, LN_T), LN_T)
        n, inv = norm_rows(src[at, :])
        hat[at, :] = n.astype(BF16)
        low[at, :] = (n * row(tab, gain) + row(tab, shift)).astype(BF16)
        inv_ref[at, :] = jnp.broadcast_to(inv, (LN_T, 128))
        return c
    lax.fori_loop(0, 12, body, 0)


def weight(g, block, first, count, cols):
    at = ds(16 * block, 16, 16)
    return jnp.concatenate([g[t % 2, t // 8, t // 4 % 2, t // 2 % 2, at, cols] for t in range(first // 16, (first + count) // 16)], axis=0)


def weight2(g, chunk, cols):
    return jnp.concatenate([g[i % 2, chunk // 2, chunk % 2, i // 2, 128:192, cols] for i in range(4)], axis=0)


def fwd_qkv(low, w, tab, q, k, v):
    def body(i, c):
        at = pl.ds(tile_start(i, ROW_T), ROW_T)
        h = low[at, :]
        for j in range(2):
            cols = slice(256 * j, 256 * j + 256)
            put2(q, at, j, dot(h, weight(w, 0, 0, D, cols), 1, 0) + row(tab, 4, j))
            put2(k, at, j, dot(h, weight(w, 1, 0, D, cols), 1, 0))
            put2(v, at, j, dot(h, weight(w, 2, 0, D, cols), 1, 0) + row(tab, 5, j))
        return c
    lax.fori_loop(0, 4, body, 0)
    tail = slice(R, RP)
    for ref in (q, k, v):
        ref[:, tail, :] = jnp.zeros((4, RP - R, 128), F32)


def each_pos(size, ig, fn):
    fn(ds(8 * ig, 8), None)
    for y in range(GRID):
        for x in range(GRID):
            fn(cell(y, x, ig), inside_at(size, y, x))


def fwd_softmax(k, sz):
    def body(i, c):
        lg, ig = i // 2, i % 2
        lane = lane_of(lg)
        size = sz[ds(8 * ig, 8), :]
        best = [None] * 4
        cnt = [0]

        def first(at, ok):
            val = k[lg, at, :]
            if ok is not None:
                val = jnp.where(ok, val, -1e30)
            j = cnt[0] % 4
            best[j] = val if best[j] is None else jnp.maximum(best[j], val)
            cnt[0] += 1
        each_pos(size, ig, first)
        top = jnp.maximum(jnp.maximum(best[0], best[1]), jnp.maximum(best[2], best[3]))
        total = [None] * 4
        cnt[0] = 0

        def second(at, ok):
            val = jnp.exp(k[lg, at, :] - top)
            if ok is not None:
                val = jnp.where(ok, val, 0.0)
            k[lg, at, :] = val
            j = cnt[0] % 4
            total[j] = val if total[j] is None else total[j] + val
            cnt[0] += 1
        each_pos(size, ig, second)
        scale = 1.0 / ((total[0] + total[1]) + (total[2] + total[3]))

        def third(at, ok):
            k[lg, at, :] = k[lg, at, :] * scale
        each_pos(size, ig, third)
        return c
    lax.fori_loop(0, 8, body, 0)


def img_load(ref, i, half):
    return jnp.concatenate([ref[2 * half + j, pl.ds(i, PADS, stride=NI), :] for j in range(2)], axis=1)


def img_store(ref, i, half, val):
    for j in range(2):
        ref[2 * half + j, pl.ds(i, PADS, stride=NI), :] = val[:, 128 * j:128 * j + 128]


def fwd_attn(q, p, v, s, f):
    def body(t, c):
        i, half = t // 2, t % 2
        pi = img_load(p, i, half).astype(BF16)
        vi = img_load(v, i, half).astype(BF16)
        summ = jnp.where(head_mask(), dot(pi, vi, 0, 0), 0.0).astype(BF16)
        s[t] = summ
        qi = img_load(q, i, half).astype(BF16)
        img_store(f, i, half, dot(qi, summ, 1, 0) * 0.125)
        return c
    lax.fori_loop(0, 2 * NI, body, 0)


def fwd_conv3(v, q, f, sz, tab, rel, att):
    def body(radius, lg, ig):
        lane = lane_of(lg)
        size = sz[ds(8 * ig, 8), :]
        bias = row8(tab, 8, lg)

        def load_row(y):
            return [jnp.where(inside_at(size, y, k), v[lg, cell(y, k, ig), :], 0.0) for k in range(GRID)]

        def emit(y, acc):
            for k in range(GRID):
                at = cell(y, k, ig)
                r = acc[k] + bias
                rel[lg, at, :] = r
                att[lg, at, :] = f[lg, at, :] + jnp.where(inside_at(size, y, k), q[lg, at, :] * r, 0.0)
        conv_pass(load_row, lambda a, b: row8(tab, TAPS + (a + 3) * 7 + b + 3, lg), radius, emit)
    for_groups(body)


def fwd_proj(att, w, tab, x1, a_low):
    def body(i, c):
        at = pl.ds(pl.multiple_of(i * 656, 16), 656)
        low = jnp.concatenate([att[g, at, :] for g in range(4)], axis=1).astype(BF16)
        a_low[at, :] = low
        for j in range(2):
            cols = slice(256 * j, 256 * j + 256)
            x1[at, cols] = x1[at, cols] + dot(low, weight(w, 3, 0, D, cols), 1, 0) + row(tab, 6, j)
        return c
    lax.fori_loop(0, 2, body, 0)


def fwd_fc1(low, w, b1, g, slope):
    def body(t, c):
        i, j = t // 8, t % 8
        at = pl.ds(tile_start(i, ROW_T), ROW_T)
        cols = pl.ds(pl.multiple_of(j * 256, 256), 256)
        half = pl.ds(pl.multiple_of(j % 2 * 256, 256), 256)
        bias = jnp.concatenate([b1[pl.ds(2 * j, 1), :], b1[pl.ds(2 * j + 1, 1), :]], axis=1)
        u = dot(low[at, :], weight(w, 4 + j // 2, 0, D, half), 1, 0) + bias
        cdf, e = normal_cdf(u)
        g[at, cols] = (u * cdf).astype(BF16)
        slope[at, cols] = (cdf + u * e * 0.3989422804014327).astype(BF16)
        return c
    lax.fori_loop(0, 32, body, 0)


def fwd_fc2(g, w, tab, x2, x3):
    def body(i, _):
        at = pl.ds(pl.multiple_of(i * 656, 16), 656)
        for j in range(2):
            cols = slice(256 * j, 256 * j + 256)
            x3[at, cols] = x2[at, cols] + dot(g[at, :], jnp.concatenate([weight2(w, c, cols) for c in range(8)], axis=0), 1, 0) + row(tab, 7, j)
        return _
    lax.fori_loop(0, 2, body, 0)


def fwd_phases(x, sz, tab, b1, w, x3, n1, inv1, h1, q, p, v, s, rel, a_low, n2, inv2, h2, g, slope, x1, f, tick=lambda: None):
    fwd_conv1(x, sz, tab, x1)
    norm_phase(x1, tab, 0, 1, n1, h1, inv1)
    tick(0)
    fwd_qkv(h1, w, tab, q, p, v)
    tick(1)
    fwd_softmax(p, sz)
    tick(2)
    fwd_attn(q, p, v, s, f)
    tick(3)
    fwd_conv3(v, q, f, sz, tab, rel, f)
    tick(4)
    fwd_proj(f, w, tab, x1, a_low)
    tick(5)
    norm_phase(x1, tab, 2, 3, n2, h2, inv2)
    tick(6)
    fwd_fc1(h2, w, b1, g, slope)
    tick(7)
    fwd_fc2(g, w, tab, x1, x3)
    tick(8)


RES = (
    ("n1", (R, D), BF16), ("inv1", (R, 128), F32), ("h1", (R, D), BF16),
    ("q", (4, RP, 128), F32), ("p", (4, RP, 128), F32), ("v", (4, RP, 128), F32),
    ("s", (2 * NI, 256, 256), BF16), ("rel", (4, R, 128), F32), ("a", (R, D), BF16),
    ("n2", (R, D), BF16), ("inv2", (R, 128), F32), ("h2", (R, D), BF16),
    ("g", (R, FF), BF16), ("slope", (R, FF), BF16))


def vspec(n):
    return [pl.BlockSpec(memory_space=pltpu.VMEM)] * n


PARAMS = pltpu.CompilerParams(vmem_limit_bytes=67043328)


MESH = pl.DeviceIdType.MESH


class Place:
    def __init__(self, line):
        w, m = lax.axis_index("wide"), lax.axis_index("narrow")
        self.line = line
        self.z, self.x, self.y, self.c = w // 2, w % 2, m // 2, m % 2

    def dev(self, z=None, x=None, y=None, c=None):
        z = self.z if z is None else z
        x = self.x if x is None else x
        y = self.y if y is None else y
        c = self.c if c is None else c
        return (z * 2 + x, y * 2 + c)

    def neighbours(self):
        n = self.line
        return (self.dev(x=1 - self.x), self.dev(y=1 - self.y), self.dev(c=1 - self.c),
                self.dev(z=lax.rem(self.z + 1, n)), self.dev(z=lax.rem(self.z + n - 1, n)))


def greet(place):
    barrier = pltpu.get_barrier_semaphore()
    for who in place.neighbours():
        pl.semaphore_signal(barrier, inc=1, device_id=who, device_id_type=MESH)
    pl.semaphore_wait(barrier, 5)


def remote(src, dst, send, recv, dev):
    return pltpu.make_async_remote_copy(src_ref=src, dst_ref=dst, send_sem=send, recv_sem=recv, device_id=dev, device_id_type=MESH)


def gather_ticks(place, g, rows, send, recv):
    n, z, x, y, c = place.line, place.z, place.x, place.y, place.c
    xs, ys, cs = 0, 1, 2

    def swap(core, sem, mine, dev):
        return remote(mine, mine, send.at[sem], recv.at[sem], dev)

    def pair_x(whole):
        part = g.at[1, :, x, :, rows] if whole else g.at[0, z, x, y, rows]
        return swap(0, xs, part, place.dev(x=1 - x))

    def pair_y(whole):
        part = g.at[1, :, x, y, rows] if whole else g.at[0, z, :, y, rows]
        return swap(0, ys, part, place.dev(y=1 - y))

    def line(core, k):
        def part(at):
            at = jnp.clip(at, 0, n - 1)
            return g.at[0, at, :, :, rows] if core == 0 else g.at[1, at, x, y, rows]
        right = remote(part(z - k + 1), part(z - k + 1), send.at[2 + k], recv.at[2 + k], place.dev(z=jnp.minimum(z + 1, n - 1)))
        left = remote(part(z + k - 1), part(z + k - 1), send.at[1 + n + k], recv.at[1 + n + k], place.dev(z=jnp.maximum(z - 1, 0)))
        return (right, (z + 1 < n) & (z - k + 1 >= 0), z - k >= 0), (left, (z > 0) & (z + k - 1 < n), z + k < n)

    def start_line(core, k):
        for copy, sends, _ in line(core, k):
            pl.when(sends)(copy.start)

    def wait_line(core, k):
        for copy, sends, gets in line(core, k):
            pl.when(sends)(copy.wait_send)
            pl.when(gets)(copy.wait_recv)

    def both(copy):
        copy.wait_send()
        copy.wait_recv()

    def core_copy(which):
        return remote(g.at[which, :, :, :, rows], g.at[which, :, :, :, rows], send.at[cs], recv.at[cs], place.dev(c=1 - c))

    first, second = [], []
    first.append(lambda: pair_x(False).start())
    first.append(lambda: (both(pair_x(False)), pair_y(False).start()))
    first.append(lambda: (both(pair_y(False)), start_line(0, 1)))
    for k in range(1, n - 1):
        first.append(lambda k=k: (wait_line(0, k), start_line(0, k + 1)))
    first.append(lambda: (wait_line(0, n - 1), core_copy(0).start()))
    first.append(lambda: both(core_copy(0)))
    second.append(lambda: start_line(1, 1))
    for k in range(1, n - 1):
        second.append(lambda k=k: (wait_line(1, k), start_line(1, k + 1)))
    second.append(lambda: (wait_line(1, n - 1), pair_y(True).start()))
    second.append(lambda: (both(pair_y(True)), pair_x(True).start()))
    second.append(lambda: (both(pair_x(True)), core_copy(1).start()))
    second.append(lambda: both(core_copy(1)))
    assert len(first) == len(second)

    def tick(a, b):
        def run():
            @pl.when(c == 0)
            def _():
                a()

            @pl.when(c == 1)
            def _():
                b()
        return run
    return [tick(a, b) for a, b in zip(first, second)]


def wave(lists):
    for r in range(max(i + len(t) for i, t in enumerate(lists))):
        for i, t in enumerate(lists):
            if 0 <= r - i < len(t):
                t[r - i]()


def gather_kernel(line, chunks, shard, g, own, send, recv):
    place = Place(line)
    mine = pltpu.make_async_copy(shard, g.at[place.c, place.z, place.x, place.y], own)
    mine.start()
    greet(place)
    mine.wait()
    wave([gather_ticks(place, g, pl.ds(a, b - a), send.at[i], recv.at[i]) for i, (a, b) in enumerate(chunks)])


def gather(shard, line, chunks, cid):
    rows = shard.shape[0]
    sems = pltpu.SemaphoreType.DMA((len(chunks), 3 + 2 * (line - 1) + 1))
    return pl.pallas_call(
        functools.partial(gather_kernel, line, chunks),
        out_shape=jax.ShapeDtypeStruct((2, line, 2, 2, rows, D), BF16),
        in_specs=[pl.BlockSpec(memory_space=pltpu.VMEM)], out_specs=pl.BlockSpec(memory_space=pltpu.VMEM),
        scratch_shapes=[pltpu.SemaphoreType.DMA, sems, sems],
        compiler_params=pltpu.CompilerParams(collective_id=cid, has_side_effects=True, vmem_limit_bytes=67043328),
        name="gather_weights")(shard)


def add_into(dst, src, out=None):
    out = dst if out is None else out
    out[...] = (dst[...].astype(F32) + src[...].astype(F32)).astype(out.dtype)


def build_tables(gs, layer, tau, y, tab, b1):
    for t in range(32):
        tau[9 * t:9 * t + 9, :] = gs[t % 2, t // 8, t // 4 % 2, t // 2 % 2, 16 * layer:16 * layer + 9, :]
    lane = lax.broadcasted_iota(jnp.int32, (8, 128), 1)

    def run(base, step, width, b):
        first, off = width * b // 128, width * b % 128
        val = tau[pl.ds(base + first, 8, stride=step), :]
        if off:
            val = pltpu.roll(val, 128 - off, 1)
            if off + width > 128:
                more = pltpu.roll(tau[pl.ds(base + first + 1, 8, stride=step), :], 128 - off, 1)
                val = jnp.where(lane < 128 - off, val, more)
        return val
    for b in range(64):
        tb = run(0, 29, TABLE, b)
        cpe = pltpu.roll(run(248, 5, 10, b), 64, 1)
        y[8 * b:8 * b + 8, :] = jnp.where(lane < TABLE, tb, jnp.where((lane >= 64) & (lane < 74), cpe, 0.0))
    r = lax.broadcasted_iota(jnp.int32, (D, D), 0)
    c = lax.broadcasted_iota(jnp.int32, (D, D), 1)
    place = jnp.where(c == 64 * (r % 8) + r // 8, 1.0, 0.0).astype(BF16)
    table = dot(y[...].astype(BF16), place, 0, 0)[:TROWS]
    tap = lax.broadcasted_iota(jnp.int32, (TROWS, D), 0) - TAPS
    head = lax.broadcasted_iota(jnp.int32, (TROWS, D), 1) // 64
    reach = jnp.where(head < 2, 1, jnp.where(head < 5, 2, 3))
    ok = (tap < 0) | (tap >= 49) | ((jnp.abs(tap // 7 - 3) <= reach) & (jnp.abs(tap % 7 - 3) <= reach))
    table = jnp.where(ok, table, 0.0)
    for g in range(4):
        tab[layer, g] = table[:, 128 * g:128 * g + 128]
    b1[layer] = tau[232:248, :]


CHUNKS = ((0, 64), (64, 128), (128, 192))


def first_kernel(line, x, sz, shard0, shard1, small,
                 x3, n1, inv1, h1, q, p, v, s, rel, a_low, n2, inv2, h2, g, slope, w0, w1, tab, b1,
                 x1, f, gs, tau, y, own, send, recv):
    place = Place(line)
    here = (place.c, place.z, place.x, place.y)
    puts = [pltpu.make_async_copy(src, dst.at[here], own.at[i]) for i, (src, dst) in enumerate(((shard0, w0), (shard1, w1), (small, gs)))]
    for cp in puts:
        cp.start()
    greet(place)
    for cp in puts:
        cp.wait()
    lists = [gather_ticks(place, gs, slice(None), send.at[0], recv.at[0])]
    lists += [gather_ticks(place, w0, pl.ds(a, b - a), send.at[1 + i], recv.at[1 + i]) for i, (a, b) in enumerate(CHUNKS)]
    lists += [gather_ticks(place, w1, pl.ds(a, b - a), send.at[4 + i], recv.at[4 + i]) for i, (a, b) in enumerate(CHUNKS)]
    depth = len(lists[0])
    rounds = []
    for r in range(depth + len(lists) - 1):
        rounds.append([t[r - i] for i, t in enumerate(lists) if 0 <= r - i < depth])
    todo = iter(rounds)
    done = [0]

    def advance(upto):
        while done[0] < upto:
            for t in next(todo):
                t()
            done[0] += 1
    advance(depth)
    for layer in range(2):
        build_tables(gs, layer, tau, y, tab, b1)
    need = {0: depth + 1, 6: depth + 3}

    def tick(i):
        advance(min(max(done[0] + 1, need.get(i, 0)), len(rounds)))
    fwd_phases(x, sz, tab.at[0], b1.at[0], w0, x3, n1, inv1, h1, q, p, v, s, rel, a_low, n2, inv2, h2, g, slope, x1, f, tick)
    advance(len(rounds))


def fwd_kernel(x, sz, tab, b1, w, *refs):
    fwd_phases(x, sz, tab, b1, w, *refs, tick=lambda i: None)


def fwd_first(line, x, sz, shard0, shard1, small):
    sd = jax.ShapeDtypeStruct
    pack = (2, line, 2, 2)
    outs = [sd((R, D), F32)] + [sd(sh, dt) for _, sh, dt in RES] + [sd(pack + (WROWS, D), BF16)] * 2 + [sd((2, 4, TROWS, 128), F32), sd((2, 16, 128), F32)]
    sems = pltpu.SemaphoreType.DMA((7, 3 + 2 * (line - 1) + 1))
    return pl.pallas_call(
        functools.partial(first_kernel, line), out_shape=outs, in_specs=vspec(5), out_specs=vspec(len(outs)),
        scratch_shapes=[pltpu.VMEM((R, D), F32), pltpu.VMEM((4, RP, 128), F32), pltpu.VMEM(pack + (32, 128), F32), pltpu.VMEM((288, 128), F32),
                        pltpu.VMEM((D, 128), F32), pltpu.SemaphoreType.DMA((3,)), sems, sems],
        compiler_params=pltpu.CompilerParams(vmem_limit_bytes=67043328, collective_id=0, has_side_effects=True), name="first_fwd",
    )(x, sz, shard0, shard1, small)


def fwd_layer(x, sz, tab, b1, w):
    outs = [jax.ShapeDtypeStruct((R, D), F32)] + [jax.ShapeDtypeStruct(sh, dt) for _, sh, dt in RES]
    return pl.pallas_call(
        fwd_kernel, out_shape=outs, in_specs=vspec(5), out_specs=vspec(len(outs)),
        scratch_shapes=[pltpu.VMEM((R, D), F32), pltpu.VMEM((4, RP, 128), F32)],
        compiler_params=PARAMS, name="block_fwd",
    )(x, sz, tab, b1, w)


def add_rows(ref, row, val):
    total = val[0:8]
    for i in range(1, val.shape[0] // 8):
        total = total + val[8 * i:8 * i + 8]
    ref[8 * row:8 * row + 8, :] += total


def bwd_du(dx, w2, slope, dm, gb1):
    def cast(i, c):
        at = pl.ds(pl.multiple_of(i * 32, 16), 32)
        dm[at, :] = dx[at, :].astype(BF16)
        return c
    lax.fori_loop(0, 41, cast, 0)

    def body(t, c):
        i, j = t // 8, t % 8
        at = pl.ds(pl.multiple_of(i * 656, 16), 656)
        cols = pl.ds(pl.multiple_of(j * 256, 256), 256)
        d = dot(dm[at, :], weight2(w2, j, slice(None)), 1, 1) * slope[at, cols].astype(F32)
        slope[at, cols] = d.astype(BF16)
        total = d[0:8]
        for k in range(1, 82):
            total = total + d[8 * k:8 * k + 8]
        keep = jnp.where(i == 0, 0.0, 1.0)
        gb1[:, cols] = gb1[:, cols] * keep + total
        return c
    gb1[...] = jnp.zeros_like(gb1)
    lax.fori_loop(0, 16, body, 0)


def norm_back_phase(up, hat, inv_ref, tab, gain, res, out_low, sums, rg, rs, rb):
    def body(i, c):
        at = pl.ds(pl.multiple_of(i * 32, 16), 32)
        u = up[at, :]
        n = hat[at, :].astype(F32)
        e = u * row(tab, gain)
        m1 = jnp.mean(e, axis=-1, keepdims=True)
        m2 = jnp.mean(e * n, axis=-1, keepdims=True)
        inv = inv_ref[at, 0:1]
        d = res[at, :] + inv * (e - m1 - n * m2)
        res[at, :] = d
        add_rows(sums, rg, u * n)
        add_rows(sums, rs, u)
        if out_low is not None:
            out_low[at, :] = d.astype(BF16)
        return c
    lax.fori_loop(0, 41, body, 0)


def mm_nt(a, g, first, blocks, out, split=False):
    def body(i, c):
        at = pl.ds(pl.multiple_of(i * 656, 16), 656)
        for j in range(2):
            w = jnp.concatenate([weight(g, first + b, 256 * j, 256, slice(None)) for b in range(blocks)], axis=1)
            val = dot(a[at, :], w, 1, 1)
            if split:
                put2(out, at, j, val)
            else:
                out[at, 256 * j:256 * j + 256] = val
        return c
    lax.fori_loop(0, 2, body, 0)


def wgrad(left, right, out):
    wide_left = left.shape[1] > 512
    blocks = max(left.shape[1], right.shape[1]) // 512
    for j in range(blocks):
        cols = slice(512 * j, 512 * j + 512)
        if wide_left:
            out[cols, :] = dot(left[:, cols], right[...], 0, 0).astype(BF16)
        else:
            out[:, cols] = dot(left[...], right[:, cols], 0, 0).astype(BF16)


def bwd_attn1(q, p, v, s, da, dq, dv, dk):
    def body(t, c):
        i, half = t // 2, t % 2
        df = (img_load(da, i, half) * 0.125).astype(BF16)
        qi = img_load(q, i, half).astype(BF16)
        dsum = jnp.where(head_mask(), dot(qi, df, 0, 0), 0.0).astype(BF16)
        img_store(dq, i, half, dot(df, s[t], 1, 1))
        pi = img_load(p, i, half).astype(BF16)
        img_store(dv, i, half, dot(pi, dsum, 1, 0))
        vi = img_load(v, i, half).astype(BF16)
        img_store(dk, i, half, dot(vi, dsum, 1, 1))
        return c
    lax.fori_loop(0, 2 * NI, body, 0)


def bwd_mix(q, p, v, rel, da, dq, dv, dk, dj, sz, tab, gsum, gtap):
    def body(radius, lg, ig):
        lane = lane_of(lg)
        size = sz[ds(8 * ig, 8), :]

        acc = {"r": None, "q": None, "s": [None] * 4, "n": 0}

        def first(at, ok):
            d = da[lg, at, :]
            qv = q[lg, at, :]
            if ok is None:
                dqv = dq[lg, at, :]
                da[lg, at, :] = jnp.zeros_like(d)
            else:
                d = jnp.where(ok, d, 0.0)
                dr = qv * d
                da[lg, at, :] = dr
                acc["r"] = dr if acc["r"] is None else acc["r"] + dr
                dqv = dq[lg, at, :] + rel[lg, at, :] * d
            dq[lg, at, :] = dqv
            acc["q"] = dqv if acc["q"] is None else acc["q"] + dqv
            t = p[lg, at, :] * dk[lg, at, :]
            j = acc["n"] % 4
            acc["s"][j] = t if acc["s"][j] is None else acc["s"][j] + t
            acc["n"] += 1
        each_pos(size, ig, first)
        dot_sum = (acc["s"][0] + acc["s"][1]) + (acc["s"][2] + acc["s"][3])

        def second(at, ok):
            dk[lg, at, :] = p[lg, at, :] * (dk[lg, at, :] - dot_sum)
        each_pos(size, ig, second)
        gsum[ds(8 * (8 + 8 * 0), 8), lane] += acc["r"]
        gsum[ds(8 * 4, 8), lane] += acc["q"]

        def load_grad(y):
            return [da[lg, cell(y, k, ig), :] for k in range(GRID)]

        def load_src(y):
            return [jnp.where(inside_at(size, y, k), v[lg, cell(y, k, ig), :], 0.0) for k in range(GRID)]

        def emit_tap(a, b, val):
            at = ds(8 * (TAPS + (a + 3) * 7 + b + 3), 8)
            gsum[at, lane] += val
        conv_kgrad(load_grad, load_src, radius, emit_tap)
        vs = [dv[lg, ds(8 * ig, 8), :]]

        def emit(y, out):
            for k in range(GRID):
                at = cell(y, k, ig)
                val = dv[lg, at, :] + jnp.where(inside_at(size, y, k), out[k], 0.0)
                dv[lg, at, :] = val
                vs[0] = vs[0] + val
        conv_pass(load_grad, lambda a, b: row8(tab, TAPS + (a + 3) * 7 + b + 3, lg), radius, emit, flip=True)
        gsum[ds(8 * 5, 8), lane] += vs[0]
    for_groups(body)

    def cast(i, c):
        at = pl.ds(pl.multiple_of(i * 32, 16), 32)
        for j, ref in enumerate((dq, dk, dv)):
            for g in range(4):
                dj[at, 512 * j + 128 * g:512 * j + 128 * g + 128] = ref[g, at, :].astype(BF16)
        return c
    lax.fori_loop(0, 41, cast, 0)


def bwd_conv1(x, dx1, dx, sz, tab, gsum):
    def body(i, c):
        lg, ig = i // 2, i % 2
        lane = lane_of(lg)
        size = sz[ds(8 * ig, 8), :]
        cls = ds(8 * ig, 8)
        dx[cls, lane] = dx1[cls, lane]

        def load_grad(y):
            return [jnp.where(inside_at(size, y, k), dx1[cell(y, k, ig), lane], 0.0) for k in range(GRID)]

        def load_src(y):
            return [jnp.where(inside_at(size, y, k), x[cell(y, k, ig), lane].astype(F32), 0.0) for k in range(GRID)]

        def emit_tap(a, b, val):
            at = ds(8 * (CPE + (a + 1) * 3 + b + 1), 8)
            gsum[at, lane] += val
        conv_kgrad(load_grad, load_src, 1, emit_tap)
        bias = [jnp.zeros((8, 128), F32)]

        def emit(y, out):
            for k in range(GRID):
                at = cell(y, k, ig)
                g = dx1[at, lane]
                ok = inside_at(size, y, k)
                bias[0] = bias[0] + jnp.where(ok, g, 0.0)
                dx[at, lane] = g + jnp.where(ok, out[k], 0.0)
        conv_pass(load_grad, lambda a, b: row8(tab, CPE + (a + 1) * 3 + b + 1, lg), 1, emit, flip=True)
        gsum[ds(8 * CPEB, 8), lane] += bias[0]
        return c
    lax.fori_loop(0, 8, body, 0)


def col_sum(src, gsum, row):
    def body(i, c):
        at = pl.ds(pl.multiple_of(i * 32, 16), 32)
        add_rows(gsum, row, src[at, :].astype(F32))
        return c
    lax.fori_loop(0, 41, body, 0)


def bwd_e_kernel(dx3, tab, w, a_low, n2, inv2, h2, g, slope,
                 dx2, da, gw1, gw2, gproj, gsum, gb1, dm, up):
    gsum[...] = jnp.zeros_like(gsum)
    dx2[...] = dx3[...]
    bwd_du(dx2, w, slope, dm, gb1)
    col_sum(dm, gsum, 7)
    wgrad(g, dm, gw2)
    wgrad(h2, slope, gw1)
    mm_nt(slope, w, 4, 4, up)
    norm_back_phase(up, n2, inv2, tab, 2, dx2, dm, gsum, 2, 3, None)
    col_sum(dm, gsum, 6)
    wgrad(a_low, dm, gproj)
    mm_nt(dm, w, 3, 1, da, True)
    da[:, R:RP, :] = jnp.zeros((4, RP - R, 128), F32)


def bwd_f_kernel(x, sz, tab, w, n1, inv1, h1, q, p, v, s, rel, dx2, da, gsum_in,
                 dx, gqkv, gsum, dq, dk, dv, dj, up):
    gsum[...] = gsum_in[...]
    bwd_attn1(q, p, v, s, da, dq, dv, dk)
    bwd_mix(q, p, v, rel, da, dq, dv, dk, dj, sz, tab, gsum, None)
    wgrad(h1, dj, gqkv)
    mm_nt(dj, w, 0, 3, up)
    norm_back_phase(up, n1, inv1, tab, 0, dx2, None, gsum, 0, 1, None)
    bwd_conv1(x, dx2, dx, sz, tab, gsum)


def bwd_layer(dx3, x, sz, tab, w, res):
    sd = jax.ShapeDtypeStruct
    r = dict(zip([n for n, _, _ in RES], res))
    dx2, da, gw1, gw2, gproj, gsum, gb1 = pl.pallas_call(
        bwd_e_kernel,
        out_shape=[sd((R, D), F32), sd((4, RP, 128), F32), sd((D, FF), BF16), sd((FF, D), BF16), sd((D, D), BF16), sd((8 * TROWS, D), F32), sd((8, FF), F32)],
        in_specs=vspec(9), out_specs=vspec(7),
        scratch_shapes=[pltpu.VMEM((R, D), BF16), pltpu.VMEM((R, D), F32)],
        compiler_params=PARAMS, name="block_bwd_e",
    )(dx3, tab, w, r["a"], r["n2"], r["inv2"], r["h2"], r["g"], r["slope"])
    dx, gqkv, gsum = pl.pallas_call(
        bwd_f_kernel,
        out_shape=[sd((R, D), F32), sd((D, 3 * D), BF16), sd((8 * TROWS, D), F32)],
        in_specs=vspec(15), out_specs=vspec(3),
        scratch_shapes=[pltpu.VMEM((4, RP, 128), F32)] * 3 + [pltpu.VMEM((R, 3 * D), BF16), pltpu.VMEM((R, D), F32)],
        compiler_params=PARAMS, name="block_bwd_f",
    )(x, sz, tab, w, r["n1"], r["inv1"], r["h1"], r["q"], r["p"], r["v"], r["s"], r["rel"], dx2, da, gsum)
    return dx, gqkv, gproj, gw1, gw2, gsum, gb1


def window_mask():
    channel = lax.broadcasted_iota(jnp.int32, (49, D), 1)
    tap = lax.broadcasted_iota(jnp.int32, (49, D), 0)
    head = channel // (D // HEADS)
    reach = jnp.where(head < 2, 1, jnp.where(head < 5, 2, 3))
    return ((jnp.abs(tap // 7 - 3) <= reach) & (jnp.abs(tap % 7 - 3) <= reach)).astype(F32)


def blocks_of(flat, rows, cols):
    return flat.reshape(rows, cols // D, D).transpose(1, 0, 2).reshape(rows * cols // D, D)


def pack(qkv, proj, fc1, fc2, n):
    per = D // n
    return jnp.concatenate([blocks_of(qkv, per, 3 * D), proj.reshape(per, D), blocks_of(fc1, per, FF), fc2.reshape(FF // n, D)])


def whole_weights(packed, small, n):
    per = D // n
    full = lax.all_gather(packed[None], AXES, axis=0, tiled=True)
    vec = lax.all_gather(small, AXES, axis=0, tiled=True)
    parts = [full[:, j * per:(j + 1) * per].reshape(32, D // 32, D) for j in range(8)] + [full[:, 8 * per:].reshape(32, FF // 32, D)]
    w = jnp.concatenate(parts, axis=1).reshape(4, 2, 2, 2, WROWS, D).transpose(3, 0, 1, 2, 4, 5)
    return w, *tables(vec)


def pack_grads(gqkv, gproj, gw1, gw2, small, n):
    per = D // n
    width = small.shape[0] // n
    pad = -width % D
    cols = [gqkv[:, j * D:(j + 1) * D] for j in range(3)] + [gproj] + [gw1[:, j * D:(j + 1) * D] for j in range(4)]
    parts = [c.reshape(n, per, D) for c in cols] + [gw2.reshape(n, FF // n, D)]
    parts.append(jnp.pad(small.reshape(n, width), ((0, 0), (0, pad))).reshape(n, -1, D).astype(BF16))
    return jnp.concatenate(parts, axis=1)


def split_grads(shard, n, width):
    per = D // n

    def cols(first, count):
        return shard[first * per:(first + count) * per].reshape(count, per, D).transpose(1, 0, 2).reshape(-1)
    fc2 = shard[8 * per:8 * per + FF // n].reshape(-1)
    small = shard[8 * per + FF // n:].reshape(-1)[:width]
    return cols(0, 3), cols(3, 1), cols(4, 4), fc2, small


def tables(small):
    small = small.astype(F32)
    end = TABLE * D
    tb = small[:end].reshape(D, TABLE).T
    cpe = small[end + FF:].reshape(D, 10).T
    tab = jnp.concatenate([tb[:9], tb[9:] * window_mask(), jnp.zeros((CPE - TABLE, D), F32), cpe, jnp.zeros((TROWS - CPE - 10, D), F32)])
    return tab.reshape(TROWS, 4, 128).transpose(1, 0, 2), small[end:end + FF].reshape(16, 128)


def small_grads(gsum, gb1):
    s = gsum.reshape(TROWS, 8, D).sum(1)
    tb = jnp.concatenate([s[:9], s[9:58] * window_mask()]).T
    return jnp.concatenate([tb.reshape(-1), gb1.sum(0), s[CPE:CPE + 10].T.reshape(-1)])


def to_rows(a):
    return jnp.transpose(a, (1, 0, 2)).reshape(R, D)


def from_rows(a):
    return jnp.transpose(a.reshape(SLOT, NI, D), (1, 0, 2))


def shards(n, images, grid_sizes, qkv, proj, fc1, fc2, small, cotangent):
    layers = qkv.shape[0]
    width = small.shape[1]
    packed = [pack(qkv[l], proj[l], fc1[l], fc2[l], n) for l in range(layers)]
    slot = lax.broadcasted_iota(jnp.int32, (SLOT, 1), 0)
    cellno = jnp.maximum(slot - 1, 0)
    far = jnp.maximum(cellno // GRID, cellno % GRID)
    present = ((slot == 0) | (far < grid_sizes[None, :]))[:, :, None]
    sz = jnp.broadcast_to(grid_sizes[:, None], (NI, 128))
    x = to_rows(images)
    saved = []
    if n == 32 and layers == 2:
        flat = jnp.pad(small.astype(F32).reshape(2, 9, 128), ((0, 0), (0, 7), (0, 0))).reshape(32, 128)
        out = fwd_first(4, x, sz, packed[0], packed[1], flat)
        count = 1 + len(RES)
        w0, w1, tab, b1 = out[count:]
        held = [(w0, tab[0], b1[0]), (w1, tab[1], b1[1])]
    else:
        held = [whole_weights(packed[l], small[l], n) for l in range(layers)]
        out = None
    for l in range(layers):
        w, tab, b1 = held[l]
        if l or out is None:
            out = fwd_layer(x, sz, tab, b1, w)
        saved.append((x, tab, w, out[1:1 + len(RES)]))
        x = out[0]
    output = from_rows(jnp.where(present, x.reshape(SLOT, NI, D), 0.0).astype(BF16))
    dx = jnp.where(present, jnp.transpose(cotangent, (1, 0, 2)), 0).astype(F32).reshape(R, D)
    shares = [None] * layers
    for l in reversed(range(layers)):
        xin, tab, w, res = saved[l]
        dx, gqkv, gproj, gw1, gw2, gsum, gb1 = bwd_layer(dx, xin, sz, tab, w, res)
        g = pack_grads(gqkv, gproj, gw1, gw2, small_grads(gsum, gb1), n)
        shares[l] = split_grads(lax.psum_scatter(g, AXES, scatter_dimension=0, tiled=True)[0].astype(F32), n, width)
    grads = [jnp.stack([shares[l][i] for l in range(layers)]) for i in range(5)]
    return (output, from_rows(dx), *grads)


def solution(mesh):
    n = mesh.shape["wide"] * mesh.shape["narrow"]
    from jax.sharding import PartitionSpec as P
    rows, flat = P(AXES, None, None), P(None, AXES)
    return jax.shard_map(
        functools.partial(shards, n), mesh=mesh,
        in_specs=(rows, P(AXES), flat, flat, flat, flat, flat, rows),
        out_specs=(rows, rows, flat, flat, flat, flat, flat),
        check_vma=False)
```

```python
import functools
import jax
import jax.numpy as jnp
from jax import lax
from jax.experimental import pallas as pl
from jax.experimental.pallas import tpu as pltpu

F32, BF16 = jnp.float32, jnp.bfloat16
D, FF, HEADS, GRID, SLOT = 512, 2048, 8, 9, 82
TABLE = 58
EPS = 1e-6
NI = 16
R = SLOT * NI
PADS = 96
RP = PADS * NI
RADII = (1, 2, 3, 3)
AXES = ("wide", "narrow")
WROWS = 192
TAPS, CPE, CPEB, TROWS = 9, 64, 73, 80


def ds(start, size, align=8):
    if not isinstance(start, int):
        start = pl.multiple_of(start, align)
    return pl.ds(start, size)


def row8(ref, i, lg):
    return ref[lg, pl.ds(i, 8, stride=0), :]


def row(tab, i, j=None):
    parts = range(4) if j is None else (2 * j, 2 * j + 1)
    return jnp.concatenate([tab[g, i:i + 1, :] for g in parts], axis=1)


def put2(ref, at, j, val):
    ref[2 * j, at, :] = val[:, :128]
    ref[2 * j + 1, at, :] = val[:, 128:]


def cell(y, x, ig):
    return ds((1 + GRID * y + x) * NI + 8 * ig, 8)


def inside_at(sz, y, x):
    return sz > max(y, x)


def conv_pass(load_row, load_tap, radius, emit, flip=False):
    span = 2 * radius + 1
    for y in range(GRID):
        acc = [None] * GRID
        for a in range(span):
            yy = y - (a - radius) if flip else y + a - radius
            if not 0 <= yy < GRID:
                continue
            row = load_row(yy)
            for b in range(span):
                tap = load_tap(a - radius, b - radius)
                for x in range(GRID):
                    xx = x - (b - radius) if flip else x + b - radius
                    if 0 <= xx < GRID:
                        term = row[xx] * tap
                        acc[x] = term if acc[x] is None else acc[x] + term
        emit(y, acc)


def conv_kgrad(load_grad, load_src, radius, emit):
    span = 2 * radius + 1
    for a in range(span):
        acc = [None] * span
        for y in range(GRID):
            yy = y + a - radius
            if not 0 <= yy < GRID:
                continue
            grad = load_grad(y)
            src = load_src(yy)
            for b in range(span):
                for x in range(GRID):
                    xx = x + b - radius
                    if 0 <= xx < GRID:
                        term = grad[x] * src[xx]
                        acc[b] = term if acc[b] is None else acc[b] + term
        for b in range(span):
            emit(a - radius, b - radius, acc[b])


def lane_of(lg):
    return ds(lg * 128, 128, 128)


def for_groups(body):
    def one(radius, base):
        def run(i, c):
            body(radius, base + i // 2, i % 2)
            return c
        return run
    lax.fori_loop(0, 2, one(1, 0), 0)
    lax.fori_loop(0, 2, one(2, 1), 0)
    lax.fori_loop(0, 4, one(3, 2), 0)


def norm_rows(x):
    mean = jnp.mean(x, axis=-1, keepdims=True)
    cen = x - mean
    inv = lax.rsqrt(jnp.mean(cen * cen, axis=-1, keepdims=True) + EPS)
    return cen * inv, inv


def normal_cdf(u):
    a = jnp.abs(u)
    t = 1.0 / (1.0 + a * (0.3275911 * 0.7071067811865476))
    e = jnp.exp(-0.5 * u * u)
    poly = t * (0.5 * 0.254829592 + t * (0.5 * -0.284496736 + t * (0.5 * 1.421413741 + t * (0.5 * -1.453152027 + t * (0.5 * 1.061405429)))))
    tail = poly * e
    return jnp.where(u >= 0, 1.0 - tail, tail), e


LN_T = 112
ROW_T = 336


def tile_start(i, size):
    return pl.multiple_of(jnp.minimum(i * size, R - size), 16)


def head_mask():
    r = lax.broadcasted_iota(jnp.int32, (256, 256), 0) // 64
    c = lax.broadcasted_iota(jnp.int32, (256, 256), 1) // 64
    return r == c


def dot(a, b, ca, cb):
    return lax.dot_general(a, b, (((ca,), (cb,)), ((), ())), preferred_element_type=F32)


def fwd_conv1(x, sz, tab, x1):
    def body(i, c):
        lg, ig = i // 2, i % 2
        lane = lane_of(lg)
        size = sz[ds(8 * ig, 8), :]
        cls = ds(8 * ig, 8)
        x1[cls, lane] = x[cls, lane].astype(F32)
        bias = row8(tab, CPEB, lg)

        def load_row(y):
            return [jnp.where(inside_at(size, y, k), x[cell(y, k, ig), lane].astype(F32), 0.0) for k in range(GRID)]

        def emit(y, acc):
            for k in range(GRID):
                at = cell(y, k, ig)
                x1[at, lane] = x[at, lane].astype(F32) + jnp.where(inside_at(size, y, k), acc[k] + bias, 0.0)

        conv_pass(load_row, lambda a, b: row8(tab, CPE + (a + 1) * 3 + b + 1, lg), 1, emit)
        return c
    lax.fori_loop(0, 8, body, 0)


def norm_phase(src, tab, gain, shift, hat, low, inv_ref):
    def body(i, c):
        at = pl.ds(tile_start(i, LN_T), LN_T)
        n, inv = norm_rows(src[at, :])
        hat[at, :] = n.astype(BF16)
        low[at, :] = (n * row(tab, gain) + row(tab, shift)).astype(BF16)
        inv_ref[at, :] = jnp.broadcast_to(inv, (LN_T, 128))
        return c
    lax.fori_loop(0, 12, body, 0)


def weight(g, block, first, count, cols):
    at = ds(16 * block, 16, 16)
    return jnp.concatenate([g[t % 2, t // 8, t // 4 % 2, t // 2 % 2, at, cols] for t in range(first // 16, (first + count) // 16)], axis=0)


def weight2(g, chunk, cols):
    return jnp.concatenate([g[i % 2, chunk // 2, chunk % 2, i // 2, 128:192, cols] for i in range(4)], axis=0)


def fwd_qkv(low, w, tab, q, k, v):
    def body(i, c):
        at = pl.ds(tile_start(i, ROW_T), ROW_T)
        h = low[at, :]
        for j in range(2):
            cols = slice(256 * j, 256 * j + 256)
            put2(q, at, j, dot(h, weight(w, 0, 0, D, cols), 1, 0) + row(tab, 4, j))
            put2(k, at, j, dot(h, weight(w, 1, 0, D, cols), 1, 0))
            put2(v, at, j, dot(h, weight(w, 2, 0, D, cols), 1, 0) + row(tab, 5, j))
        return c
    lax.fori_loop(0, 4, body, 0)
    tail = slice(R, RP)
    for ref in (q, k, v):
        ref[:, tail, :] = jnp.zeros((4, RP - R, 128), F32)


def each_pos(size, ig, fn):
    fn(ds(8 * ig, 8), None)
    for y in range(GRID):
        for x in range(GRID):
            fn(cell(y, x, ig), inside_at(size, y, x))


def fwd_softmax(k, sz):
    def body(i, c):
        lg, ig = i // 2, i % 2
        lane = lane_of(lg)
        size = sz[ds(8 * ig, 8), :]
        best = [None] * 4
        cnt = [0]

        def first(at, ok):
            val = k[lg, at, :]
            if ok is not None:
                val = jnp.where(ok, val, -1e30)
            j = cnt[0] % 4
            best[j] = val if best[j] is None else jnp.maximum(best[j], val)
            cnt[0] += 1
        each_pos(size, ig, first)
        top = jnp.maximum(jnp.maximum(best[0], best[1]), jnp.maximum(best[2], best[3]))
        total = [None] * 4
        cnt[0] = 0

        def second(at, ok):
            val = jnp.exp(k[lg, at, :] - top)
            if ok is not None:
                val = jnp.where(ok, val, 0.0)
            k[lg, at, :] = val
            j = cnt[0] % 4
            total[j] = val if total[j] is None else total[j] + val
            cnt[0] += 1
        each_pos(size, ig, second)
        scale = 1.0 / ((total[0] + total[1]) + (total[2] + total[3]))

        def third(at, ok):
            k[lg, at, :] = k[lg, at, :] * scale
        each_pos(size, ig, third)
        return c
    lax.fori_loop(0, 8, body, 0)


def img_load(ref, i, half):
    return jnp.concatenate([ref[2 * half + j, pl.ds(i, PADS, stride=NI), :] for j in range(2)], axis=1)


def img_store(ref, i, half, val):
    for j in range(2):
        ref[2 * half + j, pl.ds(i, PADS, stride=NI), :] = val[:, 128 * j:128 * j + 128]


def fwd_attn(q, p, v, s, f):
    def body(t, c):
        i, half = t // 2, t % 2
        pi = img_load(p, i, half).astype(BF16)
        vi = img_load(v, i, half).astype(BF16)
        summ = jnp.where(head_mask(), dot(pi, vi, 0, 0), 0.0).astype(BF16)
        s[t] = (summ[0:64] + summ[64:128]) + (summ[128:192] + summ[192:256])
        qi = img_load(q, i, half).astype(BF16)
        img_store(f, i, half, dot(qi, summ, 1, 0) * 0.125)
        return c
    lax.fori_loop(0, 2 * NI, body, 0)


def fwd_conv3(v, q, f, sz, tab, rel, att):
    def body(radius, lg, ig):
        lane = lane_of(lg)
        size = sz[ds(8 * ig, 8), :]
        bias = row8(tab, 8, lg)

        def load_row(y):
            return [jnp.where(inside_at(size, y, k), v[lg, cell(y, k, ig), :], 0.0) for k in range(GRID)]

        def emit(y, acc):
            for k in range(GRID):
                at = cell(y, k, ig)
                r = acc[k] + bias
                rel[lg, at, :] = r
                att[lg, at, :] = f[lg, at, :] + jnp.where(inside_at(size, y, k), q[lg, at, :] * r, 0.0)
        conv_pass(load_row, lambda a, b: row8(tab, TAPS + (a + 3) * 7 + b + 3, lg), radius, emit)
    for_groups(body)


def fwd_proj(att, w, tab, x1, a_low):
    def body(i, c):
        at = pl.ds(pl.multiple_of(i * 656, 16), 656)
        low = jnp.concatenate([att[g, at, :] for g in range(4)], axis=1).astype(BF16)
        a_low[at, :] = low
        for j in range(2):
            cols = slice(256 * j, 256 * j + 256)
            x1[at, cols] = x1[at, cols] + dot(low, weight(w, 3, 0, D, cols), 1, 0) + row(tab, 6, j)
        return c
    lax.fori_loop(0, 2, body, 0)


def fwd_fc1(low, w, b1, g, slope):
    def body(t, c):
        i, j = t // 8, t % 8
        at = pl.ds(tile_start(i, ROW_T), ROW_T)
        cols = pl.ds(pl.multiple_of(j * 256, 256), 256)
        half = pl.ds(pl.multiple_of(j % 2 * 256, 256), 256)
        bias = jnp.concatenate([b1[pl.ds(2 * j, 1), :], b1[pl.ds(2 * j + 1, 1), :]], axis=1)
        u = dot(low[at, :], weight(w, 4 + j // 2, 0, D, half), 1, 0) + bias
        cdf, e = normal_cdf(u)
        g[at, cols] = (u * cdf).astype(BF16)
        slope[at, cols] = (cdf + u * e * 0.3989422804014327).astype(BF16)
        return c
    lax.fori_loop(0, 32, body, 0)


def fwd_fc2(g, w, tab, x2, x3):
    def body(i, _):
        at = pl.ds(pl.multiple_of(i * 656, 16), 656)
        for j in range(2):
            cols = slice(256 * j, 256 * j + 256)
            x3[at, cols] = x2[at, cols] + dot(g[at, :], jnp.concatenate([weight2(w, c, cols) for c in range(8)], axis=0), 1, 0) + row(tab, 7, j)
        return _
    lax.fori_loop(0, 2, body, 0)


def fwd_phases(x, sz, tab, b1, w, x3, n1, inv1, h1, q, p, v, s, rel, a_low, n2, inv2, h2, g, slope, x1, f, tick, need):
    fwd_qkv(h1, w, tab, q, p, v)
    tick()
    fwd_softmax(p, sz)
    tick()
    fwd_attn(q, p, v, s, f)
    tick()
    fwd_conv3(v, q, f, sz, tab, rel, f)
    tick()
    fwd_proj(f, w, tab, x1, a_low)
    norm_phase(x1, tab, 2, 3, n2, h2, inv2)
    tick.upto(need)
    fwd_fc1(h2, w, b1, g, slope)
    tick()
    fwd_fc2(g, w, tab, x1, x3)


class Idle:
    def __call__(self):
        pass

    def upto(self, count):
        pass

    finish = __call__


RES = (
    ("n1", (R, D), BF16), ("inv1", (R, 128), F32), ("h1", (R, D), BF16),
    ("q", (4, RP, 128), F32), ("p", (4, RP, 128), F32), ("v", (4, RP, 128), F32),
    ("s", (2 * NI, 64, 256), BF16), ("rel", (4, R, 128), F32), ("a", (R, D), BF16),
    ("n2", (R, D), BF16), ("inv2", (R, 128), F32), ("h2", (R, D), BF16),
    ("g", (R, FF), BF16), ("slope", (R, FF), BF16))


def vspec(n):
    return [pl.BlockSpec(memory_space=pltpu.VMEM)] * n


PARAMS = pltpu.CompilerParams(vmem_limit_bytes=67043328)


MESH = pl.DeviceIdType.MESH


class Place:
    def __init__(self, line):
        w, m = lax.axis_index("wide"), lax.axis_index("narrow")
        self.line = line
        self.z, self.x, self.y, self.c = w // 2, w % 2, m // 2, m % 2

    def dev(self, z=None, x=None, y=None, c=None):
        z = self.z if z is None else z
        x = self.x if x is None else x
        y = self.y if y is None else y
        c = self.c if c is None else c
        return (z * 2 + x, y * 2 + c)

    def off(self, k):
        return lax.rem(self.z + self.line + k, self.line)


def greet(place):
    barrier = pltpu.get_barrier_semaphore()
    far = [place.dev(z=place.off(k)) for k in range(1, place.line)]
    near = [place.dev(x=1 - place.x), place.dev(y=1 - place.y), place.dev(c=1 - place.c)]
    for who in far + near:
        pl.semaphore_signal(barrier, inc=1, device_id=who, device_id_type=MESH)
    pl.semaphore_wait(barrier, place.line + 2)


def remote(src, dst, send, recv, dev):
    return pltpu.make_async_remote_copy(src_ref=src, dst_ref=dst, send_sem=send, recv_sem=recv, device_id=dev, device_id_type=MESH)


def both(copy):
    copy.wait_send()
    copy.wait_recv()


def by_core(place, a, b):
    def run():
        @pl.when(place.c == 0)
        def _():
            a()

        @pl.when(place.c == 1)
        def _():
            b()
    return run


def gather_ticks(place, g, rows, send, recv):
    n, z, x, y = place.line, place.z, place.x, place.y

    def lines():
        mine = g.at[place.c, z, x, y, rows]
        return [remote(mine, mine, send.at[k - 1], recv.at[k - 1], place.dev(z=place.off(k))) for k in range(1, n)]

    def line_waits():
        for k, cp in enumerate(lines()):
            cp.wait_send()
            got = g.at[place.c, place.off(-k - 1), x, y, rows]
            remote(got, got, send.at[k], recv.at[k], place.dev(z=place.off(1))).wait_recv()

    def parts(core):
        if core == 0:
            return (g.at[0, :, x, y, rows], g.at[0, :, x, :, rows]), (g.at[0, :, x, y, rows], g.at[0, :, x, 1 - y, rows], g.at[0, :, 1 - x, :, rows])
        return (g.at[1, :, x, y, rows], g.at[1, :, :, y, rows]), (g.at[1, :, x, y, rows], g.at[1, :, 1 - x, y, rows], g.at[1, :, :, 1 - y, rows])

    def swap(core, i):
        part = parts(core)[0][i]
        over_y = (core == 0) == (i == 0)
        return remote(part, part, send.at[n - 1 + i], recv.at[n - 1 + i], place.dev(y=1 - y) if over_y else place.dev(x=1 - x))

    def hand(core, i):
        part = parts(core)[1][i]
        return remote(part, part, send.at[n + 1 + i], recv.at[n + 1 + i], place.dev(c=1 - place.c))

    def steps(core):
        def last():
            for i in range(3):
                hand(core, i).wait_send()
                hand(1 - core, i).wait_recv()
        return [lambda: None,
                lambda: (swap(core, 0).start(), hand(core, 0).start()),
                lambda: (both(swap(core, 0)), swap(core, 1).start(), hand(core, 1).start()),
                lambda: (both(swap(core, 1)), hand(core, 2).start()),
                last]
    ticks = [by_core(place, a, b) for a, b in zip(steps(0), steps(1))]

    def first():
        for cp in lines():
            cp.start()

    def second():
        line_waits()
        ticks[1]()
    return [first, second] + ticks[2:]


def add_blocks(pairs):
    for dst, src in pairs:
        dst[...] = (dst[...].astype(F32) + src[...].astype(F32)).astype(dst.dtype)


def scatter_ticks(place, g, rows, cbuf, pbuf, sbuf, zbuf, out, send, recv):
    n, z, x, y, c = place.line, place.z, place.x, place.y, place.c

    def cores():
        return remote(g.at[1 - c, :, :, :, rows], cbuf, send.at[0], recv.at[0], place.dev(c=1 - c))

    def swaps(core):
        over_x, over_y = place.dev(x=1 - x), place.dev(y=1 - y)
        if core == 0:
            return (remote(g.at[0, :, 1 - x, :, rows], pbuf, send.at[1], recv.at[1], over_x),
                    remote(g.at[0, :, x, 1 - y, rows], sbuf, send.at[2], recv.at[2], over_y))
        return (remote(g.at[1, :, :, 1 - y, rows], pbuf, send.at[1], recv.at[1], over_y),
                remote(g.at[1, :, 1 - x, y, rows], sbuf, send.at[2], recv.at[2], over_x))

    def lines():
        return [remote(g.at[c, place.off(k), x, y, rows], zbuf.at[k - 1], send.at[2 + k], recv.at[2 + k], place.dev(z=place.off(k))) for k in range(1, n)]

    def start_cores():
        cores().start()

    def add_cores():
        both(cores())

        def body(t, carry):
            add_blocks([(g.at[c, t // 4, t // 2 % 2, t % 2, rows], cbuf.at[t // 4, t // 2 % 2, t % 2])])
            return carry
        lax.fori_loop(0, 4 * n, body, 0)

    def step1(core):
        def run():
            add_cores()
            swaps(core)[0].start()
        return run

    def step2(core):
        def run():
            both(swaps(core)[0])

            def body(t, carry):
                dst = g.at[0, t // 2, x, t % 2, rows] if core == 0 else g.at[1, t // 2, t % 2, y, rows]
                add_blocks([(dst, pbuf.at[t // 2, t % 2])])
                return carry
            lax.fori_loop(0, 2 * n, body, 0)
            swaps(core)[1].start()
        return run

    def step3(core):
        def run():
            both(swaps(core)[1])

            def body(t, carry):
                add_blocks([(g.at[core, t, x, y, rows], sbuf.at[t])])
                return carry
            lax.fori_loop(0, n, body, 0)
            for cp in lines():
                cp.start()
        return run

    def finish():
        for cp in lines():
            both(cp)
        total = g[c, z, x, y, rows].astype(F32)
        for k in range(n - 1):
            total = total + zbuf[k].astype(F32)
        out[...] = total
    return [start_cores] + [by_core(place, s(0), s(1)) for s in (step1, step2, step3)] + [finish]


def scatter_bufs(line, rows, width, dtype):
    return [pltpu.VMEM(shape + (rows, width), dtype) for shape in ((line, 2, 2), (line, 2), (line,), (line - 1,))]


class Ticker:
    def __init__(self, lists):
        depth = max(i + len(t) for i, t in lists)
        self.rounds = [[t[r - i] for i, t in lists if 0 <= r - i < len(t)] for r in range(depth)]
        self.done = 0

    def upto(self, count):
        while self.done < min(count, len(self.rounds)):
            for t in self.rounds[self.done]:
                t()
            self.done += 1

    def __call__(self):
        self.upto(self.done + 1)

    def finish(self):
        self.upto(len(self.rounds))


def build_tables(gs, layer, tau, y, tab, b1):
    for t in range(32):
        tau[9 * t:9 * t + 9, :] = gs[t % 2, t // 8, t // 4 % 2, t // 2 % 2, 16 * layer:16 * layer + 9, :]
    lane = lax.broadcasted_iota(jnp.int32, (8, 128), 1)

    def run(base, step, width, b):
        first, off = width * b // 128, width * b % 128
        val = tau[pl.ds(base + first, 8, stride=step), :]
        if off:
            val = pltpu.roll(val, 128 - off, 1)
            if off + width > 128:
                more = pltpu.roll(tau[pl.ds(base + first + 1, 8, stride=step), :], 128 - off, 1)
                val = jnp.where(lane < 128 - off, val, more)
        return val
    for b in range(64):
        tb = run(0, 29, TABLE, b)
        cpe = pltpu.roll(run(248, 5, 10, b), 64, 1)
        y[8 * b:8 * b + 8, :] = jnp.where(lane < TABLE, tb, jnp.where((lane >= 64) & (lane < 74), cpe, 0.0))
    r = lax.broadcasted_iota(jnp.int32, (D, D), 0)
    c = lax.broadcasted_iota(jnp.int32, (D, D), 1)
    place = jnp.where(c == 64 * (r % 8) + r // 8, 1.0, 0.0).astype(BF16)
    table = dot(y[...].astype(BF16), place, 0, 0)[:TROWS]
    tap = lax.broadcasted_iota(jnp.int32, (TROWS, D), 0) - TAPS
    head = lax.broadcasted_iota(jnp.int32, (TROWS, D), 1) // 64
    reach = jnp.where(head < 2, 1, jnp.where(head < 5, 2, 3))
    ok = (tap < 0) | (tap >= 49) | ((jnp.abs(tap // 7 - 3) <= reach) & (jnp.abs(tap % 7 - 3) <= reach))
    table = jnp.where(ok, table, 0.0)
    for g in range(4):
        tab[layer, g] = table[:, 128 * g:128 * g + 128]
    b1[layer] = tau[232:248, :]


FIRST = ((0, 64), (64, 128), (128, 192))
SECOND = ((64, 128), (128, 192))


def sem_rows(line, count):
    return pltpu.SemaphoreType.DMA((count, line + 4))


def put_own(pairs, sems):
    copies = [pltpu.make_async_copy(src, dst, sems.at[i]) for i, (src, dst) in enumerate(pairs)]
    for cp in copies:
        cp.start()
    return copies


def first_kernel(line, x, sz, shard0, shard1, small,
                 x3, n1, inv1, h1, q, p, v, s, rel, a_low, n2, inv2, h2, g, slope, w0, w1, tab, b1,
                 x1, f, gs, tau, y, own, send, recv):
    place = Place(line)
    here = (place.c, place.z, place.x, place.y)
    puts = put_own(((shard0, w0.at[here]), (shard1.at[0:64], w1.at[here]), (small, gs.at[here])), own)
    greet(place)
    for cp in puts:
        cp.wait()
    tiny = Ticker([(0, gather_ticks(place, gs, slice(None), send.at[0], recv.at[0]))])
    lists = [(i, gather_ticks(place, w0, pl.ds(a, b - a), send.at[1 + i], recv.at[1 + i])) for i, (a, b) in enumerate(FIRST)]
    lists.append((3, gather_ticks(place, w1, slice(None), send.at[4], recv.at[4])))
    tick = Ticker(lists)
    tiny()
    tick()
    tiny()
    tiny()
    tick()
    tiny()
    tiny()
    build_tables(gs, 0, tau, y, tab, b1)
    tick()
    fwd_conv1(x, sz, tab.at[0], x1)
    tick()
    norm_phase(x1, tab.at[0], 0, 1, n1, h1, inv1)
    build_tables(gs, 1, tau, y, tab, b1)
    tick.upto(5)
    fwd_phases(x, sz, tab.at[0], b1.at[0], w0, x3, n1, inv1, h1, q, p, v, s, rel, a_low, n2, inv2, h2, g, slope, x1, f, tick, 7)
    tick.finish()


def second_kernel(line, x, sz, tab, b1, w_in, shard,
                  x3, n1, inv1, h1, q, p, v, s, rel, a_low, n2, inv2, h2, g, slope, w, x1, f, own, load, send, recv):
    place = Place(line)
    here = (place.c, place.z, place.x, place.y)
    got = pltpu.make_async_copy(w_in, w.at[:, :, :, :, 0:64], load)
    got.start()
    puts = put_own(((shard.at[64:WROWS], w.at[here + (pl.ds(64, 128),)]),), own)
    greet(place)
    for cp in puts:
        cp.wait()
    tick = Ticker([(i, gather_ticks(place, w, pl.ds(a, b - a), send.at[i], recv.at[i])) for i, (a, b) in enumerate(SECOND)])
    tick()
    fwd_conv1(x, sz, tab, x1)
    tick()
    norm_phase(x1, tab, 0, 1, n1, h1, inv1)
    got.wait()
    fwd_phases(x, sz, tab, b1, w, x3, n1, inv1, h1, q, p, v, s, rel, a_low, n2, inv2, h2, g, slope, x1, f, tick, 6)


def fwd_kernel(x, sz, tab, b1, w, x3, n1, inv1, h1, q, p, v, s, rel, a_low, n2, inv2, h2, g, slope, x1, f):
    fwd_conv1(x, sz, tab, x1)
    norm_phase(x1, tab, 0, 1, n1, h1, inv1)
    fwd_phases(x, sz, tab, b1, w, x3, n1, inv1, h1, q, p, v, s, rel, a_low, n2, inv2, h2, g, slope, x1, f, Idle(), 0)


def sd(shape, dtype):
    return jax.ShapeDtypeStruct(shape, dtype)


def comm_params(cid):
    return pltpu.CompilerParams(vmem_limit_bytes=67043328, collective_id=cid, has_side_effects=True)


def packed(line, rows, width=D, dtype=BF16):
    return sd((2, line, 2, 2, rows, width), dtype)


ANY = pl.BlockSpec(memory_space=pl.ANY)


def fwd_outs():
    return [sd((R, D), F32)] + [sd(sh, dt) for _, sh, dt in RES]


FWD_SCRATCH = [pltpu.VMEM((R, D), F32), pltpu.VMEM((4, RP, 128), F32)]


def fwd_first(line, x, sz, shard0, shard1, small):
    outs = fwd_outs() + [packed(line, WROWS), packed(line, 64), sd((2, 4, TROWS, 128), F32), sd((2, 16, 128), F32)]
    return pl.pallas_call(
        functools.partial(first_kernel, line), out_shape=outs, in_specs=vspec(5), out_specs=vspec(len(outs)),
        scratch_shapes=FWD_SCRATCH + [pltpu.VMEM((2, line, 2, 2, 32, 128), F32), pltpu.VMEM((288, 128), F32), pltpu.VMEM((D, 128), F32),
                                      pltpu.SemaphoreType.DMA((3,)), sem_rows(line, 5), sem_rows(line, 5)],
        compiler_params=comm_params(0), name="first_fwd",
    )(x, sz, shard0, shard1, small)


def fwd_second(line, x, sz, tab, b1, w_in, shard):
    outs = fwd_outs() + [packed(line, WROWS)]
    return pl.pallas_call(
        functools.partial(second_kernel, line), out_shape=outs, in_specs=vspec(4) + [ANY] + vspec(1), out_specs=vspec(len(outs)),
        scratch_shapes=FWD_SCRATCH + [pltpu.SemaphoreType.DMA((1,)), pltpu.SemaphoreType.DMA, sem_rows(line, 2), sem_rows(line, 2)],
        compiler_params=comm_params(1), name="second_fwd",
    )(x, sz, tab, b1, w_in, shard)


def fwd_layer(x, sz, tab, b1, w):
    outs = fwd_outs()
    return pl.pallas_call(
        fwd_kernel, out_shape=outs, in_specs=vspec(5), out_specs=vspec(len(outs)),
        scratch_shapes=FWD_SCRATCH, compiler_params=PARAMS, name="block_fwd",
    )(x, sz, tab, b1, w)


def add_rows(ref, row, val):
    total = val[0:8]
    for i in range(1, val.shape[0] // 8):
        total = total + val[8 * i:8 * i + 8]
    for g in range(4):
        ref[g, 8 * row:8 * row + 8, :] += total[:, 128 * g:128 * g + 128]


def bwd_du(dx, w2, slope, dm, gb1):
    def cast(i, c):
        at = pl.ds(pl.multiple_of(i * 32, 16), 32)
        dm[at, :] = dx[at, :].astype(BF16)
        return c
    lax.fori_loop(0, 41, cast, 0)

    def body(t, c):
        i, j = t // 8, t % 8
        at = pl.ds(pl.multiple_of(i * 656, 16), 656)
        cols = pl.ds(pl.multiple_of(j * 256, 256), 256)
        d = dot(dm[at, :], weight2(w2, j, slice(None)), 1, 1) * slope[at, cols].astype(F32)
        slope[at, cols] = d.astype(BF16)
        total = d[0:8]
        for k in range(1, 82):
            total = total + d[8 * k:8 * k + 8]
        keep = jnp.where(i == 0, 0.0, 1.0)
        gb1[:, cols] = gb1[:, cols] * keep + total
        return c
    gb1[...] = jnp.zeros_like(gb1)
    lax.fori_loop(0, 16, body, 0)


def norm_back_phase(up, hat, inv_ref, tab, gain, res, out, out_low, sums, rg, rs, split=False):
    def body(i, c):
        at = pl.ds(pl.multiple_of(i * 32, 16), 32)
        u = jnp.concatenate([up[g, at, :] for g in range(4)], axis=1) if split else up[at, :]
        n = hat[at, :].astype(F32)
        e = u * row(tab, gain)
        m1 = jnp.mean(e, axis=-1, keepdims=True)
        m2 = jnp.mean(e * n, axis=-1, keepdims=True)
        inv = inv_ref[at, 0:1]
        d = res[at, :] + inv * (e - m1 - n * m2)
        out[at, :] = d
        add_rows(sums, rg, u * n)
        add_rows(sums, rs, u)
        if out_low is not None:
            out_low[at, :] = d.astype(BF16)
        return c
    lax.fori_loop(0, 41, body, 0)


def mm_nt(a, g, first, blocks, out, split=False):
    def body(i, c):
        at = pl.ds(pl.multiple_of(i * 656, 16), 656)
        for j in range(2):
            w = jnp.concatenate([weight(g, first + b, 256 * j, 256, slice(None)) for b in range(blocks)], axis=1)
            val = dot(a[at, :], w, 1, 1)
            if split:
                put2(out, at, j, val)
            else:
                out[at, 256 * j:256 * j + 256] = val
        return c
    lax.fori_loop(0, 2, body, 0)


def wgrad(left, right, gr, first):
    for j in range(right.shape[1] // 512):
        tile = dot(left[...], right[:, 512 * j:512 * j + 512], 0, 0).astype(BF16)
        for t in range(32):
            gr[t % 2, t // 8, t // 4 % 2, t // 2 % 2, first + 16 * j:first + 16 * j + 16, :] = tile[16 * t:16 * t + 16]


def wgrad2(left, right, gr, first):
    for j in range(4):
        tile = dot(left[:, 512 * j:512 * j + 512], right[...], 0, 0).astype(BF16)
        for i in range(8):
            gr[i % 2, j, i // 4, i // 2 % 2, first:first + 64, :] = tile[64 * i:64 * i + 64]


def bwd_attn1(q, p, v, s, da, dq, dv, dk):
    def body(t, c):
        i, half = t // 2, t % 2
        df = (img_load(da, i, half) * 0.125).astype(BF16)
        wide = s[t]
        wide = jnp.where(head_mask(), jnp.concatenate([wide] * 4, axis=0), jnp.zeros((), BF16))
        qi = img_load(q, i, half).astype(BF16)
        dsum = jnp.where(head_mask(), dot(qi, df, 0, 0), 0.0).astype(BF16)
        img_store(dq, i, half, dot(df, wide, 1, 1))
        pi = img_load(p, i, half).astype(BF16)
        img_store(dv, i, half, dot(pi, dsum, 1, 0))
        vi = img_load(v, i, half).astype(BF16)
        img_store(dk, i, half, dot(vi, dsum, 1, 1))
        return c
    lax.fori_loop(0, 2 * NI, body, 0)


def bwd_mix(q, p, v, rel, da, dq, dv, dk, sz, tab, gsum):
    def body(radius, lg, ig):
        lane = lane_of(lg)
        size = sz[ds(8 * ig, 8), :]

        acc = {"r": None, "q": None, "s": [None] * 4, "n": 0}

        def first(at, ok):
            d = da[lg, at, :]
            qv = q[lg, at, :]
            if ok is None:
                dqv = dq[lg, at, :]
                da[lg, at, :] = jnp.zeros_like(d)
            else:
                d = jnp.where(ok, d, 0.0)
                dr = qv * d
                da[lg, at, :] = dr
                acc["r"] = dr if acc["r"] is None else acc["r"] + dr
                dqv = dq[lg, at, :] + rel[lg, at, :] * d
            dq[lg, at, :] = dqv
            acc["q"] = dqv if acc["q"] is None else acc["q"] + dqv
            t = p[lg, at, :] * dk[lg, at, :]
            j = acc["n"] % 4
            acc["s"][j] = t if acc["s"][j] is None else acc["s"][j] + t
            acc["n"] += 1
        each_pos(size, ig, first)
        dot_sum = (acc["s"][0] + acc["s"][1]) + (acc["s"][2] + acc["s"][3])

        def second(at, ok):
            dk[lg, at, :] = p[lg, at, :] * (dk[lg, at, :] - dot_sum)
        each_pos(size, ig, second)
        gsum[lg, 64:72, :] += acc["r"]
        gsum[lg, 32:40, :] += acc["q"]

        def load_grad(y):
            return [da[lg, cell(y, k, ig), :] for k in range(GRID)]

        def load_src(y):
            return [jnp.where(inside_at(size, y, k), v[lg, cell(y, k, ig), :], 0.0) for k in range(GRID)]

        def emit_tap(a, b, val):
            at = ds(8 * (TAPS + (a + 3) * 7 + b + 3), 8)
            gsum[lg, at, :] += val
        conv_kgrad(load_grad, load_src, radius, emit_tap)
        vs = [dv[lg, ds(8 * ig, 8), :]]

        def emit(y, out):
            for k in range(GRID):
                at = cell(y, k, ig)
                val = dv[lg, at, :] + jnp.where(inside_at(size, y, k), out[k], 0.0)
                dv[lg, at, :] = val
                vs[0] = vs[0] + val
        conv_pass(load_grad, lambda a, b: row8(tab, TAPS + (a + 3) * 7 + b + 3, lg), radius, emit, flip=True)
        gsum[lg, 40:48, :] += vs[0]
    return body


def bwd_cast(dq, dk, dv, dj):
    def cast(i, c):
        at = pl.ds(pl.multiple_of(i * 32, 16), 32)
        for j, ref in enumerate((dq, dk, dv)):
            for g in range(4):
                dj[at, 512 * j + 128 * g:512 * j + 128 * g + 128] = ref[g, at, :].astype(BF16)
        return c
    lax.fori_loop(0, 41, cast, 0)


def bwd_conv1(x, dx1, dx, sz, tab, gsum):
    def body(i, c):
        lg, ig = i // 2, i % 2
        lane = lane_of(lg)
        size = sz[ds(8 * ig, 8), :]
        cls = ds(8 * ig, 8)
        dx[cls, lane] = dx1[cls, lane]

        def load_grad(y):
            return [jnp.where(inside_at(size, y, k), dx1[cell(y, k, ig), lane], 0.0) for k in range(GRID)]

        def load_src(y):
            return [jnp.where(inside_at(size, y, k), x[cell(y, k, ig), lane].astype(F32), 0.0) for k in range(GRID)]

        def emit_tap(a, b, val):
            at = ds(8 * (CPE + (a + 1) * 3 + b + 1), 8)
            gsum[lg, at, :] += val
        conv_kgrad(load_grad, load_src, 1, emit_tap)
        bias = [jnp.zeros((8, 128), F32)]

        def emit(y, out):
            for k in range(GRID):
                at = cell(y, k, ig)
                g = dx1[at, lane]
                ok = inside_at(size, y, k)
                bias[0] = bias[0] + jnp.where(ok, g, 0.0)
                dx[at, lane] = g + jnp.where(ok, out[k], 0.0)
        conv_pass(load_grad, lambda a, b: row8(tab, CPE + (a + 1) * 3 + b + 1, lg), 1, emit, flip=True)
        gsum[lg, 8 * CPEB:8 * CPEB + 8, :] += bias[0]
        return c
    lax.fori_loop(0, 8, body, 0)


def col_sum(src, gsum, row):
    def body(i, c):
        at = pl.ds(pl.multiple_of(i * 32, 16), 32)
        add_rows(gsum, row, src[at, :].astype(F32))
        return c
    lax.fori_loop(0, 41, body, 0)


def build_small(gsum, gb1, y, tau, gsm):
    r = lax.broadcasted_iota(jnp.int32, (D, D), 0)
    c = lax.broadcasted_iota(jnp.int32, (D, D), 1)
    place = jnp.where(c == 64 * (r % 8) + r // 8, 1.0, 0.0).astype(BF16)
    table = jnp.concatenate([sum(gsum[g, pl.ds(i, TROWS, stride=8), :] for i in range(8)) for g in range(4)], axis=1)
    tap = lax.broadcasted_iota(jnp.int32, (TROWS, D), 0) - TAPS
    head = lax.broadcasted_iota(jnp.int32, (TROWS, D), 1) // 64
    reach = jnp.where(head < 2, 1, jnp.where(head < 5, 2, 3))
    ok = (tap < 0) | (tap >= 49) | ((jnp.abs(tap // 7 - 3) <= reach) & (jnp.abs(tap % 7 - 3) <= reach))
    table = jnp.where(ok, table, 0.0)
    table = jnp.concatenate([table, jnp.zeros((128 - TROWS, D), F32)])
    hi = table.astype(BF16)
    mid = (table - hi.astype(F32)).astype(BF16)
    y[...] = dot(place, hi, 1, 1) + dot(place, mid, 1, 1)
    lane = lax.broadcasted_iota(jnp.int32, (8, 128), 1)

    def lay(base, step, width, start):
        for j in range(step):
            out = None
            for b in range(128 * j // width, min(64, -(-128 * (j + 1) // width))):
                first = width * b - 128 * j
                val = y[8 * b:8 * b + 8, :]
                shift = (first - start) % 128
                if shift:
                    val = pltpu.roll(val, shift, 1)
                out = val if out is None else jnp.where(lane >= first, val, out)
            tau[pl.ds(base + j, 8, stride=step), :] = out
    lay(0, 29, TABLE, 0)
    lay(248, 5, 10, CPE)
    for i in range(16):
        tau[232 + i:233 + i, :] = jnp.sum(gb1[:, 128 * i:128 * i + 128], axis=0, keepdims=True)
    for t in range(32):
        gsm[t % 2, t // 8, t // 4 % 2, t // 2 % 2, 0:9, :] = tau[9 * t:9 * t + 9, :]
        gsm[t % 2, t // 8, t // 4 % 2, t // 2 % 2, 9:16, :] = jnp.zeros((7, 128), F32)


def e_phases(dx3, tab, w, a_low, n2, inv2, h2, g, slope_in, dx2, da, gfc, gsum, gb1, dm, up, slope, load, tick):
    got = pltpu.make_async_copy(slope_in, slope, load)
    got.start()
    gsum[...] = jnp.zeros_like(gsum)
    got.wait()
    bwd_du(dx3, w, slope, dm, gb1)
    col_sum(dm, gsum, 7)
    tick()
    wgrad2(g, dm, gfc, 80)
    tick()
    wgrad(h2, slope, gfc, 16)
    tick()
    mm_nt(slope, w, 4, 4, up)
    tick()
    norm_back_phase(up, n2, inv2, tab, 2, dx3, dx2, dm, gsum, 2, 3)
    col_sum(dm, gsum, 6)
    tick()
    wgrad(a_low, dm, gfc, 0)
    mm_nt(dm, w, 3, 1, da, True)
    da[:, R:RP, :] = jnp.zeros((4, RP - R, 128), F32)


def e_kernel(dx3, tab, w, a_low, n2, inv2, h2, g, slope_in, dx2, da, gfc, gsum, gb1, dm, up, slope, load):
    e_phases(dx3, tab, w, a_low, n2, inv2, h2, g, slope_in, dx2, da, gfc, gsum, gb1, dm, up, slope, load, Idle())


def e_kernel_comm(line, dx3, tab, w, a_low, n2, inv2, h2, g, slope_in, gq_in, gs_in, dx2, da, gfc, gsum, gb1, out_q, out_s,
                  dm, up, slope, load, gq, gs, loads, *rest):
    qb, sb, (send, recv) = rest[:4], rest[4:8], rest[8:]
    place = Place(line)
    copies = put_own(((gq_in, gq), (gs_in, gs)), loads)
    greet(place)
    for cp in copies:
        cp.wait()
    tick = Ticker([(0, scatter_ticks(place, gq, slice(None), *qb, out_q, send.at[0], recv.at[0])),
                   (0, scatter_ticks(place, gs, slice(None), *sb, out_s, send.at[1], recv.at[1]))])
    tick()
    e_phases(dx3, tab, w, a_low, n2, inv2, h2, g, slope_in, dx2, da, gfc, gsum, gb1, dm, up, slope, load, tick)
    tick.finish()


def f_phases(x, sz, tab, wq, n1, inv1, h1, q, p, v, s, rel, dx2, da, gsum, dx, gq, dq, dk, dv, dj, dx1, tick):
    bwd_attn1(q, p, v, s, da, dq, dv, dk)
    tick()
    body = bwd_mix(q, p, v, rel, da, dq, dv, dk, sz, tab, gsum)
    for radius, base, count in ((1, 0, 2), (2, 1, 2), (3, 2, 2), (3, 3, 2)):
        def run(i, c, radius=radius, base=base):
            body(radius, base, i)
            return c
        lax.fori_loop(0, count, run, 0)
        tick()
    bwd_cast(dq, dk, dv, dj)
    wgrad(h1, dj, gq, 0)
    tick()
    mm_nt(dj, wq, 0, 3, dq, True)
    norm_back_phase(dq, n1, inv1, tab, 0, dx2, dx1, None, gsum, 0, 1, True)
    tick()
    bwd_conv1(x, dx1, dx, sz, tab, gsum)


def f_kernel(x, sz, tab, wq, n1, inv1, h1, q, p, v, s, rel, dx2, da_in, gsum_in, gb1, dx, gq, gsm, dq, dk, dv, dj, dx1, da, gsum, y, tau, loads):
    copies = put_own(((da_in, da), (gsum_in, gsum)), loads)
    for cp in copies:
        cp.wait()
    f_phases(x, sz, tab, wq, n1, inv1, h1, q, p, v, s, rel, dx2, da, gsum, dx, gq, dq, dk, dv, dj, dx1, Idle())
    build_small(gsum, gb1, y, tau, gsm)


GFC = ((0, 80), (80, 144))


def f_kernel_comm(line, last, x, sz, tab, w_in, n1, inv1, h1, q, p, v, s, rel, dx2, da_in, gsum_in, gb1, gfc_in, *refs):
    refs = list(refs)
    if last:
        dx, out_fc, out_q, out_s = refs[:4]
        refs = refs[4:]
        gq, gsm = refs.pop(), refs.pop()
    else:
        dx, out_fc, gq, gsm = refs[:4]
        refs = refs[4:]
    dq, dk, dv, dj, dx1, da, gsum, y, tau, wq, gfc, loads, send, recv = refs[:14]
    bufs = refs[14:]
    place = Place(line)
    copies = put_own(((gfc_in, gfc), (da_in, da), (gsum_in, gsum), (w_in.at[:, :, :, :, 0:48], wq)), loads)
    greet(place)
    for cp in copies:
        cp.wait()
    lists = []
    for i, (a, b) in enumerate(GFC):
        lists.append((i, scatter_ticks(place, gfc, pl.ds(a, b - a), *bufs[4 * i:4 * i + 4], out_fc.at[pl.ds(a, b - a)], send.at[i], recv.at[i])))
    tick = Ticker(lists)
    tick()
    if not last:
        f_phases(x, sz, tab, wq, n1, inv1, h1, q, p, v, s, rel, dx2, da, gsum, dx, gq, dq, dk, dv, dj, dx1, tick)
        tick.finish()
        build_small(gsum, gb1, y, tau, gsm)
        return
    end = Ticker([(0, scatter_ticks(place, gq, slice(None), *bufs[8:12], out_q, send.at[2], recv.at[2]))])

    class Steps(Idle):
        calls = 0

        def __call__(self):
            Steps.calls += 1
            if Steps.calls < 6:
                tick()
            else:
                tick.finish()
                end()
    f_phases(x, sz, tab, wq, n1, inv1, h1, q, p, v, s, rel, dx2, da, gsum, dx, gq, dq, dk, dv, dj, dx1, Steps())
    end()
    build_small(gsum, gb1, y, tau, gsm)
    fin = Ticker([(0, scatter_ticks(place, gsm, slice(None), *bufs[12:16], out_s, send.at[3], recv.at[3]))])
    fin()
    end.finish()
    fin.finish()


E_OUTS = [sd((R, D), F32), sd((4, RP, 128), F32), packed(4, 144), sd((4, 8 * TROWS, 128), F32), sd((8, FF), F32)]
E_SCRATCH = [pltpu.VMEM((R, D), BF16), pltpu.VMEM((R, D), F32), pltpu.VMEM((R, FF), BF16), pltpu.SemaphoreType.DMA]
F_SCRATCH = [pltpu.VMEM((4, RP, 128), F32)] * 3 + [pltpu.VMEM((R, 3 * D), BF16), pltpu.VMEM((R, D), F32), pltpu.VMEM((4, RP, 128), F32),
             pltpu.VMEM((4, 8 * TROWS, 128), F32), pltpu.VMEM((D, 128), F32), pltpu.VMEM((288, 128), F32)]


def bwd_e(dx3, tab, w, res):
    r = dict(zip([n for n, _, _ in RES], res))
    return pl.pallas_call(
        e_kernel, out_shape=E_OUTS, in_specs=vspec(8) + [ANY], out_specs=vspec(5), scratch_shapes=E_SCRATCH, compiler_params=PARAMS, name="block_bwd_e",
    )(dx3, tab, w, r["a"], r["n2"], r["inv2"], r["h2"], r["g"], r["slope"])


def bwd_e_comm(line, cid, dx3, tab, w, res, gq, gs):
    r = dict(zip([n for n, _, _ in RES], res))
    return pl.pallas_call(
        functools.partial(e_kernel_comm, line), out_shape=E_OUTS + [sd((48, D), F32), sd((16, 128), F32)],
        in_specs=vspec(8) + [ANY] * 3, out_specs=vspec(7),
        scratch_shapes=E_SCRATCH + [pltpu.VMEM((2, line, 2, 2, 48, D), BF16), pltpu.VMEM((2, line, 2, 2, 16, 128), F32), pltpu.SemaphoreType.DMA((2,))]
        + scatter_bufs(line, 48, D, BF16) + scatter_bufs(line, 16, 128, F32) + [sem_rows(line, 2)] * 2,
        compiler_params=comm_params(cid), name="comm_bwd_e",
    )(dx3, tab, w, r["a"], r["n2"], r["inv2"], r["h2"], r["g"], r["slope"], gq, gs)


def f_args(r, x, sz, tab, w, dx2, da, gsum, gb1):
    return (x, sz, tab, w, r["n1"], r["inv1"], r["h1"], r["q"], r["p"], r["v"], r["s"], r["rel"], dx2, da, gsum, gb1)


def bwd_f(x, sz, tab, w, res, dx2, da, gsum, gb1):
    r = dict(zip([n for n, _, _ in RES], res))
    return pl.pallas_call(
        f_kernel, out_shape=[sd((R, D), F32), packed(4, 48), packed(4, 16, 128, F32)],
        in_specs=vspec(13) + [ANY] * 2 + vspec(1), out_specs=vspec(3),
        scratch_shapes=F_SCRATCH + [pltpu.SemaphoreType.DMA((2,))], compiler_params=PARAMS, name="block_bwd_f",
    )(*f_args(r, x, sz, tab, w[:, :, :, :, 0:48], dx2, da, gsum, gb1))


def bwd_f_comm(line, cid, last, x, sz, tab, w, res, dx2, da, gsum, gb1, gfc):
    r = dict(zip([n for n, _, _ in RES], res))
    grads = [pltpu.VMEM((2, line, 2, 2, 16, 128), F32), pltpu.VMEM((2, line, 2, 2, 48, D), BF16)]
    outs = [sd((R, D), F32), sd((144, D), F32)]
    outs += [sd((48, D), F32), sd((16, 128), F32)] if last else [packed(line, 48), packed(line, 16, 128, F32)]
    scratch = F_SCRATCH + [pltpu.VMEM((2, line, 2, 2, 48, D), BF16), pltpu.VMEM((2, line, 2, 2, 144, D), BF16), pltpu.SemaphoreType.DMA((4,)),
                           sem_rows(line, 4), sem_rows(line, 4)]
    for a, b in GFC:
        scratch += scatter_bufs(line, b - a, D, BF16)
    if last:
        scratch += scatter_bufs(line, 48, D, BF16) + scatter_bufs(line, 16, 128, F32) + grads
    return pl.pallas_call(
        functools.partial(f_kernel_comm, line, last), out_shape=outs,
        in_specs=vspec(3) + [ANY] + vspec(9) + [ANY] * 2 + vspec(1) + [ANY], out_specs=vspec(4),
        scratch_shapes=scratch, compiler_params=comm_params(cid), name="last_bwd_f" if last else "comm_bwd_f",
    )(*f_args(r, x, sz, tab, w, dx2, da, gsum, gb1), gfc)


def window_mask():
    channel = lax.broadcasted_iota(jnp.int32, (49, D), 1)
    tap = lax.broadcasted_iota(jnp.int32, (49, D), 0)
    head = channel // (D // HEADS)
    reach = jnp.where(head < 2, 1, jnp.where(head < 5, 2, 3))
    return ((jnp.abs(tap // 7 - 3) <= reach) & (jnp.abs(tap % 7 - 3) <= reach)).astype(F32)


def blocks_of(flat, rows, cols):
    return flat.reshape(rows, cols // D, D).transpose(1, 0, 2).reshape(rows * cols // D, D)


def pack(qkv, proj, fc1, fc2, n):
    per = D // n
    return jnp.concatenate([blocks_of(qkv, per, 3 * D), proj.reshape(per, D), blocks_of(fc1, per, FF), fc2.reshape(FF // n, D)])


def whole_weights(packed, small, n):
    per = D // n
    full = lax.all_gather(packed[None], AXES, axis=0, tiled=True)
    vec = lax.all_gather(small, AXES, axis=0, tiled=True)
    parts = [full[:, j * per:(j + 1) * per].reshape(32, D // 32, D) for j in range(8)] + [full[:, 8 * per:].reshape(32, FF // 32, D)]
    w = jnp.concatenate(parts, axis=1).reshape(4, 2, 2, 2, WROWS, D).transpose(3, 0, 1, 2, 4, 5)
    return w, *tables(vec)


def share_by_xla(gfc, gq, gsm, n):
    per = D // n

    def rows(a):
        return a.transpose(1, 2, 3, 0, 4, 5).reshape((32,) + a.shape[4:])
    gq, gfc, gsm = rows(gq), rows(gfc), rows(gsm)
    every = jnp.concatenate([gq, gfc[:, :80]], axis=1)
    parts = [every[:, 16 * j:16 * j + 16].reshape(n, per, D) for j in range(8)] + [gfc[:, 80:].reshape(n, FF // n, D)]
    vec = gsm[:, :9].reshape(n, -1)
    width = vec.shape[1]
    parts.append(jnp.pad(vec, ((0, 0), (0, -width % D))).reshape(n, -1, D).astype(BF16))
    share = lax.psum_scatter(jnp.concatenate(parts, axis=1), AXES, scatter_dimension=0, tiled=True)[0].astype(F32)
    mats = split_shares(share[:8 * per + FF // n], per)
    return (*mats, share[8 * per + FF // n:].reshape(-1)[:width])


def split_shares(share, per):
    def cols(first, count):
        return share[first * per:(first + count) * per].reshape(count, per, D).transpose(1, 0, 2).reshape(-1)
    return cols(0, 3), cols(3, 1), cols(4, 4), share[8 * per:].reshape(-1)


def tables(small):
    small = small.astype(F32)
    end = TABLE * D
    tb = small[:end].reshape(D, TABLE).T
    cpe = small[end + FF:].reshape(D, 10).T
    tab = jnp.concatenate([tb[:9], tb[9:] * window_mask(), jnp.zeros((CPE - TABLE, D), F32), cpe, jnp.zeros((TROWS - CPE - 10, D), F32)])
    return tab.reshape(TROWS, 4, 128).transpose(1, 0, 2), small[end:end + FF].reshape(16, 128)


def to_rows(a):
    return jnp.transpose(a, (1, 0, 2)).reshape(R, D)


def from_rows(a):
    return jnp.transpose(a.reshape(SLOT, NI, D), (1, 0, 2))


def shards(n, images, grid_sizes, qkv, proj, fc1, fc2, small, cotangent):
    layers = qkv.shape[0]
    width = small.shape[1]
    packed_w = [pack(qkv[l], proj[l], fc1[l], fc2[l], n) for l in range(layers)]
    slot = lax.broadcasted_iota(jnp.int32, (SLOT, 1), 0)
    cellno = jnp.maximum(slot - 1, 0)
    far = jnp.maximum(cellno // GRID, cellno % GRID)
    present = ((slot == 0) | (far < grid_sizes[None, :]))[:, :, None]
    sz = jnp.broadcast_to(grid_sizes[:, None], (NI, 128))
    x = to_rows(images)
    saved = []
    dy = jnp.where(present, jnp.transpose(cotangent, (1, 0, 2)), 0).astype(F32).reshape(R, D)
    count = 1 + len(RES)
    if n == 32 and layers == 2 and width == 1152:
        line = n // 8
        flat = jnp.pad(small.astype(F32).reshape(2, 9, 128), ((0, 0), (0, 7), (0, 0))).reshape(32, 128)
        out0 = fwd_first(line, x, sz, packed_w[0], packed_w[1], flat)
        w0, w1a, tab, b1 = out0[count:]
        x1, res0 = out0[0], out0[1:count]
        out1 = fwd_second(line, x1, sz, tab[1], b1[1], w1a, packed_w[1])
        last, res1, w1 = out1[0], out1[1:count], out1[count]
        dx2, da, gfc1, gsum, gb1 = bwd_e(dy, tab[1], w1, res1)
        dx, sfc1, gq1, gsm1 = bwd_f_comm(line, 2, False, x1, sz, tab[1], w1, res1, dx2, da, gsum, gb1, gfc1)
        dx2, da, gfc0, gsum, gb1, sq1, ss1 = bwd_e_comm(line, 3, dx, tab[0], w0, res0, gq1, gsm1)
        dx, sfc0, sq0, ss0 = bwd_f_comm(line, 4, True, x, sz, tab[0], w0, res0, dx2, da, gsum, gb1, gfc0)
        shares = [(*split_shares(jnp.concatenate([q, fc]), D // n), s[:9].reshape(-1)) for q, fc, s in ((sq0, sfc0, ss0), (sq1, sfc1, ss1))]
    else:
        held = [whole_weights(packed_w[l], small[l], n) for l in range(layers)]
        last = x
        for l in range(layers):
            w, tab, b1 = held[l]
            out = fwd_layer(last, sz, tab, b1, w)
            saved.append((last, tab, w, out[1:count]))
            last = out[0]
        shares = [None] * layers
        dx = dy
        for l in reversed(range(layers)):
            xin, tab, w, res = saved[l]
            dx2, da, gfc, gsum, gb1 = bwd_e(dx, tab, w, res)
            dx, gq, gsm = bwd_f(xin, sz, tab, w, res, dx2, da, gsum, gb1)
            shares[l] = share_by_xla(gfc, gq, gsm, n)
    output = from_rows(jnp.where(present, last.reshape(SLOT, NI, D), 0.0).astype(BF16))
    grads = [jnp.stack([shares[l][i] for l in range(layers)]) for i in range(5)]
    return (output, from_rows(dx), *grads)


def solution(mesh):
    n = mesh.shape["wide"] * mesh.shape["narrow"]
    from jax.sharding import PartitionSpec as P
    rows, flat = P(AXES, None, None), P(None, AXES)
    return jax.shard_map(
        functools.partial(shards, n), mesh=mesh,
        in_specs=(rows, P(AXES), flat, flat, flat, flat, flat, rows),
        out_specs=(rows, rows, flat, flat, flat, flat, flat),
        check_vma=False)
```

```python
import functools
import jax
import jax.numpy as jnp
from jax import lax
from jax.experimental import pallas as pl
from jax.experimental.pallas import tpu as pltpu

F32, BF16 = jnp.float32, jnp.bfloat16
D, FF, HEADS, GRID, SLOT = 512, 2048, 8, 9, 82
TABLE = 58
EPS = 1e-6
NI = 16
R = SLOT * NI
PADS = 96
RP = PADS * NI
RADII = (1, 2, 3, 3)
AXES = ("wide", "narrow")
WROWS = 192
TAPS, CPE, CPEB, TROWS = 9, 64, 73, 80


def ds(start, size, align=8):
    if not isinstance(start, int):
        start = pl.multiple_of(start, align)
    return pl.ds(start, size)


def row8(ref, i, lg):
    return ref[lg, pl.ds(i, 8, stride=0), :]


def row(tab, i, j=None):
    parts = range(4) if j is None else (2 * j, 2 * j + 1)
    return jnp.concatenate([tab[g, i:i + 1, :] for g in parts], axis=1)


def put2(ref, at, j, val):
    ref[2 * j, at, :] = val[:, :128]
    ref[2 * j + 1, at, :] = val[:, 128:]


def cell(y, x, ig):
    return ds((1 + GRID * y + x) * NI + 8 * ig, 8)


def inside_at(sz, y, x):
    return sz > max(y, x)


PROW = GRID * NI
PADDED = ((GRID + 6) * PROW, 128)


def at_cell(y, x, ig):
    return pl.ds(pl.multiple_of((1 + GRID * y + x) * NI + 8 * ig, 8), 8)


def at_padded(y, x, ig):
    return pl.ds(pl.multiple_of((y + 3) * PROW + x * NI + 8 * ig, 8), 8)


def rows_loop(fn, init):
    return lax.fori_loop(0, GRID, fn, init)


def groups(fn):
    def run(ig, c):
        fn(ig)
        return c
    lax.fori_loop(0, 2, run, 0)


def lane_groups(fn):
    fn(1, 0)
    fn(2, 1)

    def run(i, c):
        fn(3, i + 2)
        return c
    lax.fori_loop(0, 2, run, 0)


def conv_pass(src, load_tap, radius, ig, emit, init, flip=False):
    span = range(-radius, radius + 1)

    def body(y, carry):
        acc = [None] * GRID
        for a in span:
            line = [src[at_padded(y - a if flip else y + a, x, ig), :] for x in range(GRID)]
            for b in span:
                tap = load_tap(a, b)
                for x in range(GRID):
                    xx = x - b if flip else x + b
                    if 0 <= xx < GRID:
                        term = line[xx] * tap
                        acc[x] = term if acc[x] is None else acc[x] + term
        return emit(y, acc, carry)
    return rows_loop(body, init)


def conv_kgrad(grad, src, radius, emit):
    span = range(-radius, radius + 1)
    rows = list(span)
    for part in (rows[:4], rows[4:]):
        if not part:
            continue

        def body(t, acc):
            y, ig = t // 2, t % 2
            acc = list(acc)
            up = [grad[at_padded(y, x, ig), :] for x in range(GRID)]
            for i, a in enumerate(part):
                line = [src[at_padded(y + a, x, ig), :] for x in range(GRID)]
                for j, b in enumerate(span):
                    k = i * len(span) + j
                    for x in range(GRID):
                        if 0 <= x + b < GRID:
                            acc[k] = acc[k] + up[x] * line[x + b]
            return tuple(acc)
        zero = jnp.zeros((8, 128), F32)
        sums = lax.fori_loop(0, 2 * GRID, body, (zero,) * (len(part) * len(span)))
        for i, a in enumerate(part):
            for j, b in enumerate(span):
                emit(a, b, sums[i * len(span) + j])


def zero_padded(ref):
    ref[...] = jnp.zeros(PADDED, F32)


def fill_padded(dst, src, lg, sz):
    def body(t, c):
        y, ig = t // 2, t % 2
        size = sz[ds(8 * ig, 8), :]
        for x in range(GRID):
            dst[at_padded(y, x, ig), :] = jnp.where(size > jnp.maximum(y, x), src[lg, at_cell(y, x, ig), :], 0.0)
        return c
    lax.fori_loop(0, 2 * GRID, body, 0)


def norm_rows(x):
    mean = jnp.mean(x, axis=-1, keepdims=True)
    cen = x - mean
    inv = lax.rsqrt(jnp.mean(cen * cen, axis=-1, keepdims=True) + EPS)
    return cen * inv, inv


def dot(a, b, ca, cb):
    return lax.dot_general(a, b, (((ca,), (cb,)), ((), ())), preferred_element_type=F32)


def head_mask():
    r = lax.broadcasted_iota(jnp.int32, (256, 256), 0) // 64
    c = lax.broadcasted_iota(jnp.int32, (256, 256), 1) // 64
    return r == c


def by_tiles(fn):
    def body(i, c):
        fn(pl.ds(pl.multiple_of(i * 256, 256), 256))
        return c
    lax.fori_loop(0, R // 256, body, 0)
    if R % 256:
        fn(pl.ds(R // 256 * 256, R % 256))


def full(ref, at):
    return jnp.concatenate([ref[g, at, :] for g in range(4)], axis=1)


def spread(ref, at, val):
    for g in range(4):
        ref[g, at, :] = val[:, 128 * g:128 * g + 128]


def fwd_conv1(x, sz, tab, x1, pv):
    def one(lg, c):
        fill_padded(pv, x, lg, sz)

        def group(ig):
            size = sz[ds(8 * ig, 8), :]
            x1[lg, ds(8 * ig, 8), :] = x[lg, ds(8 * ig, 8), :]
            bias = row8(tab, CPEB, lg)

            def emit(y, acc, carry):
                for k in range(GRID):
                    at = at_cell(y, k, ig)
                    x1[lg, at, :] = x[lg, at, :] + jnp.where(size > jnp.maximum(y, k), acc[k] + bias, 0.0)
                return carry
            conv_pass(pv, lambda a, b: row8(tab, CPE + (a + 1) * 3 + b + 1, lg), 1, ig, emit, 0)
        groups(group)
        return c
    lax.fori_loop(0, 4, one, 0)


def norm_phase(src, tab, gain, shift, hat, low, inv_ref):
    def fn(at):
        n, inv = norm_rows(full(src, at))
        hat[at, :] = n.astype(BF16)
        low[at, :] = (n * row(tab, gain) + row(tab, shift)).astype(BF16)
        inv_ref[at, :] = jnp.broadcast_to(inv, (n.shape[0], 128))
    by_tiles(fn)


def weight(g, block, first, count, cols):
    at = ds(16 * block, 16, 16)
    return jnp.concatenate([g[t % 2, t // 8, t // 4 % 2, t // 2 % 2, at, cols] for t in range(first // 16, (first + count) // 16)], axis=0)


def weight2(g, chunk, cols):
    return jnp.concatenate([g[i % 2, chunk, i // 4, i // 2 % 2, 128:192, cols] for i in range(8)], axis=0)


def halves(fn):
    def body(i, c):
        fn(pl.ds(pl.multiple_of(i * (R // 2), 16), R // 2))
        return c
    lax.fori_loop(0, 2, body, 0)


def zero_tail(ref):
    ref[:, R:RP, :] = jnp.zeros((4, RP - R, 128), F32)


def fwd_qkv(low, w, tab, q, k, v):
    def fn(at):
        h = low[at, :]
        for b, (ref, bias) in enumerate(((q, 4), (k, None), (v, 5))):
            for j in range(2):
                val = dot(h, weight(w, b, 0, D, slice(256 * j, 256 * j + 256)), 1, 0)
                put2(ref, at, j, val if bias is None else val + row(tab, bias, j))
    halves(fn)
    for ref in (q, k, v):
        zero_tail(ref)


def each_pos(size, ig, fn):
    fn(ds(8 * ig, 8), None)
    for y in range(GRID):
        for x in range(GRID):
            fn(cell(y, x, ig), inside_at(size, y, x))


def fwd_softmax(k, sz):
    def body(i, c):
        lg, ig = i // 2, i % 2
        size = sz[ds(8 * ig, 8), :]
        best = [None] * 4
        cnt = [0]

        def first(at, ok):
            val = k[lg, at, :]
            if ok is not None:
                val = jnp.where(ok, val, -1e30)
            j = cnt[0] % 4
            best[j] = val if best[j] is None else jnp.maximum(best[j], val)
            cnt[0] += 1
        each_pos(size, ig, first)
        top = jnp.maximum(jnp.maximum(best[0], best[1]), jnp.maximum(best[2], best[3]))
        total = [None] * 4
        cnt[0] = 0

        def second(at, ok):
            val = jnp.exp(k[lg, at, :] - top)
            if ok is not None:
                val = jnp.where(ok, val, 0.0)
            k[lg, at, :] = val
            j = cnt[0] % 4
            total[j] = val if total[j] is None else total[j] + val
            cnt[0] += 1
        each_pos(size, ig, second)
        scale = 1.0 / ((total[0] + total[1]) + (total[2] + total[3]))

        def third(at, ok):
            k[lg, at, :] = k[lg, at, :] * scale
        each_pos(size, ig, third)
        return c
    lax.fori_loop(0, 8, body, 0)


def img_load(ref, i, half):
    return jnp.concatenate([ref[2 * half + j, pl.ds(i, PADS, stride=NI), :] for j in range(2)], axis=1)


def img_store(ref, i, half, val):
    for j in range(2):
        ref[2 * half + j, pl.ds(i, PADS, stride=NI), :] = val[:, 128 * j:128 * j + 128]


def fwd_attn(q, p, v, s, f, first, count):
    def body(t, c):
        i, half = t // 2, t % 2
        pi = img_load(p, i, half).astype(BF16)
        vi = img_load(v, i, half).astype(BF16)
        summ = jnp.where(head_mask(), dot(pi, vi, 0, 0), 0.0).astype(BF16)
        s[t] = (summ[0:64] + summ[64:128]) + (summ[128:192] + summ[192:256])
        qi = img_load(q, i, half).astype(BF16)
        img_store(f, i, half, dot(qi, summ, 1, 0) * 0.125)
        return c
    lax.fori_loop(0, count, lambda t, c: body(t + first, c), 0, unroll=8)


def fwd_conv3(v, q, f, sz, tab, rel, pv, radius, lg):
    fill_padded(pv, v, lg, sz)
    bias = row8(tab, 8, lg)

    def group(ig):
        size = sz[ds(8 * ig, 8), :]

        def emit(y, acc, carry):
            for k in range(GRID):
                at = at_cell(y, k, ig)
                r = acc[k] + bias
                rel[lg, at, :] = r
                f[lg, at, :] = f[lg, at, :] + jnp.where(size > jnp.maximum(y, k), q[lg, at, :] * r, 0.0)
            return carry
        conv_pass(pv, lambda a, b: row8(tab, TAPS + (a + 3) * 7 + b + 3, lg), radius, ig, emit, 0)
    groups(group)


def fwd_proj(att, w, tab, x1, a_low):
    def fn(at):
        low = full(att, at).astype(BF16)
        a_low[at, :] = low
        for j in range(2):
            res = jnp.concatenate([x1[2 * j, at, :], x1[2 * j + 1, at, :]], axis=1)
            put2(x1, at, j, res + dot(low, weight(w, 3, 0, D, slice(256 * j, 256 * j + 256)), 1, 0) + row(tab, 6, j))
    halves(fn)


def normal_cdf(u):
    t = 1.0 / (1.0 + jnp.abs(u) * (0.3275911 * 0.7071067811865476))
    e = jnp.exp(-0.5 * u * u)
    poly = t * (0.5 * 0.254829592 + t * (0.5 * -0.284496736 + t * (0.5 * 1.421413741 + t * (0.5 * -1.453152027 + t * (0.5 * 1.061405429)))))
    tail = poly * e
    return jnp.where(u >= 0, 1.0 - tail, tail), e


def fwd_fc1(low, w, b1, g, slope, first, count):
    def body(j, c):
        cols = pl.ds(pl.multiple_of(j * 512, 512), 512)
        bias = jnp.concatenate([b1[pl.ds(4 * j + i, 1), :] for i in range(4)], axis=1)
        u = dot(low[...], weight(w, 4 + j, 0, D, slice(None)), 1, 0) + bias
        cdf, e = normal_cdf(u)
        g[:, cols] = (u * cdf).astype(BF16)
        slope[:, cols] = (cdf + u * e * 0.3989422804014327).astype(BF16)
        return c
    lax.fori_loop(0, count, lambda j, c: body(j + first, c), 0)


def fwd_fc2(g, w, tab, x1):
    def fn(at):
        for j in range(2):
            cols = slice(256 * j, 256 * j + 256)
            res = jnp.concatenate([x1[2 * j, at, :], x1[2 * j + 1, at, :]], axis=1)
            put2(x1, at, j, res + dot(g[at, :], jnp.concatenate([weight2(w, c, cols) for c in range(4)], axis=0), 1, 0) + row(tab, 7, j))
    halves(fn)


def fold_rows(val):
    parts = [val[8 * i:8 * i + 8] for i in range(val.shape[0] // 8)]
    while len(parts) > 1:
        parts = [a + b for a, b in zip(parts[::2], parts[1::2])] + parts[len(parts) // 2 * 2:]
    return parts[0]


def add_rows(ref, row, val):
    total = jnp.sum(fold_rows(val), axis=0, keepdims=True)
    for g in range(4):
        ref[g, row:row + 1, :] += total[:, 128 * g:128 * g + 128]


def add_sum(ref, lg, row, val):
    ref[lg, row:row + 1, :] += jnp.sum(val, axis=0, keepdims=True)


def bwd_cast_sum(dx, low, gsum, row):
    def fn(at):
        val = full(dx, at).astype(BF16)
        low[at, :] = val
        add_rows(gsum, row, val.astype(F32))
    by_tiles(fn)


def bwd_du(dm, w, slope, gb1):
    def body(j, c):
        cols = pl.ds(pl.multiple_of(j * 512, 512), 512)
        d = dot(dm[...], weight2(w, j, slice(None)), 1, 1) * slope[:, cols].astype(F32)
        slope[:, cols] = d.astype(BF16)
        gb1[:, cols] = fold_rows(d)
        return c
    lax.fori_loop(0, 4, body, 0)


def norm_back_phase(up, hat, inv_ref, tab, gain, res, out_low, sums, rg, rs, rb):
    def fn(at):
        u = full(up, at)
        n = hat[at, :].astype(F32)
        e = u * row(tab, gain)
        m1 = jnp.mean(e, axis=-1, keepdims=True)
        m2 = jnp.mean(e * n, axis=-1, keepdims=True)
        d = full(res, at) + inv_ref[at, 0:1] * (e - m1 - n * m2)
        spread(res, at, d)
        add_rows(sums, rg, u * n)
        add_rows(sums, rs, u)
        if out_low is not None:
            low = d.astype(BF16)
            out_low[at, :] = low
            add_rows(sums, rb, low.astype(F32))
    by_tiles(fn)


def mm_nt(a, cols, g, first, blocks, out):
    def fn(at):
        for j in range(2):
            w = jnp.concatenate([weight(g, first + b, 256 * j, 256, slice(None)) for b in range(blocks)], axis=1)
            put2(out, at, j, dot(a[at, cols], w, 1, 1))
    halves(fn)


def wgrad(left, right, gr, first, blocks):
    for j in range(blocks):
        tile = dot(left[...], right[:, 512 * j:512 * j + 512], 0, 0).astype(BF16)
        for t in range(32):
            gr[t % 2, t // 8, t // 4 % 2, t // 2 % 2, first + 16 * j:first + 16 * j + 16, :] = tile[16 * t:16 * t + 16]


def wgrad2(left, right, gr, first):
    for j in range(4):
        tile = dot(left[:, 512 * j:512 * j + 512], right[...], 0, 0).astype(BF16)
        for i in range(8):
            gr[i % 2, j, i // 4, i // 2 % 2, first:first + 64, :] = tile[64 * i:64 * i + 64]


def bwd_attn1(q, p, v, s, da, dq, dv, dk, first, count):
    def body(t, c):
        i, half = t // 2, t % 2
        df = (img_load(da, i, half) * 0.125).astype(BF16)
        wide = s[t]
        wide = jnp.where(head_mask(), jnp.concatenate([wide] * 4, axis=0), jnp.zeros((), BF16))
        qi = img_load(q, i, half).astype(BF16)
        dsum = jnp.where(head_mask(), dot(qi, df, 0, 0), 0.0).astype(BF16)
        img_store(dq, i, half, dot(df, wide, 1, 1))
        pi = img_load(p, i, half).astype(BF16)
        img_store(dv, i, half, dot(pi, dsum, 1, 0))
        vi = img_load(v, i, half).astype(BF16)
        img_store(dk, i, half, dot(vi, dsum, 1, 1))
        return c
    lax.fori_loop(0, count, lambda t, c: body(t + first, c), 0, unroll=8)


def bwd_mix(q, p, v, rel, da, dq, dv, dk, sz, tab, gsum, pv, pr, radius, lg):
    fill_padded(pv, v, lg, sz)

    def group(ig):
        size = sz[ds(8 * ig, 8), :]
        cls = ds(8 * ig, 8)
        dqc = dq[lg, cls, :]

        def first(y, carry):
            rs, qs, ps = carry
            for x in range(GRID):
                at = at_cell(y, x, ig)
                d = jnp.where(size > jnp.maximum(y, x), da[lg, at, :], 0.0)
                dr = q[lg, at, :] * d
                pr[at_padded(y, x, ig), :] = dr
                dqv = dq[lg, at, :] + rel[lg, at, :] * d
                dq[lg, at, :] = dqv
                rs, qs, ps = rs + dr, qs + dqv, ps + p[lg, at, :] * dk[lg, at, :]
            return rs, qs, ps
        rs, qs, ps = rows_loop(first, (jnp.zeros((8, 128), F32), dqc, p[lg, cls, :] * dk[lg, cls, :]))
        add_sum(gsum, lg, 8, rs)
        add_sum(gsum, lg, 4, qs)
        dk[lg, cls, :] = p[lg, cls, :] * (dk[lg, cls, :] - ps)

        def second(y, carry):
            for x in range(GRID):
                at = at_cell(y, x, ig)
                dk[lg, at, :] = p[lg, at, :] * (dk[lg, at, :] - ps)
            return carry
        rows_loop(second, 0)

        def emit(y, acc, total):
            for x in range(GRID):
                at = at_cell(y, x, ig)
                val = dv[lg, at, :] + jnp.where(size > jnp.maximum(y, x), acc[x], 0.0)
                dv[lg, at, :] = val
                total = total + val
            return total
        add_sum(gsum, lg, 5, conv_pass(pr, lambda a, b: row8(tab, TAPS + (a + 3) * 7 + b + 3, lg), radius, ig, emit, dv[lg, cls, :], True))
    groups(group)

    def emit_tap(a, b, val):
        add_sum(gsum, lg, TAPS + (a + 3) * 7 + b + 3, val)
    conv_kgrad(pr, pv, radius, emit_tap)


def bwd_cast(dq, dk, dv, dj):
    def fn(at):
        for j, ref in enumerate((dq, dk, dv)):
            dj[at, 512 * j:512 * j + 512] = full(ref, at).astype(BF16)
    by_tiles(fn)


def bwd_conv1(x, dx1, dx, sz, tab, gsum, pv, pr):
    def one(lg, c):
        fill_padded(pv, x, lg, sz)
        fill_padded(pr, dx1, lg, sz)

        def group(ig):
            size = sz[ds(8 * ig, 8), :]
            cls = ds(8 * ig, 8)
            dx[lg, cls, :] = dx1[lg, cls, :]

            def emit(y, acc, total):
                for k in range(GRID):
                    at = at_cell(y, k, ig)
                    total = total + pr[at_padded(y, k, ig), :]
                    dx[lg, at, :] = dx1[lg, at, :] + jnp.where(size > jnp.maximum(y, k), acc[k], 0.0)
                return total
            add_sum(gsum, lg, CPEB, conv_pass(pr, lambda a, b: row8(tab, CPE + (a + 1) * 3 + b + 1, lg), 1, ig, emit, jnp.zeros((8, 128), F32), True))
        groups(group)

        def emit_tap(a, b, val):
            add_sum(gsum, lg, CPE + (a + 1) * 3 + b + 1, val)
        conv_kgrad(pr, pv, 1, emit_tap)
        return c
    lax.fori_loop(0, 4, one, 0)


MESH = pl.DeviceIdType.MESH


class Place:
    def __init__(self, line):
        w, m = lax.axis_index("wide"), lax.axis_index("narrow")
        self.line = line
        self.z, self.x, self.y, self.c = w // 2, w % 2, m // 2, m % 2

    def dev(self, z=None, x=None, y=None, c=None):
        z = self.z if z is None else z
        x = self.x if x is None else x
        y = self.y if y is None else y
        c = self.c if c is None else c
        return (z * 2 + x, y * 2 + c)

    def off(self, k):
        return lax.rem(self.z + self.line + k, self.line)


def greet(place):
    barrier = pltpu.get_barrier_semaphore()
    far = [place.dev(z=place.off(k)) for k in range(1, place.line)]
    near = [place.dev(x=1 - place.x), place.dev(y=1 - place.y), place.dev(c=1 - place.c)]
    for who in far + near:
        pl.semaphore_signal(barrier, inc=1, device_id=who, device_id_type=MESH)
    pl.semaphore_wait(barrier, place.line + 2)


def remote(src, dst, send, recv, dev):
    return pltpu.make_async_remote_copy(src_ref=src, dst_ref=dst, send_sem=send, recv_sem=recv, device_id=dev, device_id_type=MESH)


def both(copy):
    copy.wait_send()
    copy.wait_recv()


def by_core(place, a, b):
    def run():
        @pl.when(place.c == 0)
        def _():
            a()

        @pl.when(place.c == 1)
        def _():
            b()
    return run


def gather_ticks(place, g, rows, send, recv):
    n, z, x, y = place.line, place.z, place.x, place.y

    def lines():
        mine = g.at[place.c, z, x, y, rows]
        return [remote(mine, mine, send.at[k - 1], recv.at[k - 1], place.dev(z=place.off(k))) for k in range(1, n)]

    def line_waits():
        for k, cp in enumerate(lines()):
            cp.wait_send()
            got = g.at[place.c, place.off(-k - 1), x, y, rows]
            remote(got, got, send.at[k], recv.at[k], place.dev(z=place.off(1))).wait_recv()

    def parts(core):
        if core == 0:
            return (g.at[0, :, x, y, rows], g.at[0, :, x, :, rows]), (g.at[0, :, x, y, rows], g.at[0, :, x, 1 - y, rows], g.at[0, :, 1 - x, :, rows])
        return (g.at[1, :, x, y, rows], g.at[1, :, :, y, rows]), (g.at[1, :, x, y, rows], g.at[1, :, 1 - x, y, rows], g.at[1, :, :, 1 - y, rows])

    def swap(core, i):
        part = parts(core)[0][i]
        over_y = (core == 0) == (i == 0)
        return remote(part, part, send.at[n - 1 + i], recv.at[n - 1 + i], place.dev(y=1 - y) if over_y else place.dev(x=1 - x))

    def hand(core, i):
        part = parts(core)[1][i]
        return remote(part, part, send.at[n + 1 + i], recv.at[n + 1 + i], place.dev(c=1 - place.c))

    def steps(core):
        def last():
            for i in range(3):
                hand(core, i).wait_send()
                hand(1 - core, i).wait_recv()
        return [lambda: None,
                lambda: (swap(core, 0).start(), hand(core, 0).start()),
                lambda: (both(swap(core, 0)), swap(core, 1).start(), hand(core, 1).start()),
                lambda: (both(swap(core, 1)), hand(core, 2).start()),
                last]
    ticks = [by_core(place, a, b) for a, b in zip(steps(0), steps(1))]

    def first():
        for cp in lines():
            cp.start()

    def second():
        line_waits()
        ticks[1]()
    return [first, second] + ticks[2:]


def add_blocks(pairs):
    for dst, src in pairs:
        dst[...] = (dst[...].astype(F32) + src[...].astype(F32)).astype(dst.dtype)


def scatter_ticks(place, g, rows, cbuf, pbuf, sbuf, zbuf, out, send, recv):
    n, z, x, y, c = place.line, place.z, place.x, place.y, place.c

    def cores():
        return remote(g.at[1 - c, :, :, :, rows], cbuf, send.at[0], recv.at[0], place.dev(c=1 - c))

    def swaps(core):
        over_x, over_y = place.dev(x=1 - x), place.dev(y=1 - y)
        if core == 0:
            return (remote(g.at[0, :, 1 - x, :, rows], pbuf, send.at[1], recv.at[1], over_x),
                    remote(g.at[0, :, x, 1 - y, rows], sbuf, send.at[2], recv.at[2], over_y))
        return (remote(g.at[1, :, :, 1 - y, rows], pbuf, send.at[1], recv.at[1], over_y),
                remote(g.at[1, :, 1 - x, y, rows], sbuf, send.at[2], recv.at[2], over_x))

    def lines():
        return [remote(g.at[c, place.off(k), x, y, rows], zbuf.at[k - 1], send.at[2 + k], recv.at[2 + k], place.dev(z=place.off(k))) for k in range(1, n)]

    def start_cores():
        cores().start()

    def add_cores():
        both(cores())

        def body(t, carry):
            add_blocks([(g.at[c, t // 4, t // 2 % 2, t % 2, rows], cbuf.at[t // 4, t // 2 % 2, t % 2])])
            return carry
        lax.fori_loop(0, 4 * n, body, 0)

    def step1(core):
        def run():
            add_cores()
            swaps(core)[0].start()
        return run

    def step2(core):
        def run():
            both(swaps(core)[0])

            def body(t, carry):
                dst = g.at[0, t // 2, x, t % 2, rows] if core == 0 else g.at[1, t // 2, t % 2, y, rows]
                add_blocks([(dst, pbuf.at[t // 2, t % 2])])
                return carry
            lax.fori_loop(0, 2 * n, body, 0)
            swaps(core)[1].start()
        return run

    def step3(core):
        def run():
            both(swaps(core)[1])

            def body(t, carry):
                add_blocks([(g.at[core, t, x, y, rows], sbuf.at[t])])
                return carry
            lax.fori_loop(0, n, body, 0)
            for cp in lines():
                cp.start()
        return run

    def finish():
        for cp in lines():
            both(cp)
        total = g[c, z, x, y, rows].astype(F32)
        for k in range(n - 1):
            total = total + zbuf[k].astype(F32)
        out[...] = total
    return [start_cores] + [by_core(place, s(0), s(1)) for s in (step1, step2, step3)] + [finish]


def scatter_bufs(line, rows, width, dtype):
    return [pltpu.VMEM(shape + (rows, width), dtype) for shape in ((line, 2, 2), (line, 2), (line,), (line - 1,))]


STEPS = 5


class Ticker:
    def __init__(self, lists):
        depth = max(i for i, _ in lists) + STEPS
        self.rounds = [[(lambda make=make, at=r - i: make()[at]()) for i, make in lists if 0 <= r - i < STEPS] for r in range(depth)]
        self.done = 0

    def upto(self, count):
        while self.done < min(count, len(self.rounds)):
            for t in self.rounds[self.done]:
                t()
            self.done += 1

    def __call__(self):
        self.upto(self.done + 1)

    def finish(self):
        self.upto(len(self.rounds))


def build_tables(gs, layer, tau, y, tab, b1):
    for t in range(32):
        tau[9 * t:9 * t + 9, :] = gs[t % 2, t // 8, t // 4 % 2, t // 2 % 2, 16 * layer:16 * layer + 9, :]
    lane = lax.broadcasted_iota(jnp.int32, (8, 128), 1)

    def run(base, step, width, b):
        first, off = width * b // 128, width * b % 128
        val = tau[pl.ds(base + first, 8, stride=step), :]
        if off:
            val = pltpu.roll(val, 128 - off, 1)
            if off + width > 128:
                more = pltpu.roll(tau[pl.ds(base + first + 1, 8, stride=step), :], 128 - off, 1)
                val = jnp.where(lane < 128 - off, val, more)
        return val
    for b in range(64):
        tb = run(0, 29, TABLE, b)
        cpe = pltpu.roll(run(248, 5, 10, b), 64, 1)
        y[8 * b:8 * b + 8, :] = jnp.where(lane < TABLE, tb, jnp.where((lane >= 64) & (lane < 74), cpe, 0.0))
    r = lax.broadcasted_iota(jnp.int32, (D, D), 0)
    c = lax.broadcasted_iota(jnp.int32, (D, D), 1)
    place = jnp.where(c == 64 * (r % 8) + r // 8, 1.0, 0.0).astype(BF16)
    table = dot(y[...].astype(BF16), place, 0, 0)[:TROWS]
    tap = lax.broadcasted_iota(jnp.int32, (TROWS, D), 0) - TAPS
    head = lax.broadcasted_iota(jnp.int32, (TROWS, D), 1) // 64
    reach = jnp.where(head < 2, 1, jnp.where(head < 5, 2, 3))
    ok = (tap < 0) | (tap >= 49) | ((jnp.abs(tap // 7 - 3) <= reach) & (jnp.abs(tap % 7 - 3) <= reach))
    table = jnp.where(ok, table, 0.0)
    for g in range(4):
        tab[layer, g] = table[:, 128 * g:128 * g + 128]
    b1[layer] = tau[232:248, :]


def build_small(gsum, gb1, y, tau, gsm):
    r = lax.broadcasted_iota(jnp.int32, (D, D), 0)
    c = lax.broadcasted_iota(jnp.int32, (D, D), 1)
    place = jnp.where(c == 64 * (r % 8) + r // 8, 1.0, 0.0).astype(BF16)
    table = full(gsum, slice(None))
    tap = lax.broadcasted_iota(jnp.int32, (TROWS, D), 0) - TAPS
    head = lax.broadcasted_iota(jnp.int32, (TROWS, D), 1) // 64
    reach = jnp.where(head < 2, 1, jnp.where(head < 5, 2, 3))
    ok = (tap < 0) | (tap >= 49) | ((jnp.abs(tap // 7 - 3) <= reach) & (jnp.abs(tap % 7 - 3) <= reach))
    table = jnp.where(ok, table, 0.0)
    table = jnp.concatenate([table, jnp.zeros((128 - TROWS, D), F32)])
    hi = table.astype(BF16)
    mid = (table - hi.astype(F32)).astype(BF16)
    y[...] = dot(place, hi, 1, 1) + dot(place, mid, 1, 1)
    lane = lax.broadcasted_iota(jnp.int32, (8, 128), 1)

    def lay(base, step, width, start):
        for j in range(step):
            out = None
            for b in range(128 * j // width, min(64, -(-128 * (j + 1) // width))):
                first = width * b - 128 * j
                val = y[8 * b:8 * b + 8, :]
                shift = (first - start) % 128
                if shift:
                    val = pltpu.roll(val, shift, 1)
                out = val if out is None else jnp.where(lane >= first, val, out)
            tau[pl.ds(base + j, 8, stride=step), :] = out
    lay(0, 29, TABLE, 0)
    lay(248, 5, 10, CPE)
    for i in range(16):
        tau[232 + i:233 + i, :] = jnp.sum(gb1[:, 128 * i:128 * i + 128], axis=0, keepdims=True)
    for t in range(32):
        gsm[t % 2, t // 8, t // 4 % 2, t // 2 % 2, 0:9, :] = tau[9 * t:9 * t + 9, :]
        gsm[t % 2, t // 8, t // 4 % 2, t // 2 % 2, 9:16, :] = jnp.zeros((7, 128), F32)


def sd(shape, dtype):
    return jax.ShapeDtypeStruct(shape, dtype)


def packed(rows, width=D, dtype=BF16):
    return sd((2, 4, 2, 2, rows, width), dtype)


ANY = pl.BlockSpec(memory_space=pl.ANY)
VM = pl.BlockSpec(memory_space=pltpu.VMEM)
L4 = ((4, RP, 128), F32)
WIDE = ((R, FF), BF16)
LOW = ((R, D), BF16)
INV = ((R, 128), F32)
SUMM = ((2 * NI, 64, 256), BF16)
REL = ((4, R, 128), F32)
PARK = (("q", L4), ("p", L4), ("v", L4), ("rel", REL), ("s", SUMM))
PARK0 = PARK + (("n1", LOW), ("h1", LOW), ("inv1", INV), ("a", LOW), ("n2", LOW), ("h2", LOW), ("inv2", INV), ("g", WIDE), ("slope", WIDE))
GATHERS = ((0, 64), (64, 128), (128, 192))
PIECES = ((0, 48), (48, 64), (64, 128), (128, 192))
SCATTERS = ((0, 80), (80, 144))


def cell_reach():
    cell_no = lax.broadcasted_iota(jnp.int32, (SLOT, 128), 0) - 1
    y = jnp.zeros((SLOT, 128), jnp.int32)
    for k in range(1, GRID):
        y = y + jnp.where(cell_no >= GRID * k, 1, 0)
    return jnp.where(cell_no < 0, -1, jnp.maximum(y, cell_no - GRID * y))


def take_images(src, dst, sz=None):
    reach = cell_reach() if sz is not None else None

    def body(i, c):
        for g in range(4):
            val = src[i, :, 128 * g:128 * g + 128].astype(F32)
            if sz is not None:
                val = jnp.where(reach < sz[pl.ds(i, 1), :], val, 0.0)
            dst[g, pl.ds(i, SLOT, stride=NI), :] = val
        return c
    lax.fori_loop(0, NI, body, 0)


def give_images(src, dst, sz=None):
    reach = cell_reach() if sz is not None else None

    def body(i, c):
        for g in range(4):
            val = src[g, pl.ds(i, SLOT, stride=NI), :]
            if sz is not None:
                val = jnp.where(reach < sz[pl.ds(i, 1), :], val, 0.0)
            dst[i, :, 128 * g:128 * g + 128] = val.astype(dst.dtype)
        return c
    lax.fori_loop(0, NI, body, 0)


class Copies:
    def __init__(self, sems):
        self.sems, self.used, self.open = sems, 0, {}

    def start(self, name, src, dst):
        at = self.used
        self.used += 1
        self.open[name] = lambda: pltpu.make_async_copy(src, dst, self.sems.at[at])
        self.open[name]().start()

    def wait(self, *names):
        for name in names:
            self.open.pop(name)().wait()

    def wait_all(self, prefix):
        for name in [n for n in self.open if n.startswith(prefix)]:
            self.wait(name)


class Idle:
    def __call__(self):
        pass

    def upto(self, count):
        pass

    def finish(self):
        pass


COPIES = 80
ROWS6 = (slice(None),) * 4


def step_kernel(comm, names, *refs):
    r = dict(zip(names, refs))
    cps = Copies(r["copy_sems"])
    sz, W, tab, b1 = r["sz"], r["W"], r["tab"], r["b1"]
    gsum, gb1, gfc, gq, gsm, tau = r["gsum"], r["gb1"], r["gfc"], r["gq"], r["gsm"], r["tau"]
    whbm = (r["w0"], r["w1"])
    n1, h1, inv1, a_low = r["n1"], r["h1"], r["inv1"], r["a"]
    xa, xb, da, dxb = r["xa"], r["xb"], r["da"], r["dxb"]
    pv, pr = r["pv"], r["pr"]
    y = pv.at[pl.ds(3 * PROW, D)]
    zero_padded(pv)
    zero_padded(pr)
    scope = pl.run_scoped

    def vm(*shapes):
        return [pltpu.VMEM(*sh) for sh in shapes]

    def load_piece(layer, i):
        a, b = PIECES[i]
        cps.start(f"W{i}", whbm[layer].at[ROWS6 + (pl.ds(a, b - a),)], W.at[ROWS6 + (pl.ds(a, b - a),)])

    STAGE = pltpu.VMEM((NI, SLOT, D), BF16)

    if comm:
        place = Place(4)
        here = (place.c, place.z, place.x, place.y)
        cps.start("own0", r["shard0"], r["w0"].at[here])
        cps.start("own1", r["shard1"], r["w1"].at[here])
        cps.start("own2", r["small"], r["gs"].at[here])
        greet(place)
        cps.wait("own2")
        send, recv = r["ag_send"], r["ag_recv"]
        tiny = Ticker([(0, lambda: gather_ticks(Place(4), r["gs"], slice(None), send.at[0], recv.at[0]))])
        lists = []
        for layer in range(2):
            for i, (a, b) in enumerate(GATHERS):
                n = 3 * layer + i
                lists.append((n, lambda n=n, layer=layer, a=a, b=b: gather_ticks(Place(4), whbm[layer], pl.ds(a, b - a), send.at[1 + n], recv.at[1 + n])))
        tick = Ticker(lists)
        tiny()
        cps.wait("own0", "own1")
        tick()
        tiny()

        def begin(stage):
            cps.start("images", r["images"], stage)
            cps.wait("images")
            take_images(stage, xa)
        scope(begin, STAGE)
        tiny()
        tick()
        tiny()
        tiny()
        build_tables(r["gs"], 0, tau, y, tab, b1)
        tick()
    else:
        tick = Idle()

        def begin(stage):
            cps.start("images", r["images"], stage)
            cps.wait("images")
            take_images(stage, xa)
        scope(begin, STAGE)

    def forward(layer, xin, x1, keep):
        t = tab.at[layer]
        fwd_conv1(xin, sz, t, x1, pv)
        tick()
        norm_phase(x1, t, 0, 1, n1, h1, inv1)
        if layer == 0:
            if comm:
                build_tables(r["gs"], 1, tau, y, tab, b1)
            tick.upto(5)
            load_piece(0, 0)
            load_piece(0, 1)
            for name in ("n1", "h1", "inv1"):
                cps.start("out0" + name, r[name], r["park0" + name])
        cps.wait("W0")

        def attention(q, p, v, rel, f, s):
            def park(name, ref):
                cps.start(f"park{layer}{name}", ref, r[f"park{layer}{name}"])
            fwd_qkv(h1, W, t, q, p, v)
            if layer == 0:
                tick.upto(8)
                load_piece(1, 0)
            else:
                tick()
            park("q", q)
            park("v", v)
            fwd_softmax(p, sz)
            park("p", p)
            tick()
            fwd_attn(q, p, v, s, f, 0, 16)
            tick()
            fwd_attn(q, p, v, s, f, 16, 16)
            park("s", s)
            tick()
            fwd_conv3(v, q, f, sz, t, rel, pv, 1, 0)
            fwd_conv3(v, q, f, sz, t, rel, pv, 2, 1)
            tick()

            def wide(i, c):
                fwd_conv3(v, q, f, sz, t, rel, pv, 3, i)
                return c
            lax.fori_loop(0, 2, lambda i, c: wide(i + 2, c), 0)
            tick()
            park("rel", rel)
            cps.wait("W1")
            fwd_proj(f, W, t, x1, a_low)
            cps.wait_all(f"park{layer}")
        scope(attention, *vm(L4, L4, L4, REL, L4, SUMM))
        if layer == 0:
            cps.start("out0a", a_low, r["park0a"])

        def mlp(g, slope, n2, h2, inv2, dm):
            norm_phase(x1, t, 2, 3, n2, h2, inv2)
            if layer == 0:
                tick.upto(6)
                load_piece(0, 2)
                tick.upto(7)
                load_piece(0, 3)
            else:
                tick.upto(9)
                load_piece(1, 2)
                tick.finish()
                load_piece(1, 3)
            cps.wait("W2")
            fwd_fc1(h2, W, b1.at[layer], g, slope, 0, 2)
            tick()
            fwd_fc1(h2, W, b1.at[layer], g, slope, 2, 2)
            if layer == 0:
                for name, ref in (("g", g), ("slope", slope), ("n2", n2), ("h2", h2), ("inv2", inv2)):
                    cps.start("out0" + name, ref, r["park0" + name])
            cps.wait("W3")
            fwd_fc2(g, W, t, x1)
            if layer == 0:
                tick()
                load_piece(1, 1)
                cps.wait_all("out0")
            else:
                keep(g, slope, n2, h2, inv2, dm)
        scope(mlp, *vm(WIDE, WIDE, LOW, LOW, INV, LOW))

    def first_half(layer, dx, da, g, slope, n2, h2, inv2, dm, tick):
        t = tab.at[layer]
        gsum[...] = jnp.zeros_like(gsum)
        bwd_cast_sum(dx, dm, gsum, 7)
        if layer == 0:
            cps.wait("in0slope", "W3")
        bwd_du(dm, W, slope, gb1)
        tick()
        if layer == 0:
            cps.wait("in0g")
        wgrad2(g, dm, gfc, 80)
        tick()
        if layer == 0:
            cps.wait("in0h2", "W2")
        wgrad(h2, slope, gfc, 16, 4)
        tick()
        mm_nt(slope, slice(None), W, 4, 4, da)
        if layer == 0:
            cps.wait("in0n2", "in0inv2", "in0a", "W1")
        norm_back_phase(da, n2, inv2, t, 2, dx, dm, gsum, 2, 3, 6)
        tick()
        wgrad(a_low, dm, gfc, 0, 1)
        mm_nt(dm, slice(None), W, 3, 1, da)
        zero_tail(da)
        tick()

    def second_half(layer, xin, dx, da, dv, tick, mid, end):
        t = tab.at[layer]

        def run(q, p, v, rel, dq, dk, s, dj):
            for name, ref in (("q", q), ("p", p), ("v", v), ("s", s), ("rel", rel)):
                cps.start(f"in{layer}" + name, r[f"park{layer}{name}"], ref)
            tick()
            cps.wait(*(f"in{layer}" + n for n in ("q", "p", "v", "s")))
            bwd_attn1(q, p, v, s, da, dq, dv, dk, 0, 16)
            tick()
            bwd_attn1(q, p, v, s, da, dq, dv, dk, 16, 16)
            tick()
            cps.wait(f"in{layer}rel")
            bwd_mix(q, p, v, rel, da, dq, dv, dk, sz, t, gsum, pv, pr, 1, 0)
            tick()
            bwd_mix(q, p, v, rel, da, dq, dv, dk, sz, t, gsum, pv, pr, 2, 1)
            tick()

            def wide(i, c):
                bwd_mix(q, p, v, rel, da, dq, dv, dk, sz, t, gsum, pv, pr, 3, i)
                return c
            lax.fori_loop(0, 2, lambda i, c: wide(i + 2, c), 0)
            tick()
            bwd_cast(dq, dk, dv, dj)
            if layer == 0:
                cps.wait("W0", "in0h1")
            wgrad(h1, dj, gq, 0, 3)
            mid()
            mm_nt(dj, slice(0, 1536), W, 0, 3, dq)
            if layer == 0:
                cps.wait("in0n1", "in0inv1")
            norm_back_phase(dq, n1, inv1, t, 0, dx, None, gsum, 0, 1, None)
        scope(run, *vm(L4, L4, L4, REL, L4, L4, SUMM, ((R, 3 * D), BF16)))
        end()
        bwd_conv1(xin, dx, da, sz, t, gsum, pv, pr)
        build_small(gsum, gb1, y, tau, gsm)

    def scatter(n, g, rows, out, which):
        bufs = r["bufs"][4 * which:4 * which + 4]
        return lambda: scatter_ticks(Place(4), g, rows, *bufs, out, r["rs_send"].at[n], r["rs_recv"].at[n])

    def fc_scatter(layer):
        out = r[f"sfc{layer}"]
        return Ticker([(i, scatter(4 * layer + i, gfc, pl.ds(a, b - a), out.at[pl.ds(a, b - a)], i)) for i, (a, b) in enumerate(SCATTERS)])

    def q_scatter(layer):
        return Ticker([(0, scatter(4 * layer + 2, gq, slice(None), r[f"sq{layer}"], 2))])

    def s_scatter(layer):
        return Ticker([(0, scatter(4 * layer + 3, gsm, slice(None), r[f"ss{layer}"], 3))])

    forward(0, xa, xb, None)

    def top(g, slope, n2, h2, inv2, dm):
        def emit(stage, stage2):
            cps.start("cot", r["cotangent"], stage)
            give_images(xa, stage2, sz)
            cps.start("out", stage2, r["output"])
            cps.wait("cot")
            take_images(stage, dxb, sz)
            cps.wait("out")
        scope(emit, STAGE, STAGE)
        first_half(1, dxb, da, g, slope, n2, h2, inv2, dm, Idle())
    forward(1, xb, xa, top)

    for i in (1, 2, 3):
        load_piece(0, i)
    cps.start("in0a", r["park0a"], a_low)
    if comm:
        rs = fc_scatter(1)
        rs()
    else:
        rs = Idle()
        cps.start("gfc1", gfc, r["gfc1"])

    def mid1():
        rs()

    def end1():
        rs()
        load_piece(0, 0)
        cps.start("in0h1", r["park0h1"], h1)
        cps.start("in0n1", r["park0n1"], n1)
        cps.start("in0inv1", r["park0inv1"], inv1)
    second_half(1, xb, dxb, da, xa, rs, mid1, end1)
    rs.finish()

    if comm:
        class Pair(Idle):
            def __init__(self):
                self.a, self.b = q_scatter(1), s_scatter(1)

            def __call__(self):
                self.a()
                self.b()

            def finish(self):
                self.a.finish()
                self.b.finish()
        rs2 = Pair()
        rs2()
    else:
        rs2 = Idle()
        cps.wait("gfc1")
        cps.start("gq1", gq, r["gq1"])
        cps.start("gsm1", gsm, r["gsm1"])
        cps.wait("gq1", "gsm1")

    def bottom(g, slope, n2, h2, inv2, dm):
        for name, ref in (("slope", slope), ("g", g), ("h2", h2), ("n2", n2), ("inv2", inv2)):
            cps.start("in0" + name, r["park0" + name], ref)
        first_half(0, da, dxb, g, slope, n2, h2, inv2, dm, rs2)
    scope(bottom, *vm(WIDE, WIDE, LOW, LOW, INV, LOW))
    rs2.finish()
    if comm:
        place = Place(4)
        far = [place.dev(z=place.off(k)) for k in range(1, 4)]
        near = [place.dev(x=1 - place.x), place.dev(y=1 - place.y), place.dev(c=1 - place.c)]
        for who in far + near:
            pl.semaphore_signal(r["credit"], inc=1, device_id=who, device_id_type=MESH)
        pl.semaphore_wait(r["credit"], 6)
        rs = fc_scatter(0)
        rsq = q_scatter(0)
        rss = s_scatter(0)
        rs()
    else:
        rs = rsq = rss = Idle()
        cps.start("gfc0", gfc, r["gfc0"])

    def mid0():
        rs.finish()
        rsq()

    def end0():
        rsq()

        def again(stage):
            cps.start("again", r["images"], stage)
            cps.wait("again")
            take_images(stage, xb)
        scope(again, STAGE)
        rsq()
    second_half(0, xb, da, dxb, xa, rs, mid0, end0)
    if comm:
        rss()
        rsq()
        rss()
    else:
        cps.start("gq0", gq, r["gq0"])
        cps.start("gsm0", gsm, r["gsm0"])

    def last(stage3):
        give_images(dxb, stage3)
        cps.start("dx", stage3, r["grad_images"])
        rss()
        rsq.finish()
        rss.finish()
        if not comm:
            cps.wait("gfc0", "gq0", "gsm0")
        cps.wait("dx")
    scope(last, pltpu.VMEM((NI, SLOT, D), F32))


def step(comm, images, cotangent, sz, *more):
    vmem = pltpu.VMEM
    if comm:
        inputs = ["images", "cotangent", "sz", "shard0", "shard1", "small"]
        in_specs = [ANY, ANY] + [VM] * 4
    else:
        inputs = ["images", "cotangent", "sz", "w0", "w1", "tab", "b1"]
        in_specs = [ANY, ANY, VM, ANY, ANY, VM, VM]
    outs = [("output", sd((NI, SLOT, D), BF16), ANY), ("grad_images", sd((NI, SLOT, D), F32), ANY)]
    shares = []
    for layer in (0, 1):
        if comm:
            shares += [(f"sfc{layer}", sd((144, D), F32), VM), (f"sq{layer}", sd((48, D), F32), VM), (f"ss{layer}", sd((16, 128), F32), VM)]
        else:
            shares += [(f"gfc{layer}", packed(144), ANY), (f"gq{layer}", packed(48), ANY), (f"gsm{layer}", packed(16, 128, F32), ANY)]
    outs += shares
    outs += [(f"park0{n}", sd(*sh), ANY) for n, sh in PARK0] + [(f"park1{n}", sd(*sh), ANY) for n, sh in PARK]
    if comm:
        outs += [("w0", packed(WROWS), ANY), ("w1", packed(WROWS), ANY)]
    scratch = [("W", vmem((2, 4, 2, 2, WROWS, D), BF16)), ("gfc", vmem((2, 4, 2, 2, 144, D), BF16)), ("gq", vmem((2, 4, 2, 2, 48, D), BF16)),
               ("gsm", vmem((2, 4, 2, 2, 16, 128), F32)), ("gsum", vmem((4, TROWS, 128), F32)), ("gb1", vmem((8, FF), F32)),
               ("tau", vmem((288, 128), F32)), ("pv", vmem(PADDED, F32)), ("pr", vmem(PADDED, F32)), ("n1", vmem(*LOW)), ("h1", vmem(*LOW)), ("inv1", vmem(*INV)), ("a", vmem(*LOW))]
    scratch += [(n, vmem(*L4)) for n in ("xa", "xb", "da", "dxb")] + [("copy_sems", pltpu.SemaphoreType.DMA((COPIES,)))]
    bufs = []
    if comm:
        sems = pltpu.SemaphoreType.DMA
        scratch += [("tab", vmem((2, 4, TROWS, 128), F32)), ("b1", vmem((2, 16, 128), F32)), ("gs", vmem((2, 4, 2, 2, 32, 128), F32)),
                    ("ag_send", sems((7, 8))), ("ag_recv", sems((7, 8))), ("rs_send", sems((8, 8))), ("rs_recv", sems((8, 8))), ("credit", pltpu.SemaphoreType.REGULAR)]
        for rows, width, dt in ((80, D, BF16), (64, D, BF16), (48, D, BF16), (16, 128, F32)):
            bufs += scatter_bufs(4, rows, width, dt)
    names = inputs + [n for n, _, _ in outs] + [n for n, _ in scratch]

    def kernel(*refs):
        count = len(names)
        r = list(refs[:count])
        step_kernel(comm, names + ["bufs"], *r, refs[count:])
    params = dict(vmem_limit_bytes=67043328)
    if comm:
        params.update(collective_id=0, has_side_effects=True)
    got = pl.pallas_call(
        kernel, out_shape=[o for _, o, _ in outs], in_specs=in_specs, out_specs=[sp for _, _, sp in outs],
        scratch_shapes=[sc for _, sc in scratch] + bufs, compiler_params=pltpu.CompilerParams(**params), name="step",
    )(images, cotangent, sz, *more)
    return got[:2 + len(shares)]


def window_mask():
    channel = lax.broadcasted_iota(jnp.int32, (49, D), 1)
    tap = lax.broadcasted_iota(jnp.int32, (49, D), 0)
    head = channel // (D // HEADS)
    reach = jnp.where(head < 2, 1, jnp.where(head < 5, 2, 3))
    return ((jnp.abs(tap // 7 - 3) <= reach) & (jnp.abs(tap % 7 - 3) <= reach)).astype(F32)


def blocks_of(flat, rows, cols):
    return flat.reshape(rows, cols // D, D).transpose(1, 0, 2).reshape(rows * cols // D, D)


def pack(qkv, proj, fc1, fc2, n):
    per = D // n
    return jnp.concatenate([blocks_of(qkv, per, 3 * D), proj.reshape(per, D), blocks_of(fc1, per, FF), fc2.reshape(FF // n, D)])


def tables(small):
    small = small.astype(F32)
    end = TABLE * D
    tb = small[:end].reshape(D, TABLE).T
    cpe = small[end + FF:].reshape(D, 10).T
    tab = jnp.concatenate([tb[:9], tb[9:] * window_mask(), jnp.zeros((CPE - TABLE, D), F32), cpe, jnp.zeros((TROWS - CPE - 10, D), F32)])
    return tab.reshape(TROWS, 4, 128).transpose(1, 0, 2), small[end:end + FF].reshape(16, 128)


def whole_weights(mine, small, n):
    per = D // n
    full = lax.all_gather(mine[None], AXES, axis=0, tiled=True)
    vec = lax.all_gather(small, AXES, axis=0, tiled=True)
    parts = [full[:, j * per:(j + 1) * per].reshape(32, D // 32, D) for j in range(8)] + [full[:, 8 * per:].reshape(32, FF // 32, D)]
    w = jnp.concatenate(parts, axis=1).reshape(4, 2, 2, 2, WROWS, D).transpose(3, 0, 1, 2, 4, 5)
    return w, *tables(vec)


def share_by_xla(gfc, gq, gsm, n):
    per = D // n

    def rows(a):
        return a.transpose(1, 2, 3, 0, 4, 5).reshape((32,) + a.shape[4:])
    gq, gfc, gsm = rows(gq), rows(gfc), rows(gsm)
    every = jnp.concatenate([gq, gfc[:, :80]], axis=1)
    parts = [every[:, 16 * j:16 * j + 16].reshape(n, per, D) for j in range(8)] + [gfc[:, 80:].reshape(n, FF // n, D)]
    vec = gsm[:, :9].reshape(n, -1)
    width = vec.shape[1]
    parts.append(jnp.pad(vec, ((0, 0), (0, -width % D))).reshape(n, -1, D).astype(BF16))
    share = lax.psum_scatter(jnp.concatenate(parts, axis=1), AXES, scatter_dimension=0, tiled=True)[0].astype(F32)
    mats = split_shares(share[:8 * per + FF // n], per)
    return (*mats, share[8 * per + FF // n:].reshape(-1)[:width])


def split_shares(share, per):
    def cols(first, count):
        return share[first * per:(first + count) * per].reshape(count, per, D).transpose(1, 0, 2).reshape(-1)
    return cols(0, 3), cols(3, 1), cols(4, 4), share[8 * per:].reshape(-1)


def shards(n, images, grid_sizes, qkv, proj, fc1, fc2, small, cotangent):
    layers = qkv.shape[0]
    mine = [pack(qkv[l], proj[l], fc1[l], fc2[l], n) for l in range(layers)]
    sz = jnp.broadcast_to(grid_sizes[:, None], (NI, 128))
    if n == 32:
        flat = jnp.pad(small.astype(F32).reshape(2, 9, 128), ((0, 0), (0, 7), (0, 0))).reshape(32, 128)
        output, dx, *got = step(True, images, cotangent, sz, mine[0], mine[1], flat)
        shares = [(*split_shares(jnp.concatenate([q, fc]), D // n), s[:9].reshape(-1)) for fc, q, s in (got[:3], got[3:])]
    else:
        held = [whole_weights(mine[l], small[l], n) for l in range(layers)]
        output, dx, *got = step(False, images, cotangent, sz, held[0][0], held[1][0], jnp.stack([held[0][1], held[1][1]]), jnp.stack([held[0][2], held[1][2]]))
        shares = [share_by_xla(*got[:3], n), share_by_xla(*got[3:], n)]
    grads = [jnp.stack([shares[l][i] for l in range(layers)]) for i in range(5)]
    return (output, dx, *grads)


def solution(mesh):
    n = mesh.shape["wide"] * mesh.shape["narrow"]
    from jax.sharding import PartitionSpec as P
    rows, flat = P(AXES, None, None), P(None, AXES)
    return jax.shard_map(
        functools.partial(shards, n), mesh=mesh,
        in_specs=(rows, P(AXES), flat, flat, flat, flat, flat, rows),
        out_specs=(rows, rows, flat, flat, flat, flat, flat),
        check_vma=False)
```

```python
import functools
import jax
import jax.numpy as jnp
from jax import lax
from jax.experimental import pallas as pl
from jax.experimental.pallas import tpu as pltpu

F32, BF16 = jnp.float32, jnp.bfloat16
D, FF, HEADS, GRID, SLOT = 512, 2048, 8, 9, 82
TABLE = 58
EPS = 1e-6
NI = 16
R = SLOT * NI
PADS = 96
RP = PADS * NI
RADII = (1, 2, 3, 3)
AXES = ("wide", "narrow")
WROWS = 192
TAPS, CPE, CPEB, TROWS = 9, 64, 73, 80


def ds(start, size, align=8):
    if not isinstance(start, int):
        start = pl.multiple_of(start, align)
    return pl.ds(start, size)


def row8(ref, i, lg):
    return ref[lg, pl.ds(i, 8, stride=0), :]


def row(tab, i, j=None):
    parts = range(4) if j is None else (2 * j, 2 * j + 1)
    return jnp.concatenate([tab[g, i:i + 1, :] for g in parts], axis=1)


def put2(ref, at, j, val):
    ref[2 * j, at, :] = val[:, :128]
    ref[2 * j + 1, at, :] = val[:, 128:]


def cell(y, x, ig):
    return ds((1 + GRID * y + x) * NI + 8 * ig, 8)


def inside_at(sz, y, x):
    return sz > max(y, x)


PROW = GRID * NI
PADDED = ((GRID + 6) * PROW, 128)


def at_cell(y, x, ig):
    return pl.ds(pl.multiple_of((1 + GRID * y + x) * NI + 8 * ig, 8), 8)


def at_padded(y, x, ig):
    return pl.ds(pl.multiple_of((y + 3) * PROW + x * NI + 8 * ig, 8), 8)


def rows_loop(fn, init):
    return lax.fori_loop(0, GRID, fn, init)


def groups(fn):
    def run(ig, c):
        fn(ig)
        return c
    lax.fori_loop(0, 2, run, 0)


def lane_groups(fn):
    fn(1, 0)
    fn(2, 1)

    def run(i, c):
        fn(3, i + 2)
        return c
    lax.fori_loop(0, 2, run, 0)


def conv_pass(src, load_tap, radius, ig, emit, init, flip=False):
    span = range(-radius, radius + 1)

    def body(y, carry):
        acc = [None] * GRID
        for a in span:
            line = [src[at_padded(y - a if flip else y + a, x, ig), :] for x in range(GRID)]
            for b in span:
                tap = load_tap(a, b)
                for x in range(GRID):
                    xx = x - b if flip else x + b
                    if 0 <= xx < GRID:
                        term = line[xx] * tap
                        acc[x] = term if acc[x] is None else acc[x] + term
        return emit(y, acc, carry)
    return rows_loop(body, init)


def conv_kgrad(grad, src, radius, emit):
    span = range(-radius, radius + 1)
    rows = list(span)
    for part in (rows[:4], rows[4:]):
        if not part:
            continue

        def body(t, acc):
            y, ig = t // 2, t % 2
            acc = list(acc)
            up = [grad[at_padded(y, x, ig), :] for x in range(GRID)]
            for i, a in enumerate(part):
                line = [src[at_padded(y + a, x, ig), :] for x in range(GRID)]
                for j, b in enumerate(span):
                    k = i * len(span) + j
                    for x in range(GRID):
                        if 0 <= x + b < GRID:
                            acc[k] = acc[k] + up[x] * line[x + b]
            return tuple(acc)
        zero = jnp.zeros((8, 128), F32)
        sums = lax.fori_loop(0, 2 * GRID, body, (zero,) * (len(part) * len(span)), unroll=2)
        for i, a in enumerate(part):
            for j, b in enumerate(span):
                emit(a, b, sums[i * len(span) + j])


def zero_padded(ref):
    ref[...] = jnp.zeros(PADDED, F32)


def fill_padded(dst, src, lg, sz):
    def body(t, c):
        y, ig = t // 2, t % 2
        size = sz[ds(8 * ig, 8), :]
        for x in range(GRID):
            dst[at_padded(y, x, ig), :] = jnp.where(size > jnp.maximum(y, x), src[lg, at_cell(y, x, ig), :], 0.0)
        return c
    lax.fori_loop(0, 2 * GRID, body, 0)


def norm_rows(x):
    mean = jnp.mean(x, axis=-1, keepdims=True)
    cen = x - mean
    inv = lax.rsqrt(jnp.mean(cen * cen, axis=-1, keepdims=True) + EPS)
    return cen * inv, inv


def dot(a, b, ca, cb):
    return lax.dot_general(a, b, (((ca,), (cb,)), ((), ())), preferred_element_type=F32)


def head_mask():
    r = lax.broadcasted_iota(jnp.int32, (256, 256), 0) // 64
    c = lax.broadcasted_iota(jnp.int32, (256, 256), 1) // 64
    return r == c


def by_tiles(fn):
    def body(i, c):
        fn(pl.ds(pl.multiple_of(i * 256, 256), 256))
        return c
    lax.fori_loop(0, R // 256, body, 0)
    if R % 256:
        fn(pl.ds(R // 256 * 256, R % 256))


def full(ref, at):
    return jnp.concatenate([ref[g, at, :] for g in range(4)], axis=1)


def spread(ref, at, val):
    for g in range(4):
        ref[g, at, :] = val[:, 128 * g:128 * g + 128]


def fwd_conv1(x, sz, tab, x1, pv):
    def one(lg, c):
        fill_padded(pv, x, lg, sz)

        def group(ig):
            size = sz[ds(8 * ig, 8), :]
            x1[lg, ds(8 * ig, 8), :] = x[lg, ds(8 * ig, 8), :]
            bias = row8(tab, CPEB, lg)

            def emit(y, acc, carry):
                for k in range(GRID):
                    at = at_cell(y, k, ig)
                    x1[lg, at, :] = x[lg, at, :] + jnp.where(size > jnp.maximum(y, k), acc[k] + bias, 0.0)
                return carry
            conv_pass(pv, lambda a, b: row8(tab, CPE + (a + 1) * 3 + b + 1, lg), 1, ig, emit, 0)
        groups(group)
        return c
    lax.fori_loop(0, 4, one, 0)


def norm_phase(src, tab, gain, shift, hat, low, inv_ref):
    def fn(at):
        n, inv = norm_rows(full(src, at))
        hat[at, :] = n.astype(BF16)
        low[at, :] = (n * row(tab, gain) + row(tab, shift)).astype(BF16)
        inv_ref[at, :] = jnp.broadcast_to(inv, (n.shape[0], 128))
    by_tiles(fn)


def weight(g, block, first, count, cols):
    at = ds(16 * block, 16, 16)
    return jnp.concatenate([g[t % 2, t // 8, t // 4 % 2, t // 2 % 2, at, cols] for t in range(first // 16, (first + count) // 16)], axis=0)


def weight2(g, chunk, cols):
    return jnp.concatenate([g[i % 2, chunk, i // 4, i // 2 % 2, 128:192, cols] for i in range(8)], axis=0)


def halves(fn):
    def body(i, c):
        fn(pl.ds(pl.multiple_of(i // 2 * (R // 2), 16), R // 2), i % 2)
        return c
    lax.fori_loop(0, 4, body, 0)


def cols256(j):
    return pl.ds(pl.multiple_of(j * 256, 256), 256)


def both_lanes(ref, at, j):
    return jnp.concatenate([ref[2 * j, at, :], ref[2 * j + 1, at, :]], axis=1)


def zero_tail(ref):
    ref[:, R:RP, :] = jnp.zeros((4, RP - R, 128), F32)


def fwd_qkv(low, w, tab, q, k, v):
    def fn(at, j):
        h = low[at, :]
        for b, (ref, bias) in enumerate(((q, 4), (k, None), (v, 5))):
            val = dot(h, weight(w, b, 0, D, cols256(j)), 1, 0)
            put2(ref, at, j, val if bias is None else val + row(tab, bias, j))
    halves(fn)
    for ref in (q, k, v):
        zero_tail(ref)


def each_pos(size, ig, fn):
    fn(ds(8 * ig, 8), None)
    for y in range(GRID):
        for x in range(GRID):
            fn(cell(y, x, ig), inside_at(size, y, x))


def fwd_softmax(k, sz):
    def body(i, c):
        lg, ig = i // 2, i % 2
        size = sz[ds(8 * ig, 8), :]
        best = [None] * 4
        cnt = [0]

        def first(at, ok):
            val = k[lg, at, :]
            if ok is not None:
                val = jnp.where(ok, val, -1e30)
            j = cnt[0] % 4
            best[j] = val if best[j] is None else jnp.maximum(best[j], val)
            cnt[0] += 1
        each_pos(size, ig, first)
        top = jnp.maximum(jnp.maximum(best[0], best[1]), jnp.maximum(best[2], best[3]))
        total = [None] * 4
        cnt[0] = 0

        def second(at, ok):
            val = jnp.exp(k[lg, at, :] - top)
            if ok is not None:
                val = jnp.where(ok, val, 0.0)
            k[lg, at, :] = val
            j = cnt[0] % 4
            total[j] = val if total[j] is None else total[j] + val
            cnt[0] += 1
        each_pos(size, ig, second)
        scale = 1.0 / ((total[0] + total[1]) + (total[2] + total[3]))

        def third(at, ok):
            k[lg, at, :] = k[lg, at, :] * scale
        each_pos(size, ig, third)
        return c
    lax.fori_loop(0, 8, body, 0)


def img_load(ref, i, half):
    return jnp.concatenate([ref[2 * half + j, pl.ds(i, PADS, stride=NI), :] for j in range(2)], axis=1)


def img_store(ref, i, half, val):
    for j in range(2):
        ref[2 * half + j, pl.ds(i, PADS, stride=NI), :] = val[:, 128 * j:128 * j + 128]


def fwd_attn(q, p, v, s, f):
    def body(t, c):
        i, half = t // 2, t % 2
        pi = img_load(p, i, half).astype(BF16)
        vi = img_load(v, i, half).astype(BF16)
        summ = jnp.where(head_mask(), dot(pi, vi, 0, 0), 0.0).astype(BF16)
        s[t] = (summ[0:64] + summ[64:128]) + (summ[128:192] + summ[192:256])
        qi = img_load(q, i, half).astype(BF16)
        img_store(f, i, half, dot(qi, summ, 1, 0) * 0.125)
        return c
    lax.fori_loop(0, 2 * NI, body, 0, unroll=4)


def fwd_conv3(v, q, f, sz, tab, rel, pv, radius, lg):
    fill_padded(pv, v, lg, sz)
    bias = row8(tab, 8, lg)

    def group(ig):
        size = sz[ds(8 * ig, 8), :]

        def emit(y, acc, carry):
            for k in range(GRID):
                at = at_cell(y, k, ig)
                r = acc[k] + bias
                rel[lg, at, :] = r
                f[lg, at, :] = f[lg, at, :] + jnp.where(size > jnp.maximum(y, k), q[lg, at, :] * r, 0.0)
            return carry
        conv_pass(pv, lambda a, b: row8(tab, TAPS + (a + 3) * 7 + b + 3, lg), radius, ig, emit, 0)
    groups(group)


def fwd_proj(att, w, tab, x1, a_low):
    def low(at):
        a_low[at, :] = full(att, at).astype(BF16)
    by_tiles(low)

    def fn(at, j):
        put2(x1, at, j, both_lanes(x1, at, j) + dot(a_low[at, :], weight(w, 3, 0, D, cols256(j)), 1, 0) + row(tab, 6, j))
    halves(fn)


def normal_cdf(u):
    t = 1.0 / (1.0 + jnp.abs(u) * (0.3275911 * 0.7071067811865476))
    e = jnp.exp(-0.5 * u * u)
    poly = t * (0.5 * 0.254829592 + t * (0.5 * -0.284496736 + t * (0.5 * 1.421413741 + t * (0.5 * -1.453152027 + t * (0.5 * 1.061405429)))))
    tail = poly * e
    return jnp.where(u >= 0, 1.0 - tail, tail), e


def fwd_fc1(low, w, b1, g, slope):
    def body(j, c):
        cols = pl.ds(pl.multiple_of(j * 512, 512), 512)
        bias = jnp.concatenate([b1[pl.ds(4 * j + i, 1), :] for i in range(4)], axis=1)
        u = dot(low[...], weight(w, 4 + j, 0, D, slice(None)), 1, 0) + bias
        cdf, e = normal_cdf(u)
        g[:, cols] = (u * cdf).astype(BF16)
        slope[:, cols] = (cdf + u * e * 0.3989422804014327).astype(BF16)
        return c
    lax.fori_loop(0, 4, body, 0)


def fwd_fc2(g, w, tab, x1):
    def fn(at, j):
        wide = jnp.concatenate([weight2(w, c, cols256(j)) for c in range(4)], axis=0)
        put2(x1, at, j, both_lanes(x1, at, j) + dot(g[at, :], wide, 1, 0) + row(tab, 7, j))
    halves(fn)


def fold_rows(val):
    parts = [val[8 * i:8 * i + 8] for i in range(val.shape[0] // 8)]
    while len(parts) > 1:
        parts = [a + b for a, b in zip(parts[::2], parts[1::2])] + parts[len(parts) // 2 * 2:]
    return parts[0]


def add_rows(ref, row, val):
    total = jnp.sum(fold_rows(val), axis=0, keepdims=True)
    for g in range(4):
        ref[g, row:row + 1, :] += total[:, 128 * g:128 * g + 128]


def add_sum(ref, lg, row, val):
    ref[lg, row:row + 1, :] += jnp.sum(val, axis=0, keepdims=True)


def bwd_cast_sum(dx, low, gsum, row):
    def fn(at):
        val = full(dx, at).astype(BF16)
        low[at, :] = val
        add_rows(gsum, row, val.astype(F32))
    by_tiles(fn)


def bwd_du(dm, w, slope, gb1):
    def body(j, c):
        cols = pl.ds(pl.multiple_of(j * 512, 512), 512)
        d = dot(dm[...], weight2(w, j, slice(None)), 1, 1) * slope[:, cols].astype(F32)
        slope[:, cols] = d.astype(BF16)
        gb1[:, cols] = fold_rows(d)
        return c
    lax.fori_loop(0, 4, body, 0)


def norm_back_phase(up, hat, inv_ref, tab, gain, res, out_low, sums, rg, rs, rb):
    def fn(at):
        u = full(up, at)
        n = hat[at, :].astype(F32)
        e = u * row(tab, gain)
        m1 = jnp.mean(e, axis=-1, keepdims=True)
        m2 = jnp.mean(e * n, axis=-1, keepdims=True)
        d = full(res, at) + inv_ref[at, 0:1] * (e - m1 - n * m2)
        spread(res, at, d)
        add_rows(sums, rg, u * n)
        add_rows(sums, rs, u)
        if out_low is not None:
            low = d.astype(BF16)
            out_low[at, :] = low
            add_rows(sums, rb, low.astype(F32))
    by_tiles(fn)


def mm_nt(a, cols, g, first, blocks, out):
    def fn(at, j):
        def rows(b):
            here = slice(16 * b, 16 * b + 16)
            return jnp.concatenate([g[i % 2, 2 * j + i // 8, i // 4 % 2, i // 2 % 2, here, :] for i in range(16)], axis=0)
        w = jnp.concatenate([rows(first + b) for b in range(blocks)], axis=1)
        put2(out, at, j, dot(a[at, cols], w, 1, 1))
    halves(fn)


def wgrad(left, right, gr, first, blocks):
    def body(j, c):
        tile = dot(left[...], right[:, pl.ds(pl.multiple_of(512 * j, 512), 512)], 0, 0).astype(BF16)
        at = pl.ds(pl.multiple_of(first + 16 * j, 16), 16)
        for t in range(32):
            gr[t % 2, t // 8, t // 4 % 2, t // 2 % 2, at, :] = tile[16 * t:16 * t + 16]
        return c
    lax.fori_loop(0, blocks, body, 0)


def wgrad2(left, right, gr, first):
    def body(j, c):
        tile = dot(left[:, pl.ds(pl.multiple_of(512 * j, 512), 512)], right[...], 0, 0).astype(BF16)
        for i in range(8):
            gr[i % 2, j, i // 4, i // 2 % 2, first:first + 64, :] = tile[64 * i:64 * i + 64]
        return c
    lax.fori_loop(0, 4, body, 0)


def bwd_attn1(q, p, v, s, da, dq, dv, dk):
    def body(t, c):
        i, half = t // 2, t % 2
        df = (img_load(da, i, half) * 0.125).astype(BF16)
        wide = s[t]
        wide = jnp.where(head_mask(), jnp.concatenate([wide] * 4, axis=0), jnp.zeros((), BF16))
        qi = img_load(q, i, half).astype(BF16)
        dsum = jnp.where(head_mask(), dot(qi, df, 0, 0), 0.0).astype(BF16)
        img_store(dq, i, half, dot(df, wide, 1, 1))
        pi = img_load(p, i, half).astype(BF16)
        img_store(dv, i, half, dot(pi, dsum, 1, 0))
        vi = img_load(v, i, half).astype(BF16)
        img_store(dk, i, half, dot(vi, dsum, 1, 1))
        return c
    lax.fori_loop(0, 2 * NI, body, 0, unroll=4)


def bwd_mix(q, p, v, rel, da, dq, dv, dk, sz, tab, gsum, pv, pr, radius, lg):
    fill_padded(pv, v, lg, sz)

    def group(ig):
        size = sz[ds(8 * ig, 8), :]
        cls = ds(8 * ig, 8)
        dqc = dq[lg, cls, :]

        def first(y, carry):
            rs, qs, ps = carry
            for x in range(GRID):
                at = at_cell(y, x, ig)
                d = jnp.where(size > jnp.maximum(y, x), da[lg, at, :], 0.0)
                dr = q[lg, at, :] * d
                pr[at_padded(y, x, ig), :] = dr
                dqv = dq[lg, at, :] + rel[lg, at, :] * d
                dq[lg, at, :] = dqv
                rs, qs, ps = rs + dr, qs + dqv, ps + p[lg, at, :] * dk[lg, at, :]
            return rs, qs, ps
        rs, qs, ps = rows_loop(first, (jnp.zeros((8, 128), F32), dqc, p[lg, cls, :] * dk[lg, cls, :]))
        add_sum(gsum, lg, 8, rs)
        add_sum(gsum, lg, 4, qs)
        dk[lg, cls, :] = p[lg, cls, :] * (dk[lg, cls, :] - ps)

        def second(y, carry):
            for x in range(GRID):
                at = at_cell(y, x, ig)
                dk[lg, at, :] = p[lg, at, :] * (dk[lg, at, :] - ps)
            return carry
        rows_loop(second, 0)

        def emit(y, acc, total):
            for x in range(GRID):
                at = at_cell(y, x, ig)
                val = dv[lg, at, :] + jnp.where(size > jnp.maximum(y, x), acc[x], 0.0)
                dv[lg, at, :] = val
                total = total + val
            return total
        add_sum(gsum, lg, 5, conv_pass(pr, lambda a, b: row8(tab, TAPS + (a + 3) * 7 + b + 3, lg), radius, ig, emit, dv[lg, cls, :], True))
    groups(group)

    def emit_tap(a, b, val):
        add_sum(gsum, lg, TAPS + (a + 3) * 7 + b + 3, val)
    conv_kgrad(pr, pv, radius, emit_tap)


def bwd_cast(dq, dk, dv, dj):
    def fn(at):
        for j, ref in enumerate((dq, dk, dv)):
            dj[at, 512 * j:512 * j + 512] = full(ref, at).astype(BF16)
    by_tiles(fn)


def bwd_conv1(x, dx1, dx, sz, tab, gsum, pv, pr):
    def one(lg, c):
        fill_padded(pv, x, lg, sz)
        fill_padded(pr, dx1, lg, sz)

        def group(ig):
            size = sz[ds(8 * ig, 8), :]
            cls = ds(8 * ig, 8)
            dx[lg, cls, :] = dx1[lg, cls, :]

            def emit(y, acc, total):
                for k in range(GRID):
                    at = at_cell(y, k, ig)
                    total = total + pr[at_padded(y, k, ig), :]
                    dx[lg, at, :] = dx1[lg, at, :] + jnp.where(size > jnp.maximum(y, k), acc[k], 0.0)
                return total
            add_sum(gsum, lg, CPEB, conv_pass(pr, lambda a, b: row8(tab, CPE + (a + 1) * 3 + b + 1, lg), 1, ig, emit, jnp.zeros((8, 128), F32), True))
        groups(group)

        def emit_tap(a, b, val):
            add_sum(gsum, lg, CPE + (a + 1) * 3 + b + 1, val)
        conv_kgrad(pr, pv, 1, emit_tap)
        return c
    lax.fori_loop(0, 4, one, 0)


MESH = pl.DeviceIdType.MESH


class Place:
    def __init__(self, line):
        w, m = lax.axis_index("wide"), lax.axis_index("narrow")
        self.line = line
        self.z, self.x, self.y, self.c = w // 2, w % 2, m // 2, m % 2

    def dev(self, z=None, x=None, y=None, c=None):
        z = self.z if z is None else z
        x = self.x if x is None else x
        y = self.y if y is None else y
        c = self.c if c is None else c
        return (z * 2 + x, y * 2 + c)

    def off(self, k):
        return lax.rem(self.z + self.line + k, self.line)


def greet(place):
    barrier = pltpu.get_barrier_semaphore()
    far = [place.dev(z=place.off(k)) for k in range(1, place.line)]
    near = [place.dev(x=1 - place.x), place.dev(y=1 - place.y), place.dev(c=1 - place.c)]
    for who in far + near:
        pl.semaphore_signal(barrier, inc=1, device_id=who, device_id_type=MESH)
    pl.semaphore_wait(barrier, place.line + 2)


def remote(src, dst, send, recv, dev):
    return pltpu.make_async_remote_copy(src_ref=src, dst_ref=dst, send_sem=send, recv_sem=recv, device_id=dev, device_id_type=MESH)


def both(copy):
    copy.wait_send()
    copy.wait_recv()


def by_core(place, a, b):
    def run():
        @pl.when(place.c == 0)
        def _():
            a()

        @pl.when(place.c == 1)
        def _():
            b()
    return run


def gather_ticks(place, g, rows, send, recv):
    n, z, x, y = place.line, place.z, place.x, place.y

    def lines():
        mine = g.at[place.c, z, x, y, rows]
        return [remote(mine, mine, send.at[k - 1], recv.at[k - 1], place.dev(z=place.off(k))) for k in range(1, n)]

    def line_waits():
        for k, cp in enumerate(lines()):
            cp.wait_send()
            got = g.at[place.c, place.off(-k - 1), x, y, rows]
            remote(got, got, send.at[k], recv.at[k], place.dev(z=place.off(1))).wait_recv()

    def parts(core):
        if core == 0:
            return (g.at[0, :, x, y, rows], g.at[0, :, x, :, rows]), (g.at[0, :, x, y, rows], g.at[0, :, x, 1 - y, rows], g.at[0, :, 1 - x, :, rows])
        return (g.at[1, :, x, y, rows], g.at[1, :, :, y, rows]), (g.at[1, :, x, y, rows], g.at[1, :, 1 - x, y, rows], g.at[1, :, :, 1 - y, rows])

    def swap(core, i):
        part = parts(core)[0][i]
        over_y = (core == 0) == (i == 0)
        return remote(part, part, send.at[n - 1 + i], recv.at[n - 1 + i], place.dev(y=1 - y) if over_y else place.dev(x=1 - x))

    def hand(core, i):
        part = parts(core)[1][i]
        return remote(part, part, send.at[n + 1 + i], recv.at[n + 1 + i], place.dev(c=1 - place.c))

    def steps(core):
        def last():
            for i in range(3):
                hand(core, i).wait_send()
                hand(1 - core, i).wait_recv()
        return [lambda: None,
                lambda: (swap(core, 0).start(), hand(core, 0).start()),
                lambda: (both(swap(core, 0)), swap(core, 1).start(), hand(core, 1).start()),
                lambda: (both(swap(core, 1)), hand(core, 2).start()),
                last]
    ticks = [by_core(place, a, b) for a, b in zip(steps(0), steps(1))]

    def first():
        for cp in lines():
            cp.start()

    def second():
        line_waits()
        ticks[1]()
    return [first, second] + ticks[2:]


def add_blocks(pairs):
    for dst, src in pairs:
        dst[...] = (dst[...].astype(F32) + src[...].astype(F32)).astype(dst.dtype)


def scatter_ticks(place, g, rows, cbuf, pbuf, sbuf, zbuf, out, send, recv):
    n, z, x, y, c = place.line, place.z, place.x, place.y, place.c

    def cores():
        return remote(g.at[1 - c, :, :, :, rows], cbuf, send.at[0], recv.at[0], place.dev(c=1 - c))

    def swaps(core):
        over_x, over_y = place.dev(x=1 - x), place.dev(y=1 - y)
        if core == 0:
            return (remote(g.at[0, :, 1 - x, :, rows], pbuf, send.at[1], recv.at[1], over_x),
                    remote(g.at[0, :, x, 1 - y, rows], sbuf, send.at[2], recv.at[2], over_y))
        return (remote(g.at[1, :, :, 1 - y, rows], pbuf, send.at[1], recv.at[1], over_y),
                remote(g.at[1, :, 1 - x, y, rows], sbuf, send.at[2], recv.at[2], over_x))

    def lines():
        return [remote(g.at[c, place.off(k), x, y, rows], zbuf.at[k - 1], send.at[2 + k], recv.at[2 + k], place.dev(z=place.off(k))) for k in range(1, n)]

    def start_cores():
        cores().start()

    def add_cores():
        both(cores())

        def body(t, carry):
            add_blocks([(g.at[c, t // 4, t // 2 % 2, t % 2, rows], cbuf.at[t // 4, t // 2 % 2, t % 2])])
            return carry
        lax.fori_loop(0, 4 * n, body, 0)

    def step1(core):
        def run():
            add_cores()
            swaps(core)[0].start()
        return run

    def step2(core):
        def run():
            both(swaps(core)[0])

            def body(t, carry):
                dst = g.at[0, t // 2, x, t % 2, rows] if core == 0 else g.at[1, t // 2, t % 2, y, rows]
                add_blocks([(dst, pbuf.at[t // 2, t % 2])])
                return carry
            lax.fori_loop(0, 2 * n, body, 0)
            swaps(core)[1].start()
        return run

    def step3(core):
        def run():
            both(swaps(core)[1])

            def body(t, carry):
                add_blocks([(g.at[core, t, x, y, rows], sbuf.at[t])])
                return carry
            lax.fori_loop(0, n, body, 0)
            for cp in lines():
                cp.start()
        return run

    def finish():
        for cp in lines():
            both(cp)
        total = g[c, z, x, y, rows].astype(F32)
        for k in range(n - 1):
            total = total + zbuf[k].astype(F32)
        out[...] = total
    return [start_cores] + [by_core(place, s(0), s(1)) for s in (step1, step2, step3)] + [finish]


def scatter_bufs(line, rows, width, dtype):
    return [pltpu.VMEM(shape + (rows, width), dtype) for shape in ((line, 2, 2), (line, 2), (line,), (line - 1,))]


STEPS = 5


class Ticker:
    def __init__(self, lists):
        depth = max(i for i, _ in lists) + STEPS
        self.rounds = [[(lambda make=make, at=r - i: make()[at]()) for i, make in lists if 0 <= r - i < STEPS] for r in range(depth)]
        self.done = 0

    def upto(self, count):
        while self.done < min(count, len(self.rounds)):
            for t in self.rounds[self.done]:
                t()
            self.done += 1

    def __call__(self):
        self.upto(self.done + 1)

    def finish(self):
        self.upto(len(self.rounds))


def build_tables(gs, layer, tau, y, tab, b1):
    for t in range(32):
        tau[9 * t:9 * t + 9, :] = gs[t % 2, t // 8, t // 4 % 2, t // 2 % 2, 16 * layer:16 * layer + 9, :]
    lane = lax.broadcasted_iota(jnp.int32, (8, 128), 1)

    def run(base, step, width, b):
        first, off = width * b // 128, width * b % 128
        val = tau[pl.ds(base + first, 8, stride=step), :]
        if off:
            val = pltpu.roll(val, 128 - off, 1)
            if off + width > 128:
                more = pltpu.roll(tau[pl.ds(base + first + 1, 8, stride=step), :], 128 - off, 1)
                val = jnp.where(lane < 128 - off, val, more)
        return val
    for b in range(64):
        tb = run(0, 29, TABLE, b)
        cpe = pltpu.roll(run(248, 5, 10, b), 64, 1)
        y[8 * b:8 * b + 8, :] = jnp.where(lane < TABLE, tb, jnp.where((lane >= 64) & (lane < 74), cpe, 0.0))
    r = lax.broadcasted_iota(jnp.int32, (D, D), 0)
    c = lax.broadcasted_iota(jnp.int32, (D, D), 1)
    place = jnp.where(c == 64 * (r % 8) + r // 8, 1.0, 0.0).astype(BF16)
    table = dot(y[...].astype(BF16), place, 0, 0)[:TROWS]
    tap = lax.broadcasted_iota(jnp.int32, (TROWS, D), 0) - TAPS
    head = lax.broadcasted_iota(jnp.int32, (TROWS, D), 1) // 64
    reach = jnp.where(head < 2, 1, jnp.where(head < 5, 2, 3))
    ok = (tap < 0) | (tap >= 49) | ((jnp.abs(tap // 7 - 3) <= reach) & (jnp.abs(tap % 7 - 3) <= reach))
    table = jnp.where(ok, table, 0.0)
    for g in range(4):
        tab[layer, g] = table[:, 128 * g:128 * g + 128]
    b1[layer] = tau[232:248, :]


def build_small(gsum, gb1, y, tau, gsm):
    r = lax.broadcasted_iota(jnp.int32, (D, D), 0)
    c = lax.broadcasted_iota(jnp.int32, (D, D), 1)
    place = jnp.where(c == 64 * (r % 8) + r // 8, 1.0, 0.0).astype(BF16)
    table = full(gsum, slice(None))
    tap = lax.broadcasted_iota(jnp.int32, (TROWS, D), 0) - TAPS
    head = lax.broadcasted_iota(jnp.int32, (TROWS, D), 1) // 64
    reach = jnp.where(head < 2, 1, jnp.where(head < 5, 2, 3))
    ok = (tap < 0) | (tap >= 49) | ((jnp.abs(tap // 7 - 3) <= reach) & (jnp.abs(tap % 7 - 3) <= reach))
    table = jnp.where(ok, table, 0.0)
    table = jnp.concatenate([table, jnp.zeros((128 - TROWS, D), F32)])
    hi = table.astype(BF16)
    mid = (table - hi.astype(F32)).astype(BF16)
    y[...] = dot(place, hi, 1, 1) + dot(place, mid, 1, 1)
    lane = lax.broadcasted_iota(jnp.int32, (8, 128), 1)

    def lay(base, step, width, start):
        for j in range(step):
            out = None
            for b in range(128 * j // width, min(64, -(-128 * (j + 1) // width))):
                first = width * b - 128 * j
                val = y[8 * b:8 * b + 8, :]
                shift = (first - start) % 128
                if shift:
                    val = pltpu.roll(val, shift, 1)
                out = val if out is None else jnp.where(lane >= first, val, out)
            tau[pl.ds(base + j, 8, stride=step), :] = out
    lay(0, 29, TABLE, 0)
    lay(248, 5, 10, CPE)
    for i in range(16):
        tau[232 + i:233 + i, :] = jnp.sum(gb1[:, 128 * i:128 * i + 128], axis=0, keepdims=True)
    for t in range(32):
        gsm[t % 2, t // 8, t // 4 % 2, t // 2 % 2, 0:9, :] = tau[9 * t:9 * t + 9, :]
        gsm[t % 2, t // 8, t // 4 % 2, t // 2 % 2, 9:16, :] = jnp.zeros((7, 128), F32)


def sd(shape, dtype):
    return jax.ShapeDtypeStruct(shape, dtype)


def packed(rows, width=D, dtype=BF16):
    return sd((2, 4, 2, 2, rows, width), dtype)


ANY = pl.BlockSpec(memory_space=pl.ANY)
VM = pl.BlockSpec(memory_space=pltpu.VMEM)
L4 = ((4, RP, 128), F32)
WIDE = ((R, FF), BF16)
LOW = ((R, D), BF16)
INV = ((R, 128), F32)
SUMM = ((2 * NI, 64, 256), BF16)
REL = ((4, R, 128), F32)
PARK = (("q", L4), ("p", L4), ("v", L4), ("rel", REL), ("s", SUMM))
PARK0 = PARK + (("n1", LOW), ("h1", LOW), ("inv1", INV), ("a", LOW), ("n2", LOW), ("h2", LOW), ("inv2", INV), ("g", WIDE), ("slope", WIDE))
GATHERS = ((0, 0, 16, 0), (0, 16, 32, 1), (0, 32, 48, 2), (0, 48, 128, 4), (0, 128, 192, 6), (1, 0, 64, 8), (1, 64, 128, 10), (1, 128, 192, 12))
PIECES = ((0, 48), (48, 64), (64, 128), (128, 192))
SCATTERS = ((0, 80), (80, 144))


def take_rows(src, dst):
    def fn(at):
        spread(dst, at, src[at, :].astype(F32))
    by_tiles(fn)


def give_rows(src, dst):
    def fn(at):
        dst[at, :] = full(src, at).astype(dst.dtype)
    by_tiles(fn)


def split_rows(flat, packs):
    def row(name, at, first, c):
        val = flat[name][:, pl.ds(pl.multiple_of(at * 512, 512), 512)].astype(F32)
        for layer in range(2):
            packs[layer][pl.ds(first, 1), :] = val[layer:layer + 1, :]
        return c

    def narrow(i, c):
        for j in range(3):
            row("qkv", 3 * i + j, 16 * j + i, c)
        row("proj", i, 48 + i, c)
        for j in range(4):
            row("fc1", 4 * i + j, 64 + 16 * j + i, c)
            row("fc2", 4 * i + j, 128 + 4 * i + j, c)
        return c
    lax.fori_loop(0, 16, narrow, 0)


def join_rows(layer, outs, fc, q):
    def put(name, at, val):
        outs[name][layer:layer + 1, pl.ds(pl.multiple_of(at * 512, 512), 512)] = val

    def body(i, c):
        if q is not None:
            for j in range(3):
                put("qkv", 3 * i + j, q[pl.ds(16 * j + i, 1), :])
        if fc is not None:
            put("proj", i, fc[pl.ds(i, 1), :])
            for j in range(4):
                put("fc1", 4 * i + j, fc[pl.ds(16 + 16 * j + i, 1), :])
                put("fc2", 4 * i + j, fc[pl.ds(80 + 4 * i + j, 1), :])
        return c
    lax.fori_loop(0, 16, body, 0)


FLAT = (("qkv", 24576), ("proj", 8192), ("fc1", 32768), ("fc2", 32768), ("small", 1152))


def mask_rows(ref, sz):
    def body(t, c):
        lg, y = t // GRID, t % GRID
        for ig in range(2):
            size = sz[8 * ig:8 * ig + 8, :]
            for x in range(GRID):
                at = at_cell(y, x, ig)
                ref[lg, at, :] = jnp.where(size > jnp.maximum(y, x), ref[lg, at, :], 0.0)
        return c
    lax.fori_loop(0, 4 * GRID, body, 0)


class Copies:
    def __init__(self, sems):
        self.sems, self.used, self.open = sems, 0, {}

    def start(self, name, src, dst):
        at = self.used
        self.used += 1
        self.open[name] = lambda: pltpu.make_async_copy(src, dst, self.sems.at[at])
        self.open[name]().start()

    def wait(self, *names):
        for name in names:
            self.open.pop(name)().wait()

    def wait_all(self, prefix):
        for name in [n for n in self.open if n.startswith(prefix)]:
            self.wait(name)


class Idle:
    def __call__(self):
        pass

    def upto(self, count):
        pass

    def finish(self):
        pass


COPIES = 80
ROWS6 = (slice(None),) * 4


def step_kernel(comm, names, *refs):
    r = dict(zip(names, refs))
    cps = Copies(r["cs"])
    sz, W, tab, b1 = r["sz"], r["W"], r["tab"], r["b1"]
    gsum, gb1, gfc, gq, gsm, tau = r["gsum"], r["gb1"], r["gfc"], r["gq"], r["gsm"], r["tau"]
    whbm = (r["w0"], r["w1"])
    n1, h1, inv1, a_low = r["n1"], r["h1"], r["inv1"], r["a"]
    xa, xb, da, dxb = r["xa"], r["xb"], r["da"], r["dxb"]
    pv, pr = r["pv"], r["pr"]
    y = pv.at[pl.ds(3 * PROW, D)]
    zero_padded(pv)
    zero_padded(pr)
    scope = pl.run_scoped

    def vm(*shapes):
        return [pltpu.VMEM(*sh) for sh in shapes]

    def load_piece(layer, i):
        a, b = PIECES[i]
        cps.start(f"W{i}", whbm[layer].at[ROWS6 + (pl.ds(a, b - a),)], W.at[ROWS6 + (pl.ds(a, b - a),)])

    STAGE = pltpu.VMEM((R, D), BF16)

    if comm:
        place = Place(4)
        here = (place.c, place.z, place.x, place.y)
        for name, _ in FLAT:
            cps.start("flat" + name, r[name], r["st_" + name])
        for i in range(NI):
            sz[i:i + 1, :] = jnp.full((1, 128), r["sizes"][i], jnp.int32)
        cps.wait("flatsmall")
        r["osm"][...] = jnp.zeros((32, 128), F32)
        for i in range(9):
            val = r["st_small"][:, 128 * i:128 * i + 128].astype(F32)
            for layer in range(2):
                r["osm"][16 * layer + i:16 * layer + i + 1, :] = val[layer:layer + 1, :]
        cps.start("own2", r["osm"], r["gs"].at[here])
        greet(place)
        send, recv = r["as"], r["ar"]
        tiny = Ticker([(0, lambda: gather_ticks(Place(4), r["gs"], slice(None), send.at[0], recv.at[0]))])
        lists = []
        for n, (layer, a, b, first) in enumerate(GATHERS):
            lists.append((first, lambda n=n, layer=layer, a=a, b=b: gather_ticks(Place(4), whbm[layer], pl.ds(a, b - a), send.at[1 + n], recv.at[1 + n])))
        tick = Ticker(lists)
        cps.wait("own2")
        tiny()

        def pack_shards(p0, p1, b0, b1_):
            cps.wait(*("flat" + n for n, _ in FLAT[:4]))
            split_rows({n: r["st_" + n] for n, _ in FLAT[:4]}, (p0, p1))
            b0[...] = p0[...].astype(BF16)
            b1_[...] = p1[...].astype(BF16)
            cps.start("own0", b0, r["w0"].at[here])
            cps.start("own1", b1_, r["w1"].at[here])
            tiny()
            cps.wait("own0", "own1")
        scope(pack_shards, *vm(((WROWS, D), F32), ((WROWS, D), F32), ((WROWS, D), BF16), ((WROWS, D), BF16)))
        tick()
        tiny()

        def begin(stage):
            cps.start("images", r["img"], stage)
            cps.wait("images")
            take_rows(stage, xa)
        scope(begin, STAGE)
        tick()
        tiny()
        tick()
        tiny()
        build_tables(r["gs"], 0, tau, y, tab, b1)
        tick()
    else:
        tick = Idle()

        def begin(stage):
            cps.start("images", r["img"], stage)
            cps.wait("images")
            take_rows(stage, xa)
        scope(begin, STAGE)

    def forward(layer, xin, x1, keep):
        t = tab.at[layer]
        fwd_conv1(xin, sz, t, x1, pv)
        if layer == 0:
            tick()
        norm_phase(x1, t, 0, 1, n1, h1, inv1)
        tick.upto(7 if layer == 0 else 13)
        load_piece(layer, 0)
        if layer == 0:
            for name in ("n1", "h1", "inv1"):
                cps.start("out0" + name, r[name], r["park0" + name])
            if comm:
                build_tables(r["gs"], 1, tau, y, tab, b1)
        else:
            load_piece(1, 1)
        cps.wait("W0")

        def attention(q, p, v, rel, f, s):
            def park(name, ref):
                cps.start(f"park{layer}{name}", ref, r[f"park{layer}{name}"])
            fwd_qkv(h1, W, t, q, p, v)
            park("q", q)
            park("v", v)
            fwd_softmax(p, sz)
            park("p", p)
            if layer == 1:
                tick()
            fwd_attn(q, p, v, s, f)
            park("s", s)
            tick()
            if layer == 1:
                load_piece(1, 2)
            fwd_conv3(v, q, f, sz, t, rel, pv, 1, 0)
            fwd_conv3(v, q, f, sz, t, rel, pv, 2, 1)

            def wide(i, c):
                fwd_conv3(v, q, f, sz, t, rel, pv, 3, i + 2)
                return c
            lax.fori_loop(0, 2, wide, 0)
            park("rel", rel)
            tick()
            if layer == 0:
                load_piece(0, 1)
                load_piece(0, 2)
            cps.wait("W1")
            fwd_proj(f, W, t, x1, a_low)
            cps.wait_all(f"park{layer}")
        scope(attention, *vm(L4, L4, L4, REL, L4, SUMM))
        if layer == 0:
            cps.start("out0a", a_low, r["park0a"])

        def mlp(g, slope, n2, h2, inv2, dm):
            norm_phase(x1, t, 2, 3, n2, h2, inv2)
            if layer == 0:
                tick()
            cps.wait("W2")
            fwd_fc1(h2, W, b1.at[layer], g, slope)
            if layer == 0:
                for name, ref in (("g", g), ("slope", slope), ("n2", n2), ("h2", h2), ("inv2", inv2)):
                    cps.start("out0" + name, ref, r["park0" + name])
                tick.upto(11)
                load_piece(0, 3)
            else:
                tick.upto(17)
                load_piece(1, 3)
            cps.wait("W3")
            fwd_fc2(g, W, t, x1)
            if layer == 0:
                tick()
                cps.wait_all("out0")
            else:
                keep(g, slope, n2, h2, inv2, dm)
        scope(mlp, *vm(WIDE, WIDE, LOW, LOW, INV, LOW))

    events = {}

    def at(layer, point):
        for event in events.get((layer, point), ()):
            event()

    def first_half(layer, dx, da, g, slope, n2, h2, inv2, dm):
        t = tab.at[layer]
        gsum[...] = jnp.zeros_like(gsum)
        bwd_cast_sum(dx, dm, gsum, 7)
        if layer == 0:
            cps.wait("in0slope", "W3")
        bwd_du(dm, W, slope, gb1)
        at(layer, "e0")
        if layer == 0:
            cps.wait("in0g")
        wgrad2(g, dm, gfc, 80)
        at(layer, "e1")
        if layer == 0:
            cps.wait("in0h2", "W2")
        wgrad(h2, slope, gfc, 16, 4)
        at(layer, "e2")
        mm_nt(slope, slice(None), W, 4, 4, da)
        at(layer, "e3")
        if layer == 0:
            cps.wait("in0n2", "in0inv2", "in0a", "W1")
        norm_back_phase(da, n2, inv2, t, 2, dx, dm, gsum, 2, 3, 6)
        at(layer, "e4")
        wgrad(a_low, dm, gfc, 0, 1)
        at(layer, "e5")
        mm_nt(dm, slice(None), W, 3, 1, da)
        zero_tail(da)

    def second_half(layer, xin, dx, da, dv, end):
        t = tab.at[layer]

        def run(q, p, v, rel, dq, dk, s, dj):
            for name, ref in (("q", q), ("p", p), ("v", v), ("s", s), ("rel", rel)):
                cps.start(f"in{layer}" + name, r[f"park{layer}{name}"], ref)
            at(layer, "f0")
            cps.wait(*(f"in{layer}" + n for n in ("q", "p", "v", "s")))
            bwd_attn1(q, p, v, s, da, dq, dv, dk)
            at(layer, "f1")
            cps.wait(f"in{layer}rel")
            bwd_mix(q, p, v, rel, da, dq, dv, dk, sz, t, gsum, pv, pr, 1, 0)
            at(layer, "f2")
            bwd_mix(q, p, v, rel, da, dq, dv, dk, sz, t, gsum, pv, pr, 2, 1)
            at(layer, "f3")

            def wide(i, c):
                bwd_mix(q, p, v, rel, da, dq, dv, dk, sz, t, gsum, pv, pr, 3, i + 2)
                return c
            lax.fori_loop(0, 2, wide, 0)
            at(layer, "f4")
            bwd_cast(dq, dk, dv, dj)
            if layer == 0:
                cps.wait("W0", "in0h1")
            wgrad(h1, dj, gq, 0, 3)
            at(layer, "f5")
            mm_nt(dj, slice(0, 1536), W, 0, 3, dq)
            at(layer, "f6")
            if layer == 0:
                cps.wait("in0n1", "in0inv1")
            norm_back_phase(dq, n1, inv1, t, 0, dx, None, gsum, 0, 1, None)
            at(layer, "f7")
        scope(run, *vm(L4, L4, L4, REL, L4, L4, SUMM, ((R, 3 * D), BF16)))
        end()
        at(layer, "f8")
        bwd_conv1(xin, dx, da, sz, t, gsum, pv, pr)
        at(layer, "f9")
        build_small(gsum, gb1, y, tau, gsm)
        at(layer, "f10")

    if comm:
        def scatter(n, g, rows, out, which):
            bufs = r["bufs"][4 * which:4 * which + 4]
            return Ticker([(0, lambda: scatter_ticks(Place(4), g, rows, *bufs, out, r["rs"].at[n], r["rr"].at[n]))])

        def release(which):
            def run():
                place = Place(4)
                far = [place.dev(z=place.off(k)) for k in range(1, 4)]
                near = [place.dev(x=1 - place.x), place.dev(y=1 - place.y), place.dev(c=1 - place.c)]
                for who in far + near:
                    pl.semaphore_signal(r["cr"].at[which], inc=1, device_id=who, device_id_type=MESH)
            return run

        def claim(which):
            return lambda: pl.semaphore_wait(r["cr"].at[which], 6)
        fa, fb, qt, st = {}, {}, {}, {}
        for layer in (0, 1):
            (a0, b0), (a1, b1_) = SCATTERS
            out = r[f"sfc{layer}"]
            fa[layer] = scatter(4 * layer, gfc, pl.ds(a0, b0 - a0), out.at[pl.ds(a0, b0 - a0)], 0)
            fb[layer] = scatter(4 * layer + 1, gfc, pl.ds(a1, b1_ - a1), out.at[pl.ds(a1, b1_ - a1)], 1)
            qt[layer] = scatter(4 * layer + 2, gq, slice(None), r[f"sq{layer}"], 2)
            st[layer] = scatter(4 * layer + 3, gsm, slice(None), r[f"ss{layer}"], 3)
        for layer in (0, 1):
            A, B, Q = fa[layer], fb[layer], qt[layer]
            events.update({
                (layer, "e1"): [B], (layer, "e3"): [B], (layer, "e5"): [A], (layer, "f1"): [B, A], (layer, "f3"): [B, A], (layer, "f4"): [B, A],
                (layer, "f5"): [Q], (layer, "f7"): [A, Q], (layer, "f9"): [Q], (layer, "f10"): [st[layer]]})
        events[1, "f7"].append(release(0))
        events[0, "e0"] = [qt[1], st[1]]
        events[0, "e1"] = [qt[1], st[1], claim(0), fb[0]]
        events[0, "e2"] = [st[1]]
        events[0, "e3"] = [st[1], release(1), fb[0]]
        events[0, "f5"] = [claim(1), qt[0]]
    else:
        def put(name, src):
            return lambda: cps.start(name, src, r[name])
        events.update({
            (1, "f0"): [put("gfc1", gfc)], (1, "f4"): [lambda: cps.wait("gfc1")], (1, "f5"): [put("gq1", gq)], (1, "f10"): [put("gsm1", gsm)],
            (0, "e0"): [lambda: cps.wait("gq1", "gsm1")], (0, "f0"): [put("gfc0", gfc)], (0, "f5"): [put("gq0", gq)], (0, "f10"): [put("gsm0", gsm)],
        })

    forward(0, xa, xb, None)

    def top(g, slope, n2, h2, inv2, dm):
        def emit(stage, stage2):
            cps.start("cot", r["ct"], stage)
            mask_rows(xa, sz)
            give_rows(xa, stage2)
            cps.start("out", stage2, r["output"])
            cps.wait("cot")
            take_rows(stage, dxb)
            mask_rows(dxb, sz)
            cps.wait("out")
        scope(emit, STAGE, STAGE)
        first_half(1, dxb, da, g, slope, n2, h2, inv2, dm)
    forward(1, xb, xa, top)

    for i in (1, 2, 3):
        load_piece(0, i)
    cps.start("in0a", r["park0a"], a_low)

    def end1():
        load_piece(0, 0)
        for name, ref in (("h1", h1), ("n1", n1), ("inv1", inv1)):
            cps.start("in0" + name, r["park0" + name], ref)
    second_half(1, xb, dxb, da, xa, end1)

    def bottom(g, slope, n2, h2, inv2, dm):
        for name, ref in (("slope", slope), ("g", g), ("h2", h2), ("n2", n2), ("inv2", inv2)):
            cps.start("in0" + name, r["park0" + name], ref)
        first_half(0, da, dxb, g, slope, n2, h2, inv2, dm)
    scope(bottom, *vm(WIDE, WIDE, LOW, LOW, INV, LOW))

    def end0():
        def again(stage):
            cps.start("again", r["img"], stage)
            cps.wait("again")
            take_rows(stage, xb)
        scope(again, STAGE)
    second_half(0, xb, da, dxb, xa, end0)

    def last(stage3, *flat):
        give_rows(dxb, stage3)
        cps.start("dx", stage3, r["gi"])
        if not comm:
            cps.wait("gfc0", "gq0", "gsm0", "dx")
            return
        o = dict(zip([n for n, _ in FLAT], flat))
        st[0]()
        join_rows(1, o, r["sfc1"], r["sq1"])
        qt[0]()
        st[0]()
        join_rows(0, o, r["sfc0"], None)
        qt[0]()
        st[0]()
        join_rows(0, o, None, r["sq0"])
        for name, _ in FLAT[:4]:
            cps.start("g" + name, o[name], r["g_" + name])
        st[0].finish()
        for layer in (0, 1):
            for i in range(9):
                o["small"][layer:layer + 1, 128 * i:128 * i + 128] = r[f"ss{layer}"][i:i + 1, :]
        cps.start("gsmall", o["small"], r["g_small"])
        cps.wait("dx", *("g" + n for n, _ in FLAT))
    scope(last, pltpu.VMEM((R, D), F32), *([pltpu.VMEM((2, n), F32) for _, n in FLAT] if comm else []))


def step(comm, images, cotangent, sz, *more):
    vmem = pltpu.VMEM
    if comm:
        inputs = ["img", "ct", "sizes"] + [n for n, _ in FLAT]
        in_specs = [ANY, ANY, pl.BlockSpec(memory_space=pltpu.SMEM)] + [ANY] * 5
    else:
        inputs = ["img", "ct", "sz", "w0", "w1", "tab", "b1"]
        in_specs = [ANY, ANY, VM, ANY, ANY, VM, VM]
    outs = [("output", sd((R, D), BF16), ANY), ("gi", sd((R, D), F32), ANY)]
    shares = []
    if comm:
        shares = [("g_" + n, sd((2, count), F32), ANY) for n, count in FLAT]
    for layer in (0, 1):
        if not comm:
            shares += [(f"gfc{layer}", packed(144), ANY), (f"gq{layer}", packed(48), ANY), (f"gsm{layer}", packed(16, 128, F32), ANY)]
    outs += shares
    outs += [(f"park0{n}", sd(*sh), ANY) for n, sh in PARK0] + [(f"park1{n}", sd(*sh), ANY) for n, sh in PARK]
    if comm:
        outs += [("w0", packed(WROWS), ANY), ("w1", packed(WROWS), ANY)]
    scratch = [("W", vmem((2, 4, 2, 2, WROWS, D), BF16)), ("gfc", vmem((2, 4, 2, 2, 144, D), BF16)), ("gq", vmem((2, 4, 2, 2, 48, D), BF16)),
               ("gsm", vmem((2, 4, 2, 2, 16, 128), F32)), ("gsum", vmem((4, TROWS, 128), F32)), ("gb1", vmem((8, FF), F32)),
               ("tau", vmem((288, 128), F32)), ("pv", vmem(PADDED, F32)), ("pr", vmem(PADDED, F32)), ("n1", vmem(*LOW)), ("h1", vmem(*LOW)), ("inv1", vmem(*INV)), ("a", vmem(*LOW))]
    scratch += [(n, vmem(*L4)) for n in ("xa", "xb", "da", "dxb")] + [("cs", pltpu.SemaphoreType.DMA((COPIES,)))]
    bufs = []
    if comm:
        sems = pltpu.SemaphoreType.DMA
        for layer in (0, 1):
            scratch += [(f"sfc{layer}", vmem((144, D), F32)), (f"sq{layer}", vmem((48, D), F32)), (f"ss{layer}", vmem((16, 128), F32))]
        scratch += [("st_" + n, vmem((2, count), BF16)) for n, count in FLAT] + [("osm", vmem((32, 128), F32)), ("sz", vmem((NI, 128), jnp.int32))]
        scratch += [("tab", vmem((2, 4, TROWS, 128), F32)), ("b1", vmem((2, 16, 128), F32)), ("gs", vmem((2, 4, 2, 2, 32, 128), F32)),
                    ("as", sems((9, 8))), ("ar", sems((9, 8))), ("rs", sems((8, 8))), ("rr", sems((8, 8))), ("cr", pltpu.SemaphoreType.REGULAR((2,)))]
        for rows, width, dt in ((80, D, BF16), (64, D, BF16), (48, D, BF16), (16, 128, F32)):
            bufs += scatter_bufs(4, rows, width, dt)
    names = inputs + [n for n, _, _ in outs] + [n for n, _ in scratch]

    def kernel(*refs):
        count = len(names)
        r = list(refs[:count])
        step_kernel(comm, names + ["bufs"], *r, refs[count:])
    params = dict(vmem_limit_bytes=67043328)
    if comm:
        params.update(collective_id=0, has_side_effects=True)
    got = pl.pallas_call(
        kernel, out_shape=[o for _, o, _ in outs], in_specs=in_specs, out_specs=[sp for _, _, sp in outs],
        scratch_shapes=[sc for _, sc in scratch] + bufs, compiler_params=pltpu.CompilerParams(**params), name="step",
    )(images, cotangent, sz, *more)
    return got[:2 + len(shares)]


def window_mask():
    channel = lax.broadcasted_iota(jnp.int32, (49, D), 1)
    tap = lax.broadcasted_iota(jnp.int32, (49, D), 0)
    head = channel // (D // HEADS)
    reach = jnp.where(head < 2, 1, jnp.where(head < 5, 2, 3))
    return ((jnp.abs(tap // 7 - 3) <= reach) & (jnp.abs(tap % 7 - 3) <= reach)).astype(F32)


def blocks_of(flat, rows, cols):
    return flat.reshape(rows, cols // D, D).transpose(1, 0, 2).reshape(rows * cols // D, D)


def pack(qkv, proj, fc1, fc2, n):
    per = D // n
    return jnp.concatenate([blocks_of(qkv, per, 3 * D), proj.reshape(per, D), blocks_of(fc1, per, FF), fc2.reshape(FF // n, D)])


def tables(small):
    small = small.astype(F32)
    end = TABLE * D
    tb = small[:end].reshape(D, TABLE).T
    cpe = small[end + FF:].reshape(D, 10).T
    tab = jnp.concatenate([tb[:9], tb[9:] * window_mask(), jnp.zeros((CPE - TABLE, D), F32), cpe, jnp.zeros((TROWS - CPE - 10, D), F32)])
    return tab.reshape(TROWS, 4, 128).transpose(1, 0, 2), small[end:end + FF].reshape(16, 128)


def whole_weights(mine, small, n):
    per = D // n
    full = lax.all_gather(mine[None], AXES, axis=0, tiled=True)
    vec = lax.all_gather(small, AXES, axis=0, tiled=True)
    parts = [full[:, j * per:(j + 1) * per].reshape(32, D // 32, D) for j in range(8)] + [full[:, 8 * per:].reshape(32, FF // 32, D)]
    w = jnp.concatenate(parts, axis=1).reshape(4, 2, 2, 2, WROWS, D).transpose(3, 0, 1, 2, 4, 5)
    return w, *tables(vec)


def share_by_xla(gfc, gq, gsm, n):
    per = D // n

    def rows(a):
        return a.transpose(1, 2, 3, 0, 4, 5).reshape((32,) + a.shape[4:])
    gq, gfc, gsm = rows(gq), rows(gfc), rows(gsm)
    every = jnp.concatenate([gq, gfc[:, :80]], axis=1)
    parts = [every[:, 16 * j:16 * j + 16].reshape(n, per, D) for j in range(8)] + [gfc[:, 80:].reshape(n, FF // n, D)]
    vec = gsm[:, :9].reshape(n, -1)
    width = vec.shape[1]
    parts.append(jnp.pad(vec, ((0, 0), (0, -width % D))).reshape(n, -1, D).astype(BF16))
    share = lax.psum_scatter(jnp.concatenate(parts, axis=1), AXES, scatter_dimension=0, tiled=True)[0].astype(F32)
    mats = split_shares(share[:8 * per + FF // n], per)
    return (*mats, share[8 * per + FF // n:].reshape(-1)[:width])


def split_shares(share, per):
    def cols(first, count):
        return share[first * per:(first + count) * per].reshape(count, per, D).transpose(1, 0, 2).reshape(-1)
    return cols(0, 3), cols(3, 1), cols(4, 4), share[8 * per:].reshape(-1)


def shards(n, images, grid_sizes, qkv, proj, fc1, fc2, small, cotangent):
    layers = qkv.shape[0]
    images = images.transpose(1, 0, 2).reshape(R, D)
    cotangent = cotangent.transpose(1, 0, 2).reshape(R, D)
    if n == 32:
        output, dx, *grads = step(True, images, cotangent, grid_sizes, qkv, proj, fc1, fc2, small)
    else:
        sz = jnp.broadcast_to(grid_sizes[:, None], (NI, 128))
        mine = [pack(qkv[l], proj[l], fc1[l], fc2[l], n) for l in range(layers)]
        held = [whole_weights(mine[l], small[l], n) for l in range(layers)]
        output, dx, *got = step(False, images, cotangent, sz, held[0][0], held[1][0], jnp.stack([held[0][1], held[1][1]]), jnp.stack([held[0][2], held[1][2]]))
        shares = [share_by_xla(*got[:3], n), share_by_xla(*got[3:], n)]
        grads = [jnp.stack([shares[l][i] for l in range(layers)]) for i in range(5)]
    output, dx = (a.reshape(SLOT, NI, D).transpose(1, 0, 2) for a in (output, dx))
    return (output, dx, *grads)


def solution(mesh):
    n = mesh.shape["wide"] * mesh.shape["narrow"]
    from jax.sharding import PartitionSpec as P
    rows, flat = P(AXES, None, None), P(None, AXES)
    return jax.shard_map(
        functools.partial(shards, n), mesh=mesh,
        in_specs=(rows, P(AXES), flat, flat, flat, flat, flat, rows),
        out_specs=(rows, rows, flat, flat, flat, flat, flat),
        check_vma=False)
```

```python
import functools
import jax
import jax.numpy as jnp
from jax import lax
from jax.experimental import pallas as pl
from jax.experimental.pallas import tpu as pltpu

F32, BF16 = jnp.float32, jnp.bfloat16
D, FF, HEADS, GRID, SLOT = 512, 2048, 8, 9, 82
TABLE = 58
EPS = 1e-6
NI = 16
R = SLOT * NI
PADS = 96
RP = PADS * NI
RADII = (1, 2, 3, 3)
AXES = ("wide", "narrow")
WROWS = 192
TAPS, CPE, CPEB, TROWS = 9, 64, 73, 80


def ds(start, size, align=8):
    if not isinstance(start, int):
        start = pl.multiple_of(start, align)
    return pl.ds(start, size)


def row8(ref, i, lg):
    return ref[lg, pl.ds(i, 8, stride=0), :]


def row(tab, i, j=None):
    parts = range(4) if j is None else (2 * j, 2 * j + 1)
    return jnp.concatenate([tab[g, i:i + 1, :] for g in parts], axis=1)


def put2(ref, at, j, val):
    ref[2 * j, at, :] = val[:, :128]
    ref[2 * j + 1, at, :] = val[:, 128:]


def cell(y, x, ig):
    return ds((1 + GRID * y + x) * NI + 8 * ig, 8)


def inside_at(sz, y, x):
    return sz > max(y, x)


PROW = GRID * NI
PADDED = ((GRID + 6) * PROW, 128)


def at_cell(y, x, ig):
    return pl.ds(pl.multiple_of((1 + GRID * y + x) * NI + 8 * ig, 8), 8)


def at_padded(y, x, ig):
    return pl.ds(pl.multiple_of((y + 3) * PROW + x * NI + 8 * ig, 8), 8)


def rows_loop(fn, init):
    return lax.fori_loop(0, GRID, fn, init)


def groups(fn):
    def run(ig, c):
        fn(ig)
        return c
    lax.fori_loop(0, 2, run, 0)


def lane_groups(fn):
    fn(1, 0)
    fn(2, 1)

    def run(i, c):
        fn(3, i + 2)
        return c
    lax.fori_loop(0, 2, run, 0)


def conv_pass(src, load_tap, radius, ig, emit, init, flip=False):
    span = range(-radius, radius + 1)

    def body(y, carry):
        acc = [None] * GRID
        for a in span:
            line = [src[at_padded(y - a if flip else y + a, x, ig), :] for x in range(GRID)]
            for b in span:
                tap = load_tap(a, b)
                for x in range(GRID):
                    xx = x - b if flip else x + b
                    if 0 <= xx < GRID:
                        term = line[xx] * tap
                        acc[x] = term if acc[x] is None else acc[x] + term
        return emit(y, acc, carry)
    return rows_loop(body, init)


def conv_kgrad(grad, src, radius, emit):
    span = range(-radius, radius + 1)
    rows = list(span)
    for part in (rows[:4], rows[4:]):
        if not part:
            continue

        def body(t, acc):
            y, ig = t // 2, t % 2
            acc = list(acc)
            up = [grad[at_padded(y, x, ig), :] for x in range(GRID)]
            for i, a in enumerate(part):
                line = [src[at_padded(y + a, x, ig), :] for x in range(GRID)]
                for j, b in enumerate(span):
                    k = i * len(span) + j
                    for x in range(GRID):
                        if 0 <= x + b < GRID:
                            acc[k] = acc[k] + up[x] * line[x + b]
            return tuple(acc)
        zero = jnp.zeros((8, 128), F32)
        sums = lax.fori_loop(0, 2 * GRID, body, (zero,) * (len(part) * len(span)), unroll=2)
        for i, a in enumerate(part):
            for j, b in enumerate(span):
                emit(a, b, sums[i * len(span) + j])


def zero_padded(ref):
    ref[...] = jnp.zeros(PADDED, F32)


def fill_padded(dst, src, lg, sz):
    def body(t, c):
        y, ig = t // 2, t % 2
        size = sz[ds(8 * ig, 8), :]
        for x in range(GRID):
            dst[at_padded(y, x, ig), :] = jnp.where(size > jnp.maximum(y, x), src[lg, at_cell(y, x, ig), :], 0.0)
        return c
    lax.fori_loop(0, 2 * GRID, body, 0)


def norm_rows(x):
    mean = jnp.mean(x, axis=-1, keepdims=True)
    cen = x - mean
    inv = lax.rsqrt(jnp.mean(cen * cen, axis=-1, keepdims=True) + EPS)
    return cen * inv, inv


def dot(a, b, ca, cb):
    return lax.dot_general(a, b, (((ca,), (cb,)), ((), ())), preferred_element_type=F32)


def head_mask():
    r = lax.broadcasted_iota(jnp.int32, (256, 256), 0) // 64
    c = lax.broadcasted_iota(jnp.int32, (256, 256), 1) // 64
    return r == c


def by_tiles(fn):
    def body(i, c):
        fn(pl.ds(pl.multiple_of(i * 256, 256), 256))
        return c
    lax.fori_loop(0, R // 256, body, 0)
    if R % 256:
        fn(pl.ds(R // 256 * 256, R % 256))


def full(ref, at):
    return jnp.concatenate([ref[g, at, :] for g in range(4)], axis=1)


def spread(ref, at, val):
    for g in range(4):
        ref[g, at, :] = val[:, 128 * g:128 * g + 128]


def fwd_conv1(x, sz, tab, x1, pv):
    def one(lg, c):
        fill_padded(pv, x, lg, sz)

        def group(ig):
            size = sz[ds(8 * ig, 8), :]
            x1[lg, ds(8 * ig, 8), :] = x[lg, ds(8 * ig, 8), :]
            bias = row8(tab, CPEB, lg)

            def emit(y, acc, carry):
                for k in range(GRID):
                    at = at_cell(y, k, ig)
                    x1[lg, at, :] = x[lg, at, :] + jnp.where(size > jnp.maximum(y, k), acc[k] + bias, 0.0)
                return carry
            conv_pass(pv, lambda a, b: row8(tab, CPE + (a + 1) * 3 + b + 1, lg), 1, ig, emit, 0)
        groups(group)
        return c
    lax.fori_loop(0, 4, one, 0)


def norm_phase(src, tab, gain, shift, hat, low, inv_ref):
    def fn(at):
        n, inv = norm_rows(full(src, at))
        hat[at, :] = n.astype(BF16)
        low[at, :] = (n * row(tab, gain) + row(tab, shift)).astype(BF16)
        inv_ref[at, :] = jnp.broadcast_to(inv, (n.shape[0], 128))
    by_tiles(fn)


def weight(g, block, first, count, cols):
    at = ds(16 * block, 16, 16)
    return jnp.concatenate([g[t % 2, t // 8, t // 4 % 2, t // 2 % 2, at, cols] for t in range(first // 16, (first + count) // 16)], axis=0)


def weight2(g, chunk, cols):
    return jnp.concatenate([g[i % 2, chunk, i // 4, i // 2 % 2, 128:192, cols] for i in range(8)], axis=0)


def halves(fn):
    def body(i, c):
        fn(pl.ds(pl.multiple_of(i // 2 * (R // 2), 16), R // 2), i % 2)
        return c
    lax.fori_loop(0, 4, body, 0)


def cols256(j):
    return pl.ds(pl.multiple_of(j * 256, 256), 256)


def both_lanes(ref, at, j):
    return jnp.concatenate([ref[2 * j, at, :], ref[2 * j + 1, at, :]], axis=1)


def zero_tail(ref):
    ref[:, R:RP, :] = jnp.zeros((4, RP - R, 128), F32)


def fwd_qkv(low, w, tab, q, k, v):
    def fn(at, j):
        h = low[at, :]
        for b, (ref, bias) in enumerate(((q, 4), (k, None), (v, 5))):
            val = dot(h, weight(w, b, 0, D, cols256(j)), 1, 0)
            put2(ref, at, j, val if bias is None else val + row(tab, bias, j))
    halves(fn)
    for ref in (q, k, v):
        zero_tail(ref)


def each_pos(size, ig, fn):
    fn(ds(8 * ig, 8), None)
    for y in range(GRID):
        for x in range(GRID):
            fn(cell(y, x, ig), inside_at(size, y, x))


def fwd_softmax(k, sz):
    def body(i, c):
        lg, ig = i // 2, i % 2
        size = sz[ds(8 * ig, 8), :]
        best = [None] * 4
        cnt = [0]

        def first(at, ok):
            val = k[lg, at, :]
            if ok is not None:
                val = jnp.where(ok, val, -1e30)
            j = cnt[0] % 4
            best[j] = val if best[j] is None else jnp.maximum(best[j], val)
            cnt[0] += 1
        each_pos(size, ig, first)
        top = jnp.maximum(jnp.maximum(best[0], best[1]), jnp.maximum(best[2], best[3]))
        total = [None] * 4
        cnt[0] = 0

        def second(at, ok):
            val = jnp.exp(k[lg, at, :] - top)
            if ok is not None:
                val = jnp.where(ok, val, 0.0)
            k[lg, at, :] = val
            j = cnt[0] % 4
            total[j] = val if total[j] is None else total[j] + val
            cnt[0] += 1
        each_pos(size, ig, second)
        scale = 1.0 / ((total[0] + total[1]) + (total[2] + total[3]))

        def third(at, ok):
            k[lg, at, :] = k[lg, at, :] * scale
        each_pos(size, ig, third)
        return c
    lax.fori_loop(0, 8, body, 0)


def img_load(ref, i, half):
    return jnp.concatenate([ref[2 * half + j, pl.ds(i, PADS, stride=NI), :] for j in range(2)], axis=1)


def img_store(ref, i, half, val):
    for j in range(2):
        ref[2 * half + j, pl.ds(i, PADS, stride=NI), :] = val[:, 128 * j:128 * j + 128]


def fwd_attn(q, p, v, s, f):
    def body(t, c):
        i, half = t // 2, t % 2
        pi = img_load(p, i, half).astype(BF16)
        vi = img_load(v, i, half).astype(BF16)
        summ = jnp.where(head_mask(), dot(pi, vi, 0, 0), 0.0).astype(BF16)
        s[t] = (summ[0:64] + summ[64:128]) + (summ[128:192] + summ[192:256])
        qi = img_load(q, i, half).astype(BF16)
        img_store(f, i, half, dot(qi, summ, 1, 0) * 0.125)
        return c
    lax.fori_loop(0, 2 * NI, body, 0, unroll=4)


def fwd_conv3(v, q, f, sz, tab, rel, pv, radius, lg):
    fill_padded(pv, v, lg, sz)
    bias = row8(tab, 8, lg)

    def group(ig):
        size = sz[ds(8 * ig, 8), :]

        def emit(y, acc, carry):
            for k in range(GRID):
                at = at_cell(y, k, ig)
                r = acc[k] + bias
                rel[lg, at, :] = r
                f[lg, at, :] = f[lg, at, :] + jnp.where(size > jnp.maximum(y, k), q[lg, at, :] * r, 0.0)
            return carry
        conv_pass(pv, lambda a, b: row8(tab, TAPS + (a + 3) * 7 + b + 3, lg), radius, ig, emit, 0)
    groups(group)


def fwd_proj(att, w, tab, x1, a_low):
    def low(at):
        a_low[at, :] = full(att, at).astype(BF16)
    by_tiles(low)

    def fn(at, j):
        put2(x1, at, j, both_lanes(x1, at, j) + dot(a_low[at, :], weight(w, 3, 0, D, cols256(j)), 1, 0) + row(tab, 6, j))
    halves(fn)


def normal_cdf(u):
    t = 1.0 / (1.0 + jnp.abs(u) * (0.3275911 * 0.7071067811865476))
    e = jnp.exp(-0.5 * u * u)
    poly = t * (0.5 * 0.254829592 + t * (0.5 * -0.284496736 + t * (0.5 * 1.421413741 + t * (0.5 * -1.453152027 + t * (0.5 * 1.061405429)))))
    tail = poly * e
    return jnp.where(u >= 0, 1.0 - tail, tail), e


def fwd_fc1(low, w, b1, g, slope):
    def body(j, c):
        cols = pl.ds(pl.multiple_of(j * 512, 512), 512)
        bias = jnp.concatenate([b1[pl.ds(4 * j + i, 1), :] for i in range(4)], axis=1)
        u = dot(low[...], weight(w, 4 + j, 0, D, slice(None)), 1, 0) + bias
        cdf, e = normal_cdf(u)
        g[:, cols] = (u * cdf).astype(BF16)
        slope[:, cols] = (cdf + u * e * 0.3989422804014327).astype(BF16)
        return c
    lax.fori_loop(0, 4, body, 0)


def fwd_fc2(g, w, tab, x1):
    def fn(at, j):
        wide = jnp.concatenate([weight2(w, c, cols256(j)) for c in range(4)], axis=0)
        put2(x1, at, j, both_lanes(x1, at, j) + dot(g[at, :], wide, 1, 0) + row(tab, 7, j))
    halves(fn)


def fold_rows(val):
    parts = [val[8 * i:8 * i + 8] for i in range(val.shape[0] // 8)]
    while len(parts) > 1:
        parts = [a + b for a, b in zip(parts[::2], parts[1::2])] + parts[len(parts) // 2 * 2:]
    return parts[0]


def add_rows(ref, row, val):
    total = jnp.sum(fold_rows(val), axis=0, keepdims=True)
    for g in range(4):
        ref[g, row:row + 1, :] += total[:, 128 * g:128 * g + 128]


def add_sum(ref, lg, row, val):
    ref[lg, row:row + 1, :] += jnp.sum(val, axis=0, keepdims=True)


def bwd_cast_sum(dx, low, gsum, row):
    def fn(at):
        val = full(dx, at).astype(BF16)
        low[at, :] = val
        add_rows(gsum, row, val.astype(F32))
    by_tiles(fn)


def bwd_du(dm, w, slope, gb1):
    def body(j, c):
        cols = pl.ds(pl.multiple_of(j * 512, 512), 512)
        d = dot(dm[...], weight2(w, j, slice(None)), 1, 1) * slope[:, cols].astype(F32)
        slope[:, cols] = d.astype(BF16)
        gb1[:, cols] = fold_rows(d)
        return c
    lax.fori_loop(0, 4, body, 0)


def norm_back_phase(up, hat, inv_ref, tab, gain, res, out_low, sums, rg, rs, rb):
    def fn(at):
        u = full(up, at)
        n = hat[at, :].astype(F32)
        e = u * row(tab, gain)
        m1 = jnp.mean(e, axis=-1, keepdims=True)
        m2 = jnp.mean(e * n, axis=-1, keepdims=True)
        d = full(res, at) + inv_ref[at, 0:1] * (e - m1 - n * m2)
        spread(res, at, d)
        add_rows(sums, rg, u * n)
        add_rows(sums, rs, u)
        if out_low is not None:
            low = d.astype(BF16)
            out_low[at, :] = low
            add_rows(sums, rb, low.astype(F32))
    by_tiles(fn)


def mm_nt(a, cols, g, first, blocks, out):
    def fn(at, j):
        def rows(b):
            here = slice(16 * b, 16 * b + 16)
            return jnp.concatenate([g[i % 2, 2 * j + i // 8, i // 4 % 2, i // 2 % 2, here, :] for i in range(16)], axis=0)
        w = jnp.concatenate([rows(first + b) for b in range(blocks)], axis=1)
        put2(out, at, j, dot(a[at, cols], w, 1, 1))
    halves(fn)


def proj_back(dx, g, out):
    def fn(at, j):
        w = jnp.concatenate([g[i % 2, 2 * j + i // 8, i // 4 % 2, i // 2 % 2, 48:64, :] for i in range(16)], axis=0)
        put2(out, at, j, dot(full(dx, at).astype(BF16), w, 1, 1))
    halves(fn)


def wgrad(left, right, gr, first, blocks):
    def body(j, c):
        tile = dot(left[...], right[:, pl.ds(pl.multiple_of(512 * j, 512), 512)], 0, 0).astype(BF16)
        at = pl.ds(pl.multiple_of(first + 16 * j, 16), 16)
        for t in range(32):
            gr[t % 2, t // 8, t // 4 % 2, t // 2 % 2, at, :] = tile[16 * t:16 * t + 16]
        return c
    lax.fori_loop(0, blocks, body, 0)


def wgrad2(left, right, gr, first):
    def body(j, c):
        tile = dot(left[:, pl.ds(pl.multiple_of(512 * j, 512), 512)], right[...], 0, 0).astype(BF16)
        for i in range(8):
            gr[i % 2, j, i // 4, i // 2 % 2, first:first + 64, :] = tile[64 * i:64 * i + 64]
        return c
    lax.fori_loop(0, 4, body, 0)


def bwd_attn1(q, p, v, s, da, dq, dv, dk):
    def body(t, c):
        i, half = t // 2, t % 2
        df = (img_load(da, i, half) * 0.125).astype(BF16)
        wide = s[t]
        wide = jnp.where(head_mask(), jnp.concatenate([wide] * 4, axis=0), jnp.zeros((), BF16))
        qi = img_load(q, i, half).astype(BF16)
        dsum = jnp.where(head_mask(), dot(qi, df, 0, 0), 0.0).astype(BF16)
        img_store(dq, i, half, dot(df, wide, 1, 1))
        pi = img_load(p, i, half).astype(BF16)
        img_store(dv, i, half, dot(pi, dsum, 1, 0))
        vi = img_load(v, i, half).astype(BF16)
        img_store(dk, i, half, dot(vi, dsum, 1, 1))
        return c
    lax.fori_loop(0, 2 * NI, body, 0, unroll=4)


def bwd_mix(q, p, v, rel, da, dq, dv, dk, sz, tab, gsum, pv, pr, radius, lg):
    fill_padded(pv, v, lg, sz)

    def group(ig):
        size = sz[ds(8 * ig, 8), :]
        cls = ds(8 * ig, 8)
        dqc = dq[lg, cls, :]

        def first(y, carry):
            rs, qs, ps = carry
            for x in range(GRID):
                at = at_cell(y, x, ig)
                d = jnp.where(size > jnp.maximum(y, x), da[lg, at, :], 0.0)
                dr = q[lg, at, :] * d
                pr[at_padded(y, x, ig), :] = dr
                dqv = dq[lg, at, :] + rel[lg, at, :] * d
                dq[lg, at, :] = dqv
                rs, qs, ps = rs + dr, qs + dqv, ps + p[lg, at, :] * dk[lg, at, :]
            return rs, qs, ps
        rs, qs, ps = rows_loop(first, (jnp.zeros((8, 128), F32), dqc, p[lg, cls, :] * dk[lg, cls, :]))
        add_sum(gsum, lg, 8, rs)
        add_sum(gsum, lg, 4, qs)
        dk[lg, cls, :] = p[lg, cls, :] * (dk[lg, cls, :] - ps)

        def second(y, carry):
            for x in range(GRID):
                at = at_cell(y, x, ig)
                dk[lg, at, :] = p[lg, at, :] * (dk[lg, at, :] - ps)
            return carry
        rows_loop(second, 0)

        def emit(y, acc, total):
            for x in range(GRID):
                at = at_cell(y, x, ig)
                val = dv[lg, at, :] + jnp.where(size > jnp.maximum(y, x), acc[x], 0.0)
                dv[lg, at, :] = val
                total = total + val
            return total
        add_sum(gsum, lg, 5, conv_pass(pr, lambda a, b: row8(tab, TAPS + (a + 3) * 7 + b + 3, lg), radius, ig, emit, dv[lg, cls, :], True))
    groups(group)

    def emit_tap(a, b, val):
        add_sum(gsum, lg, TAPS + (a + 3) * 7 + b + 3, val)
    conv_kgrad(pr, pv, radius, emit_tap)


def bwd_cast(dq, dk, dv, dj):
    def fn(at):
        for j, ref in enumerate((dq, dk, dv)):
            dj[at, 512 * j:512 * j + 512] = full(ref, at).astype(BF16)
    by_tiles(fn)


def bwd_conv1(x, dx1, dx, sz, tab, gsum, pv, pr):
    def one(lg, c):
        fill_padded(pv, x, lg, sz)
        fill_padded(pr, dx1, lg, sz)

        def group(ig):
            size = sz[ds(8 * ig, 8), :]
            cls = ds(8 * ig, 8)
            dx[lg, cls, :] = dx1[lg, cls, :]

            def emit(y, acc, total):
                for k in range(GRID):
                    at = at_cell(y, k, ig)
                    total = total + pr[at_padded(y, k, ig), :]
                    dx[lg, at, :] = dx1[lg, at, :] + jnp.where(size > jnp.maximum(y, k), acc[k], 0.0)
                return total
            add_sum(gsum, lg, CPEB, conv_pass(pr, lambda a, b: row8(tab, CPE + (a + 1) * 3 + b + 1, lg), 1, ig, emit, jnp.zeros((8, 128), F32), True))
        groups(group)

        def emit_tap(a, b, val):
            add_sum(gsum, lg, CPE + (a + 1) * 3 + b + 1, val)
        conv_kgrad(pr, pv, 1, emit_tap)
        return c
    lax.fori_loop(0, 4, one, 0)


MESH = pl.DeviceIdType.MESH


class Place:
    def __init__(self, line):
        w, m = lax.axis_index("wide"), lax.axis_index("narrow")
        self.line = line
        self.z, self.x, self.y, self.c = w // 2, w % 2, m // 2, m % 2

    def dev(self, z=None, x=None, y=None, c=None):
        z = self.z if z is None else z
        x = self.x if x is None else x
        y = self.y if y is None else y
        c = self.c if c is None else c
        return (z * 2 + x, y * 2 + c)

    def off(self, k):
        return lax.rem(self.z + self.line + k, self.line)


def greet(place):
    barrier = pltpu.get_barrier_semaphore()
    far = [place.dev(z=place.off(k)) for k in range(1, place.line)]
    near = [place.dev(x=1 - place.x), place.dev(y=1 - place.y), place.dev(c=1 - place.c)]
    for who in far + near:
        pl.semaphore_signal(barrier, inc=1, device_id=who, device_id_type=MESH)
    pl.semaphore_wait(barrier, place.line + 2)


def remote(src, dst, send, recv, dev):
    return pltpu.make_async_remote_copy(src_ref=src, dst_ref=dst, send_sem=send, recv_sem=recv, device_id=dev, device_id_type=MESH)


def both(copy):
    copy.wait_send()
    copy.wait_recv()


def by_core(place, a, b):
    def run():
        @pl.when(place.c == 0)
        def _():
            a()

        @pl.when(place.c == 1)
        def _():
            b()
    return run


def gather_ticks(place, g, rows, send, recv):
    n, z, x, y = place.line, place.z, place.x, place.y

    def lines():
        mine = g.at[place.c, z, x, y, rows]
        return [remote(mine, mine, send.at[k - 1], recv.at[k - 1], place.dev(z=place.off(k))) for k in range(1, n)]

    def line_waits():
        for k, cp in enumerate(lines()):
            cp.wait_send()
            got = g.at[place.c, place.off(-k - 1), x, y, rows]
            remote(got, got, send.at[k], recv.at[k], place.dev(z=place.off(1))).wait_recv()

    def parts(core):
        if core == 0:
            return (g.at[0, :, x, y, rows], g.at[0, :, x, :, rows]), (g.at[0, :, x, y, rows], g.at[0, :, x, 1 - y, rows], g.at[0, :, 1 - x, :, rows])
        return (g.at[1, :, x, y, rows], g.at[1, :, :, y, rows]), (g.at[1, :, x, y, rows], g.at[1, :, 1 - x, y, rows], g.at[1, :, :, 1 - y, rows])

    def swap(core, i):
        part = parts(core)[0][i]
        over_y = (core == 0) == (i == 0)
        return remote(part, part, send.at[n - 1 + i], recv.at[n - 1 + i], place.dev(y=1 - y) if over_y else place.dev(x=1 - x))

    def hand(core, i):
        part = parts(core)[1][i]
        return remote(part, part, send.at[n + 1 + i], recv.at[n + 1 + i], place.dev(c=1 - place.c))

    def steps(core):
        def last():
            for i in range(3):
                hand(core, i).wait_send()
                hand(1 - core, i).wait_recv()
        return [lambda: None,
                lambda: (swap(core, 0).start(), hand(core, 0).start()),
                lambda: (both(swap(core, 0)), swap(core, 1).start(), hand(core, 1).start()),
                lambda: (both(swap(core, 1)), hand(core, 2).start()),
                last]
    ticks = [by_core(place, a, b) for a, b in zip(steps(0), steps(1))]

    def first():
        for cp in lines():
            cp.start()

    def second():
        line_waits()
        ticks[1]()
    return [first, second] + ticks[2:]


def add_blocks(pairs):
    for dst, src in pairs:
        dst[...] = (dst[...].astype(F32) + src[...].astype(F32)).astype(dst.dtype)


def scatter_ticks(place, g, rows, cbuf, pbuf, sbuf, zbuf, out, send, recv):
    n, z, x, y, c = place.line, place.z, place.x, place.y, place.c

    def cores():
        return remote(g.at[1 - c, :, :, :, rows], cbuf, send.at[0], recv.at[0], place.dev(c=1 - c))

    def swaps(core):
        over_x, over_y = place.dev(x=1 - x), place.dev(y=1 - y)
        if core == 0:
            return (remote(g.at[0, :, 1 - x, :, rows], pbuf, send.at[1], recv.at[1], over_x),
                    remote(g.at[0, :, x, 1 - y, rows], sbuf, send.at[2], recv.at[2], over_y))
        return (remote(g.at[1, :, :, 1 - y, rows], pbuf, send.at[1], recv.at[1], over_y),
                remote(g.at[1, :, 1 - x, y, rows], sbuf, send.at[2], recv.at[2], over_x))

    def lines():
        return [remote(g.at[c, place.off(k), x, y, rows], zbuf.at[k - 1], send.at[2 + k], recv.at[2 + k], place.dev(z=place.off(k))) for k in range(1, n)]

    def start_cores():
        cores().start()

    def add_cores():
        both(cores())

        def body(t, carry):
            add_blocks([(g.at[c, t // 4, t // 2 % 2, t % 2, rows], cbuf.at[t // 4, t // 2 % 2, t % 2])])
            return carry
        lax.fori_loop(0, 4 * n, body, 0)

    def step1(core):
        def run():
            add_cores()
            swaps(core)[0].start()
        return run

    def step2(core):
        def run():
            both(swaps(core)[0])

            def body(t, carry):
                dst = g.at[0, t // 2, x, t % 2, rows] if core == 0 else g.at[1, t // 2, t % 2, y, rows]
                add_blocks([(dst, pbuf.at[t // 2, t % 2])])
                return carry
            lax.fori_loop(0, 2 * n, body, 0)
            swaps(core)[1].start()
        return run

    def step3(core):
        def run():
            both(swaps(core)[1])

            def body(t, carry):
                add_blocks([(g.at[core, t, x, y, rows], sbuf.at[t])])
                return carry
            lax.fori_loop(0, n, body, 0)
            for cp in lines():
                cp.start()
        return run

    def finish():
        for cp in lines():
            both(cp)
        total = g[c, z, x, y, rows].astype(F32)
        for k in range(n - 1):
            total = total + zbuf[k].astype(F32)
        out[...] = total
    return [start_cores] + [by_core(place, s(0), s(1)) for s in (step1, step2, step3)] + [finish]


def scatter_bufs(line, rows, width, dtype):
    return [pltpu.VMEM(shape + (rows, width), dtype) for shape in ((line, 2, 2), (line, 2), (line,), (line - 1,))]


STEPS = 5


class Ticker:
    def __init__(self, lists):
        depth = max(i for i, _ in lists) + STEPS
        self.rounds = [[(lambda make=make, at=r - i: make()[at]()) for i, make in lists if 0 <= r - i < STEPS] for r in range(depth)]
        self.done = 0

    def upto(self, count):
        while self.done < min(count, len(self.rounds)):
            for t in self.rounds[self.done]:
                t()
            self.done += 1

    def __call__(self):
        self.upto(self.done + 1)

    def finish(self):
        self.upto(len(self.rounds))


def build_tables(gs, layer, tau, y, tab, b1):
    for t in range(32):
        tau[9 * t:9 * t + 9, :] = gs[t % 2, t // 8, t // 4 % 2, t // 2 % 2, 16 * layer:16 * layer + 9, :]
    lane = lax.broadcasted_iota(jnp.int32, (8, 128), 1)

    def run(base, step, width, b):
        first, off = width * b // 128, width * b % 128
        val = tau[pl.ds(base + first, 8, stride=step), :]
        if off:
            val = pltpu.roll(val, 128 - off, 1)
            if off + width > 128:
                more = pltpu.roll(tau[pl.ds(base + first + 1, 8, stride=step), :], 128 - off, 1)
                val = jnp.where(lane < 128 - off, val, more)
        return val
    for b in range(64):
        tb = run(0, 29, TABLE, b)
        cpe = pltpu.roll(run(248, 5, 10, b), 64, 1)
        y[8 * b:8 * b + 8, :] = jnp.where(lane < TABLE, tb, jnp.where((lane >= 64) & (lane < 74), cpe, 0.0))
    r = lax.broadcasted_iota(jnp.int32, (D, D), 0)
    c = lax.broadcasted_iota(jnp.int32, (D, D), 1)
    place = jnp.where(c == 64 * (r % 8) + r // 8, 1.0, 0.0).astype(BF16)
    table = dot(y[...].astype(BF16), place, 0, 0)[:TROWS]
    tap = lax.broadcasted_iota(jnp.int32, (TROWS, D), 0) - TAPS
    head = lax.broadcasted_iota(jnp.int32, (TROWS, D), 1) // 64
    reach = jnp.where(head < 2, 1, jnp.where(head < 5, 2, 3))
    ok = (tap < 0) | (tap >= 49) | ((jnp.abs(tap // 7 - 3) <= reach) & (jnp.abs(tap % 7 - 3) <= reach))
    table = jnp.where(ok, table, 0.0)
    for g in range(4):
        tab[layer, g] = table[:, 128 * g:128 * g + 128]
    b1[layer] = tau[232:248, :]


def build_small(gsum, gb1, y, tau, gsm):
    r = lax.broadcasted_iota(jnp.int32, (D, D), 0)
    c = lax.broadcasted_iota(jnp.int32, (D, D), 1)
    place = jnp.where(c == 64 * (r % 8) + r // 8, 1.0, 0.0).astype(BF16)
    table = full(gsum, slice(None))
    tap = lax.broadcasted_iota(jnp.int32, (TROWS, D), 0) - TAPS
    head = lax.broadcasted_iota(jnp.int32, (TROWS, D), 1) // 64
    reach = jnp.where(head < 2, 1, jnp.where(head < 5, 2, 3))
    ok = (tap < 0) | (tap >= 49) | ((jnp.abs(tap // 7 - 3) <= reach) & (jnp.abs(tap % 7 - 3) <= reach))
    table = jnp.where(ok, table, 0.0)
    table = jnp.concatenate([table, jnp.zeros((128 - TROWS, D), F32)])
    hi = table.astype(BF16)
    mid = (table - hi.astype(F32)).astype(BF16)
    y[...] = dot(place, hi, 1, 1) + dot(place, mid, 1, 1)
    lane = lax.broadcasted_iota(jnp.int32, (8, 128), 1)

    def lay(base, step, width, start):
        for j in range(step):
            out = None
            for b in range(128 * j // width, min(64, -(-128 * (j + 1) // width))):
                first = width * b - 128 * j
                val = y[8 * b:8 * b + 8, :]
                shift = (first - start) % 128
                if shift:
                    val = pltpu.roll(val, shift, 1)
                out = val if out is None else jnp.where(lane >= first, val, out)
            tau[pl.ds(base + j, 8, stride=step), :] = out
    lay(0, 29, TABLE, 0)
    lay(248, 5, 10, CPE)
    for i in range(16):
        tau[232 + i:233 + i, :] = jnp.sum(gb1[:, 128 * i:128 * i + 128], axis=0, keepdims=True)
    for t in range(32):
        gsm[t % 2, t // 8, t // 4 % 2, t // 2 % 2, 0:9, :] = tau[9 * t:9 * t + 9, :]
        gsm[t % 2, t // 8, t // 4 % 2, t // 2 % 2, 9:16, :] = jnp.zeros((7, 128), F32)


def sd(shape, dtype):
    return jax.ShapeDtypeStruct(shape, dtype)


def packed(rows, width=D, dtype=BF16):
    return sd((2, 4, 2, 2, rows, width), dtype)


ANY = pl.BlockSpec(memory_space=pl.ANY)
VM = pl.BlockSpec(memory_space=pltpu.VMEM)
L4 = ((4, RP, 128), F32)
WIDE = ((R, FF), BF16)
LOW = ((R, D), BF16)
INV = ((R, 128), F32)
SUMM = ((2 * NI, 64, 256), BF16)
REL = ((4, R, 128), F32)
PARK = (("q", L4), ("p", L4), ("v", L4), ("rel", REL), ("s", SUMM))
PARK0 = PARK + (("n1", LOW), ("h1", LOW), ("inv1", INV), ("a", LOW), ("n2", LOW), ("h2", LOW), ("inv2", INV), ("g", WIDE), ("slope", WIDE))
GATHERS = ((0, 0, 16, 0), (0, 16, 32, 1), (0, 32, 48, 2), (0, 48, 128, 4), (0, 128, 192, 6), (1, 0, 64, 8), (1, 64, 128, 10), (1, 128, 192, 12))
PIECES = ((0, 48), (48, 64), (64, 128), (128, 192))
SCATTERS = ((0, 80), (80, 144))


def take_rows(src, dst):
    def fn(at):
        spread(dst, at, src[at, :].astype(F32))
    by_tiles(fn)


def give_rows(src, dst):
    def fn(at):
        dst[at, :] = full(src, at).astype(dst.dtype)
    by_tiles(fn)


def split_rows(flat, packs):
    def row(name, at, first, c):
        val = flat[name][:, pl.ds(pl.multiple_of(at * 512, 512), 512)].astype(F32)
        for layer in range(2):
            packs[layer][pl.ds(first, 1), :] = val[layer:layer + 1, :]
        return c

    def narrow(i, c):
        for j in range(3):
            row("qkv", 3 * i + j, 16 * j + i, c)
        row("proj", i, 48 + i, c)
        for j in range(4):
            row("fc1", 4 * i + j, 64 + 16 * j + i, c)
            row("fc2", 4 * i + j, 128 + 4 * i + j, c)
        return c
    lax.fori_loop(0, 16, narrow, 0)


def join_rows(layer, outs, fc, q):
    def put(name, at, val):
        outs[name][layer:layer + 1, pl.ds(pl.multiple_of(at * 512, 512), 512)] = val

    def body(i, c):
        if q is not None:
            for j in range(3):
                put("qkv", 3 * i + j, q[pl.ds(16 * j + i, 1), :])
        if fc is not None:
            put("proj", i, fc[pl.ds(i, 1), :])
            for j in range(4):
                put("fc1", 4 * i + j, fc[pl.ds(16 + 16 * j + i, 1), :])
                put("fc2", 4 * i + j, fc[pl.ds(80 + 4 * i + j, 1), :])
        return c
    lax.fori_loop(0, 16, body, 0)


FLAT = (("qkv", 24576), ("proj", 8192), ("fc1", 32768), ("fc2", 32768), ("small", 1152))


def mask_rows(ref, sz):
    def body(t, c):
        lg, y = t // GRID, t % GRID
        for ig in range(2):
            size = sz[8 * ig:8 * ig + 8, :]
            for x in range(GRID):
                at = at_cell(y, x, ig)
                ref[lg, at, :] = jnp.where(size > jnp.maximum(y, x), ref[lg, at, :], 0.0)
        return c
    lax.fori_loop(0, 4 * GRID, body, 0)


class Copies:
    def __init__(self, sems):
        self.sems, self.used, self.open = sems, 0, {}

    def start(self, name, src, dst):
        at = self.used
        self.used += 1
        self.open[name] = lambda: pltpu.make_async_copy(src, dst, self.sems.at[at])
        self.open[name]().start()

    def wait(self, *names):
        for name in names:
            self.open.pop(name)().wait()

    def wait_all(self, prefix):
        for name in [n for n in self.open if n.startswith(prefix)]:
            self.wait(name)


class Idle:
    def __call__(self):
        pass

    def upto(self, count):
        pass

    def finish(self):
        pass


COPIES = 80
ROWS6 = (slice(None),) * 4


def step_kernel(comm, names, *refs):
    r = dict(zip(names, refs))
    cps = Copies(r["cs"])
    sz, W, tab, b1 = r["sz"], r["W"], r["tab"], r["b1"]
    gsum, gb1, gfc, gq, gsm, tau = r["gsum"], r["gb1"], r["gfc"], r["gq"], r["gsm"], r["tau"]
    whbm = (r["w0"], r["w1"])
    n1, h1, inv1, a_low = r["n1"], r["h1"], r["inv1"], r["a"]
    xa, xb, da, dxb = r["xa"], r["xb"], r["da"], r["dxb"]
    pv, pr = r["pv"], r["pr"]
    y = pv.at[pl.ds(3 * PROW, D)]
    zero_padded(pv)
    zero_padded(pr)
    scope = pl.run_scoped

    def vm(*shapes):
        return [pltpu.VMEM(*sh) for sh in shapes]

    def load_piece(layer, i):
        a, b = PIECES[i]
        cps.start(f"W{i}", whbm[layer].at[ROWS6 + (pl.ds(a, b - a),)], W.at[ROWS6 + (pl.ds(a, b - a),)])

    STAGE = pltpu.VMEM((R, D), BF16)

    if comm:
        place = Place(4)
        here = (place.c, place.z, place.x, place.y)
        for name, _ in FLAT:
            cps.start("flat" + name, r[name], r["st_" + name])
        for i in range(NI):
            sz[i:i + 1, :] = jnp.full((1, 128), r["sizes"][i], jnp.int32)
        cps.wait("flatsmall")
        r["osm"][...] = jnp.zeros((32, 128), F32)
        for i in range(9):
            val = r["st_small"][:, 128 * i:128 * i + 128].astype(F32)
            for layer in range(2):
                r["osm"][16 * layer + i:16 * layer + i + 1, :] = val[layer:layer + 1, :]
        cps.start("own2", r["osm"], r["gs"].at[here])
        greet(place)
        send, recv = r["as"], r["ar"]
        tiny = Ticker([(0, lambda: gather_ticks(Place(4), r["gs"], slice(None), send.at[0], recv.at[0]))])
        lists = []
        for n, (layer, a, b, first) in enumerate(GATHERS):
            lists.append((first, lambda n=n, layer=layer, a=a, b=b: gather_ticks(Place(4), whbm[layer], pl.ds(a, b - a), send.at[1 + n], recv.at[1 + n])))
        tick = Ticker(lists)
        cps.wait("own2")
        tiny()

        def pack_shards(p0, p1, b0, b1_):
            cps.wait(*("flat" + n for n, _ in FLAT[:4]))
            split_rows({n: r["st_" + n] for n, _ in FLAT[:4]}, (p0, p1))
            b0[...] = p0[...].astype(BF16)
            b1_[...] = p1[...].astype(BF16)
            cps.start("own0", b0, r["w0"].at[here])
            cps.start("own1", b1_, r["w1"].at[here])
            tiny()
            cps.wait("own0", "own1")
        scope(pack_shards, *vm(((WROWS, D), F32), ((WROWS, D), F32), ((WROWS, D), BF16), ((WROWS, D), BF16)))
        tick()
        tiny()

        def begin(stage):
            cps.start("images", r["img"], stage)
            cps.wait("images")
            take_rows(stage, xa)
        scope(begin, STAGE)
        tick()
        tiny()
        tick()
        tiny()
        build_tables(r["gs"], 0, tau, y, tab, b1)
        tick()
    else:
        tick = Idle()

        def begin(stage):
            cps.start("images", r["img"], stage)
            cps.wait("images")
            take_rows(stage, xa)
        scope(begin, STAGE)

    def forward(layer, xin, x1, keep):
        t = tab.at[layer]
        fwd_conv1(xin, sz, t, x1, pv)
        if layer == 0:
            tick()
        norm_phase(x1, t, 0, 1, n1, h1, inv1)
        tick.upto(7 if layer == 0 else 13)
        load_piece(layer, 0)
        if layer == 0:
            for name in ("n1", "h1", "inv1"):
                cps.start("out0" + name, r[name], r["park0" + name])
            if comm:
                build_tables(r["gs"], 1, tau, y, tab, b1)
        else:
            load_piece(1, 1)
        cps.wait("W0")

        def attention(q, p, v, rel, f, s):
            def park(name, ref):
                cps.start(f"park{layer}{name}", ref, r[f"park{layer}{name}"])
            fwd_qkv(h1, W, t, q, p, v)
            park("q", q)
            park("v", v)
            fwd_softmax(p, sz)
            park("p", p)
            if layer == 1:
                tick()
            fwd_attn(q, p, v, s, f)
            park("s", s)
            tick()
            if layer == 1:
                load_piece(1, 2)
            fwd_conv3(v, q, f, sz, t, rel, pv, 1, 0)
            fwd_conv3(v, q, f, sz, t, rel, pv, 2, 1)

            def wide(i, c):
                fwd_conv3(v, q, f, sz, t, rel, pv, 3, i + 2)
                return c
            lax.fori_loop(0, 2, wide, 0)
            park("rel", rel)
            tick()
            if layer == 0:
                load_piece(0, 1)
                load_piece(0, 2)
            cps.wait("W1")
            fwd_proj(f, W, t, x1, a_low)
            cps.wait_all(f"park{layer}")
        scope(attention, *vm(L4, L4, L4, REL, L4, SUMM))
        if layer == 0:
            cps.start("out0a", a_low, r["park0a"])

        def mlp(g, slope, n2, h2, inv2, dm):
            norm_phase(x1, t, 2, 3, n2, h2, inv2)
            if layer == 0:
                tick()
            cps.wait("W2")
            fwd_fc1(h2, W, b1.at[layer], g, slope)
            if layer == 0:
                for name, ref in (("g", g), ("slope", slope), ("n2", n2), ("h2", h2), ("inv2", inv2)):
                    cps.start("out0" + name, ref, r["park0" + name])
                tick.upto(11)
                load_piece(0, 3)
            else:
                tick.upto(17)
                load_piece(1, 3)
            cps.wait("W3")
            fwd_fc2(g, W, t, x1)
            if layer == 0:
                tick()
                cps.wait_all("out0")
            else:
                keep(g, slope, n2, h2, inv2, dm)
        scope(mlp, *vm(WIDE, WIDE, LOW, LOW, INV, LOW))

    events = {}

    def at(layer, point):
        for event in events.get((layer, point), ()):
            event()

    def first_half(layer, dx, da, g, slope, n2, h2, inv2, dm):
        t = tab.at[layer]
        gsum[...] = jnp.zeros_like(gsum)
        bwd_cast_sum(dx, dm, gsum, 7)
        if layer == 0:
            cps.wait("in0slope", "W3")
        bwd_du(dm, W, slope, gb1)
        at(layer, "e0")
        if layer == 0:
            cps.wait("in0g")
        wgrad2(g, dm, gfc, 80)
        at(layer, "e1")
        if layer == 0:
            cps.wait("in0h2", "W2")
        wgrad(h2, slope, gfc, 16, 4)
        at(layer, "e2")
        mm_nt(slope, slice(None), W, 4, 4, da)
        at(layer, "e3")
        if layer == 0:
            cps.wait("in0n2", "in0inv2", "in0a", "W1")
        norm_back_phase(da, n2, inv2, t, 2, dx, dm, gsum, 2, 3, 6)
        at(layer, "e4")
        wgrad(a_low, dm, gfc, 0, 1)
        at(layer, "e5")

    def second_half(layer, xin, dx, da, dv, end):
        t = tab.at[layer]

        def run(q, p, v, rel, dq, dk, s, dj):
            for name, ref in (("q", q), ("p", p), ("v", v), ("s", s), ("rel", rel)):
                cps.start(f"in{layer}" + name, r[f"park{layer}{name}"], ref)
            proj_back(dx, W, da)
            zero_tail(da)
            cps.wait(*(f"in{layer}" + n for n in ("q", "p", "v", "s")))
            bwd_attn1(q, p, v, s, da, dq, dv, dk)
            at(layer, "f1")
            cps.wait(f"in{layer}rel")
            bwd_mix(q, p, v, rel, da, dq, dv, dk, sz, t, gsum, pv, pr, 1, 0)
            at(layer, "f2")
            bwd_mix(q, p, v, rel, da, dq, dv, dk, sz, t, gsum, pv, pr, 2, 1)
            at(layer, "f3")

            def wide(i, c):
                bwd_mix(q, p, v, rel, da, dq, dv, dk, sz, t, gsum, pv, pr, 3, i + 2)
                return c
            lax.fori_loop(0, 2, wide, 0)
            at(layer, "f4")
            bwd_cast(dq, dk, dv, dj)
            if layer == 0:
                cps.wait("W0", "in0h1")
            wgrad(h1, dj, gq, 0, 3)
            at(layer, "f5")
            mm_nt(dj, slice(0, 1536), W, 0, 3, dq)
            at(layer, "f6")
            if layer == 0:
                cps.wait("in0n1", "in0inv1")
            norm_back_phase(dq, n1, inv1, t, 0, dx, None, gsum, 0, 1, None)
            at(layer, "f7")
        scope(run, *vm(L4, L4, L4, REL, L4, L4, SUMM, ((R, 3 * D), BF16)))
        end()
        at(layer, "f8")
        bwd_conv1(xin, dx, da, sz, t, gsum, pv, pr)
        at(layer, "f9")
        build_small(gsum, gb1, y, tau, gsm)
        at(layer, "f10")

    if comm:
        def scatter(n, g, rows, out, which):
            bufs = r["bufs"][4 * which:4 * which + 4]
            return Ticker([(0, lambda: scatter_ticks(Place(4), g, rows, *bufs, out, r["rs"].at[n], r["rr"].at[n]))])

        def release(which):
            def run():
                place = Place(4)
                far = [place.dev(z=place.off(k)) for k in range(1, 4)]
                near = [place.dev(x=1 - place.x), place.dev(y=1 - place.y), place.dev(c=1 - place.c)]
                for who in far + near:
                    pl.semaphore_signal(r["cr"].at[which], inc=1, device_id=who, device_id_type=MESH)
            return run

        def claim(which):
            return lambda: pl.semaphore_wait(r["cr"].at[which], 6)
        fa, fb, qt, st = {}, {}, {}, {}
        for layer in (0, 1):
            (a0, b0), (a1, b1_) = SCATTERS
            out = r[f"sfc{layer}"]
            fa[layer] = scatter(4 * layer, gfc, pl.ds(a0, b0 - a0), out.at[pl.ds(a0, b0 - a0)], 0)
            fb[layer] = scatter(4 * layer + 1, gfc, pl.ds(a1, b1_ - a1), out.at[pl.ds(a1, b1_ - a1)], 1)
            qt[layer] = scatter(4 * layer + 2, gq, slice(None), r[f"sq{layer}"], 2)
            st[layer] = scatter(4 * layer + 3, gsm, slice(None), r[f"ss{layer}"], 3)
        for layer in (0, 1):
            A, B, Q = fa[layer], fb[layer], qt[layer]
            events.update({
                (layer, "e1"): [B], (layer, "e3"): [B], (layer, "e5"): [A], (layer, "f1"): [B, A], (layer, "f3"): [B, A], (layer, "f4"): [B, A],
                (layer, "f5"): [Q], (layer, "f7"): [A, Q], (layer, "f9"): [Q], (layer, "f10"): [st[layer]]})
        events[1, "f7"].append(release(0))
        events[0, "e0"] = [qt[1], st[1]]
        events[0, "e1"] = [qt[1], st[1], claim(0), fb[0]]
        events[0, "e2"] = [st[1]]
        events[0, "e3"] = [st[1], release(1), fb[0]]
        events[0, "f5"] = [claim(1), qt[0]]
    else:
        def put(name, src):
            return lambda: cps.start(name, src, r[name])
        events.update({
            (1, "e5"): [put("gfc1", gfc)], (1, "f4"): [lambda: cps.wait("gfc1")], (1, "f5"): [put("gq1", gq)], (1, "f10"): [put("gsm1", gsm)],
            (0, "e0"): [lambda: cps.wait("gq1", "gsm1")], (0, "e5"): [put("gfc0", gfc)], (0, "f5"): [put("gq0", gq)], (0, "f10"): [put("gsm0", gsm)],
        })

    forward(0, xa, xb, None)

    def top(g, slope, n2, h2, inv2, dm):
        def emit(stage, stage2):
            cps.start("cot", r["ct"], stage)
            mask_rows(xa, sz)
            give_rows(xa, stage2)
            cps.start("out", stage2, r["output"])
            cps.wait("cot")
            take_rows(stage, dxb)
            mask_rows(dxb, sz)
            cps.wait("out")
        scope(emit, STAGE, STAGE)
        first_half(1, dxb, da, g, slope, n2, h2, inv2, dm)
    forward(1, xb, xa, top)

    for i in (2, 3):
        load_piece(0, i)
    cps.start("in0a", r["park0a"], a_low)

    def end1():
        load_piece(0, 0)
        load_piece(0, 1)
        for name, ref in (("h1", h1), ("n1", n1), ("inv1", inv1)):
            cps.start("in0" + name, r["park0" + name], ref)
    second_half(1, xb, dxb, da, xa, end1)

    def bottom(g, slope, n2, h2, inv2, dm):
        for name, ref in (("slope", slope), ("g", g), ("h2", h2), ("n2", n2), ("inv2", inv2)):
            cps.start("in0" + name, r["park0" + name], ref)
        first_half(0, da, dxb, g, slope, n2, h2, inv2, dm)
    scope(bottom, *vm(WIDE, WIDE, LOW, LOW, INV, LOW))

    def end0():
        def again(stage):
            cps.start("again", r["img"], stage)
            cps.wait("again")
            take_rows(stage, xb)
        scope(again, STAGE)
    second_half(0, xb, da, dxb, xa, end0)

    def last(stage3, *flat):
        give_rows(dxb, stage3)
        cps.start("dx", stage3, r["gi"])
        if not comm:
            cps.wait("gfc0", "gq0", "gsm0", "dx")
            return
        o = dict(zip([n for n, _ in FLAT], flat))
        st[0]()
        join_rows(1, o, r["sfc1"], r["sq1"])
        qt[0]()
        st[0]()
        join_rows(0, o, r["sfc0"], None)
        qt[0]()
        st[0]()
        join_rows(0, o, None, r["sq0"])
        for name, _ in FLAT[:4]:
            cps.start("g" + name, o[name], r["g_" + name])
        st[0].finish()
        for layer in (0, 1):
            for i in range(9):
                o["small"][layer:layer + 1, 128 * i:128 * i + 128] = r[f"ss{layer}"][i:i + 1, :]
        cps.start("gsmall", o["small"], r["g_small"])
        cps.wait("dx", *("g" + n for n, _ in FLAT))
    scope(last, pltpu.VMEM((R, D), F32), *([pltpu.VMEM((2, n), F32) for _, n in FLAT] if comm else []))


def step(comm, images, cotangent, sz, *more):
    vmem = pltpu.VMEM
    if comm:
        inputs = ["img", "ct", "sizes"] + [n for n, _ in FLAT]
        in_specs = [ANY, ANY, pl.BlockSpec(memory_space=pltpu.SMEM)] + [ANY] * 5
    else:
        inputs = ["img", "ct", "sz", "w0", "w1", "tab", "b1"]
        in_specs = [ANY, ANY, VM, ANY, ANY, VM, VM]
    outs = [("output", sd((R, D), BF16), ANY), ("gi", sd((R, D), F32), ANY)]
    shares = []
    if comm:
        shares = [("g_" + n, sd((2, count), F32), ANY) for n, count in FLAT]
    for layer in (0, 1):
        if not comm:
            shares += [(f"gfc{layer}", packed(144), ANY), (f"gq{layer}", packed(48), ANY), (f"gsm{layer}", packed(16, 128, F32), ANY)]
    outs += shares
    outs += [(f"park0{n}", sd(*sh), ANY) for n, sh in PARK0] + [(f"park1{n}", sd(*sh), ANY) for n, sh in PARK]
    if comm:
        outs += [("w0", packed(WROWS), ANY), ("w1", packed(WROWS), ANY)]
    scratch = [("W", vmem((2, 4, 2, 2, WROWS, D), BF16)), ("gfc", vmem((2, 4, 2, 2, 144, D), BF16)), ("gq", vmem((2, 4, 2, 2, 48, D), BF16)),
               ("gsm", vmem((2, 4, 2, 2, 16, 128), F32)), ("gsum", vmem((4, TROWS, 128), F32)), ("gb1", vmem((8, FF), F32)),
               ("tau", vmem((288, 128), F32)), ("pv", vmem(PADDED, F32)), ("pr", vmem(PADDED, F32)), ("n1", vmem(*LOW)), ("h1", vmem(*LOW)), ("inv1", vmem(*INV)), ("a", vmem(*LOW))]
    scratch += [(n, vmem(*L4)) for n in ("xa", "xb", "da", "dxb")] + [("cs", pltpu.SemaphoreType.DMA((COPIES,)))]
    bufs = []
    if comm:
        sems = pltpu.SemaphoreType.DMA
        for layer in (0, 1):
            scratch += [(f"sfc{layer}", vmem((144, D), F32)), (f"sq{layer}", vmem((48, D), F32)), (f"ss{layer}", vmem((16, 128), F32))]
        scratch += [("st_" + n, vmem((2, count), BF16)) for n, count in FLAT] + [("osm", vmem((32, 128), F32)), ("sz", vmem((NI, 128), jnp.int32))]
        scratch += [("tab", vmem((2, 4, TROWS, 128), F32)), ("b1", vmem((2, 16, 128), F32)), ("gs", vmem((2, 4, 2, 2, 32, 128), F32)),
                    ("as", sems((9, 8))), ("ar", sems((9, 8))), ("rs", sems((8, 8))), ("rr", sems((8, 8))), ("cr", pltpu.SemaphoreType.REGULAR((2,)))]
        for rows, width, dt in ((80, D, BF16), (64, D, BF16), (48, D, BF16), (16, 128, F32)):
            bufs += scatter_bufs(4, rows, width, dt)
    names = inputs + [n for n, _, _ in outs] + [n for n, _ in scratch]

    def kernel(*refs):
        count = len(names)
        r = list(refs[:count])
        step_kernel(comm, names + ["bufs"], *r, refs[count:])
    params = dict(vmem_limit_bytes=67043328)
    if comm:
        params.update(collective_id=0, has_side_effects=True)
    got = pl.pallas_call(
        kernel, out_shape=[o for _, o, _ in outs], in_specs=in_specs, out_specs=[sp for _, _, sp in outs],
        scratch_shapes=[sc for _, sc in scratch] + bufs, compiler_params=pltpu.CompilerParams(**params), name="step",
    )(images, cotangent, sz, *more)
    return got[:2 + len(shares)]


def window_mask():
    channel = lax.broadcasted_iota(jnp.int32, (49, D), 1)
    tap = lax.broadcasted_iota(jnp.int32, (49, D), 0)
    head = channel // (D // HEADS)
    reach = jnp.where(head < 2, 1, jnp.where(head < 5, 2, 3))
    return ((jnp.abs(tap // 7 - 3) <= reach) & (jnp.abs(tap % 7 - 3) <= reach)).astype(F32)


def blocks_of(flat, rows, cols):
    return flat.reshape(rows, cols // D, D).transpose(1, 0, 2).reshape(rows * cols // D, D)


def pack(qkv, proj, fc1, fc2, n):
    per = D // n
    return jnp.concatenate([blocks_of(qkv, per, 3 * D), proj.reshape(per, D), blocks_of(fc1, per, FF), fc2.reshape(FF // n, D)])


def tables(small):
    small = small.astype(F32)
    end = TABLE * D
    tb = small[:end].reshape(D, TABLE).T
    cpe = small[end + FF:].reshape(D, 10).T
    tab = jnp.concatenate([tb[:9], tb[9:] * window_mask(), jnp.zeros((CPE - TABLE, D), F32), cpe, jnp.zeros((TROWS - CPE - 10, D), F32)])
    return tab.reshape(TROWS, 4, 128).transpose(1, 0, 2), small[end:end + FF].reshape(16, 128)


def whole_weights(mine, small, n):
    per = D // n
    full = lax.all_gather(mine[None], AXES, axis=0, tiled=True)
    vec = lax.all_gather(small, AXES, axis=0, tiled=True)
    parts = [full[:, j * per:(j + 1) * per].reshape(32, D // 32, D) for j in range(8)] + [full[:, 8 * per:].reshape(32, FF // 32, D)]
    w = jnp.concatenate(parts, axis=1).reshape(4, 2, 2, 2, WROWS, D).transpose(3, 0, 1, 2, 4, 5)
    return w, *tables(vec)


def share_by_xla(gfc, gq, gsm, n):
    per = D // n

    def rows(a):
        return a.transpose(1, 2, 3, 0, 4, 5).reshape((32,) + a.shape[4:])
    gq, gfc, gsm = rows(gq), rows(gfc), rows(gsm)
    every = jnp.concatenate([gq, gfc[:, :80]], axis=1)
    parts = [every[:, 16 * j:16 * j + 16].reshape(n, per, D) for j in range(8)] + [gfc[:, 80:].reshape(n, FF // n, D)]
    vec = gsm[:, :9].reshape(n, -1)
    width = vec.shape[1]
    parts.append(jnp.pad(vec, ((0, 0), (0, -width % D))).reshape(n, -1, D).astype(BF16))
    share = lax.psum_scatter(jnp.concatenate(parts, axis=1), AXES, scatter_dimension=0, tiled=True)[0].astype(F32)
    mats = split_shares(share[:8 * per + FF // n], per)
    return (*mats, share[8 * per + FF // n:].reshape(-1)[:width])


def split_shares(share, per):
    def cols(first, count):
        return share[first * per:(first + count) * per].reshape(count, per, D).transpose(1, 0, 2).reshape(-1)
    return cols(0, 3), cols(3, 1), cols(4, 4), share[8 * per:].reshape(-1)


def shards(n, images, grid_sizes, qkv, proj, fc1, fc2, small, cotangent):
    layers = qkv.shape[0]
    images = images.transpose(1, 0, 2).reshape(R, D)
    cotangent = cotangent.transpose(1, 0, 2).reshape(R, D)
    if n == 32:
        output, dx, *grads = step(True, images, cotangent, grid_sizes, qkv, proj, fc1, fc2, small)
    else:
        sz = jnp.broadcast_to(grid_sizes[:, None], (NI, 128))
        mine = [pack(qkv[l], proj[l], fc1[l], fc2[l], n) for l in range(layers)]
        held = [whole_weights(mine[l], small[l], n) for l in range(layers)]
        output, dx, *got = step(False, images, cotangent, sz, held[0][0], held[1][0], jnp.stack([held[0][1], held[1][1]]), jnp.stack([held[0][2], held[1][2]]))
        shares = [share_by_xla(*got[:3], n), share_by_xla(*got[3:], n)]
        grads = [jnp.stack([shares[l][i] for l in range(layers)]) for i in range(5)]
    output, dx = (a.reshape(SLOT, NI, D).transpose(1, 0, 2) for a in (output, dx))
    return (output, dx, *grads)


def solution(mesh):
    n = mesh.shape["wide"] * mesh.shape["narrow"]
    from jax.sharding import PartitionSpec as P
    rows, flat = P(AXES, None, None), P(None, AXES)
    return jax.shard_map(
        functools.partial(shards, n), mesh=mesh,
        in_specs=(rows, P(AXES), flat, flat, flat, flat, flat, rows),
        out_specs=(rows, rows, flat, flat, flat, flat, flat),
        check_vma=False)
```
